32 devices in a mesh: region: 2 (over y), member: 8 (over z, core), space: 2 (over x).
Axes of the slice: x: 2, y: 2, z: 4, core: 2. Of those that a mesh axis runs over, the one named last changes fastest.
Arguments:
- prior_trials: bfloat16 [80, 1536, 256], P('member', ('region', 'space')), parts along dimension 1, may hold values from -6 to 6
- prior_at_sensors: bfloat16 [80, 1536], P('member', ('region', 'space')), parts along dimension 1, may hold values from -6 to 6
- sensor_readings: bfloat16 [1536], P(('region', 'space')), parts along dimension 0, may hold values from -8 to 8
- sensor_noise_spread: bfloat16 [1536], P(('region', 'space')), parts along dimension 0, may hold values from 1 to 10
- nearby_readings: int32 [1536, 128], P(('region', 'space')), parts along dimension 0, may hold values from 0 to 1023, as said below
- subarea_cutoff_level: int32 [1536], P(('region', 'space')), parts along dimension 0, may hold values from 0 to 3
Outputs:
- analysis: bfloat16 [80, 1536, 256], P('member', ('region', 'space')), parts along dimension 1
The draws below stay inside these ranges and needn't reach their ends.
There are 2 independent parts, one for each index of `region`. The reference program is written for one: setup_inputs(seed, part) draws one part's arguments, and reference() takes and returns one part's arrays. A program takes and returns all parts, laid end to end along the dimension named above; each array names one. Nothing has to cross between parts.
Inputs may be any that keep to these rules, and one draw needn't show every extreme that they name: `nearby_readings`: row c lists 128 distinct observations whose region-wide index o lies within (subarea_cutoff_level[c] + 2) * 64 of c and inside the region.
All inputs are finite; a program needn't handle non-finite values. Where the reference program divides by a largest or mean magnitude, that divisor is 1e-20 or more.
Results may differ from the reference program's by a relative error of at most 0.0053.
Values may be sent and summed in bfloat16 or wider, within the bound.
A program may use at most 64 MiB of HBM per device.

```python
import math
import jax
import jax.numpy as jnp
from jax import lax

TRIAL_COUNT = 80
CELL_QUANTITIES = 256
OBS_DOM = 128
TIERS = 4
NS_STEPS = 4
PATCH_CELLS = 384
AREA_CELLS = 768
HALO = 320


def tier_table(key):
    return jax.random.randint(jax.random.fold_in(key, 11), (AREA_CELLS,), 0, TIERS).astype(jnp.int32)


def draw_subarea_cutoff_level(key, part):
    return tier_table(key)


def draw_nearby_readings(key, part):
    tier_ids = tier_table(key)
    columns = jnp.arange(AREA_CELLS, dtype=jnp.int32)
    width_all = 2 * HALO + 1
    offsets = jnp.arange(width_all, dtype=jnp.int32) - HALO
    reach_twice = (tier_ids + 2) * OBS_DOM
    position = columns[:, None] + offsets[None, :]
    usable = (2 * jnp.abs(offsets)[None, :] <= reach_twice[:, None]) & (position >= 0) & (position < AREA_CELLS)
    raw_bits = jax.random.randint(jax.random.fold_in(key, 12), (AREA_CELLS, width_all), 0, 1 << 20).astype(jnp.int32)
    slot_ids = (offsets + HALO)[None, :]
    score = jnp.where(usable, raw_bits * width_all + slot_ids, -1 - slot_ids)
    unused, chosen = lax.top_k(score, OBS_DOM)
    return ((columns % PATCH_CELLS)[:, None] + chosen).astype(jnp.int32)


def draw_sensor_readings(key, part):
    ramp = jnp.arange(AREA_CELLS, dtype=jnp.float32) / AREA_CELLS
    noise = jnp.clip(jax.random.normal(jax.random.fold_in(key, 22), (AREA_CELLS,), jnp.float32), -4.0, 4.0)
    values = 0.6 * (1.0 + 2.0 * ramp) * noise
    return values.astype(jnp.bfloat16)


def block_levels(key, extent, split, low, largest):
    level, own = 1.0, jax.random.fold_in(key, 6)
    for dim, parts in split:
        heights = jnp.exp(jax.random.uniform(jax.random.fold_in(own, dim), (parts,), jnp.float32, low / len(split), largest / len(split)))
        level = level * jnp.repeat(heights, extent[dim] // parts).reshape([-1 if axis == dim else 1 for axis in range(len(extent))])
    return level


def gaussian(own_key, shape, scale, most, pieces=(), kind=jnp.bfloat16):
    drawn = scale * jax.random.normal(own_key, shape, jnp.float32)
    if pieces:
        drawn = drawn * block_levels(own_key, shape, pieces, -0.22, 0.18)
    return jnp.clip(drawn, -most, most).astype(kind)


def setup_inputs(seed: int = 0, part: int = 0) -> dict:
    keys = jax.random.split(jax.random.key(seed), 7)
    own_keys = jax.random.split(jax.random.fold_in(keys[6], part), 7)
    return {
        "prior_trials": gaussian(own_keys[0], (TRIAL_COUNT, AREA_CELLS, CELL_QUANTITIES), 1.0, 6.0, ((0, 8), (1, 2))),
        "prior_at_sensors": gaussian(own_keys[1], (TRIAL_COUNT, AREA_CELLS), 1.0, 6.0, ((0, 8), (1, 2))),
        "sensor_readings": draw_sensor_readings(jax.random.fold_in(jax.random.fold_in(keys[6], part), 71), part),
        "sensor_noise_spread": jnp.clip(jnp.exp(math.log(10.0) - 2.3025851 * jax.random.uniform(own_keys[3], (AREA_CELLS,), jnp.float32) ** block_levels(own_keys[3], (AREA_CELLS,), ((0, 2),), -0.2, 0.2)), 1.0, 10.0).astype(jnp.bfloat16),
        "nearby_readings": draw_nearby_readings(jax.random.fold_in(jax.random.fold_in(keys[6], part), 71), part),
        "subarea_cutoff_level": draw_subarea_cutoff_level(jax.random.fold_in(jax.random.fold_in(keys[6], part), 71), part),
    }


def prepare(picked, trial_lines, offsets, tier_ids, obs_count):
    observ = picked[:trial_lines]
    ens_mean = lax.optimization_barrier(jnp.mean(observ, axis=0))
    anomaly = observ - ens_mean
    innovation = picked[trial_lines] - ens_mean
    radius = (tier_ids.astype(jnp.float32) + 2.0) * (0.5 * obs_count)
    distance = jnp.abs(offsets).astype(jnp.float32) / radius[:, None]
    weight = jnp.exp(-2.0 * distance * distance) / picked[trial_lines + 1]
    return (anomaly, innovation, weight)

def spread_terms(anomaly, innovation, weight, trial_lines):
    fit_sum = jnp.sum(weight * innovation * innovation)
    spread = jnp.sum(weight * lax.optimization_barrier(jnp.sum(anomaly * anomaly, axis=0))) / (trial_lines - 1.0)
    return (fit_sum, spread)

def transform(anomaly, innovation, weight, inflation, trial_lines, sweeps):
    exact = lax.Precision.HIGHEST
    weighted = anomaly * weight[None]
    gram = jnp.einsum('ank,bnk->abn', weighted, anomaly, precision=exact)
    identity = jnp.eye(trial_lines, dtype=jnp.float32)[:, :, None]
    matrix = gram + (trial_lines - 1.0) / inflation * identity
    row_bound = lax.optimization_barrier(jnp.max(lax.optimization_barrier(jnp.sum(jnp.abs(matrix), axis=1)), axis=0))
    root_iter = matrix / row_bound
    inverse = jnp.broadcast_to(identity, matrix.shape)
    for repeat in range(sweeps):
        factor = 1.5 * identity - 0.5 * jnp.einsum('abn,bcn->acn', inverse, root_iter, precision=exact)
        root_iter = jnp.einsum('abn,bcn->acn', root_iter, factor, precision=exact)
        inverse = jnp.einsum('abn,bcn->acn', factor, inverse, precision=exact)
    inv_root = inverse / jnp.sqrt(row_bound)
    target = lax.optimization_barrier(jnp.sum(weighted * innovation[None], axis=2))
    half_gain = jnp.einsum('abn,bn->an', inv_root, target, precision=exact)
    mean_gain = jnp.einsum('abn,bn->an', inv_root, half_gain, precision=exact)
    weights_full = jnp.sqrt(trial_lines - 1.0) * inv_root + mean_gain[:, None, :]
    centred = weights_full - lax.optimization_barrier(jnp.mean(weights_full, axis=0, keepdims=True)) + 1.0 / trial_lines
    return centred.astype(jnp.bfloat16)

def reference(prior_trials, prior_at_sensors, sensor_readings, sensor_noise_spread, nearby_readings, subarea_cutoff_level):
    trial_lines = prior_at_sensors.shape[0]
    obs_count = nearby_readings.shape[1]
    columns = jnp.arange(AREA_CELLS, dtype=jnp.int32)
    global_obs = (nearby_readings + (columns // PATCH_CELLS * PATCH_CELLS - HALO)[:, None]).astype(jnp.int32)
    block_count = AREA_CELLS // PATCH_CELLS

    def block_data(block_no):
        patch_start_index = (block_no * PATCH_CELLS).astype(jnp.int32)
        obs_lists = lax.dynamic_slice_in_dim(global_obs, patch_start_index, PATCH_CELLS, 0)
        col_ids = lax.dynamic_slice_in_dim(columns, patch_start_index, PATCH_CELLS, 0)
        tier_ids = lax.dynamic_slice_in_dim(subarea_cutoff_level, patch_start_index, PATCH_CELLS, 0)
        ens_part = jnp.take(prior_at_sensors, obs_lists, axis=1).astype(jnp.float32)
        value_part = jnp.take(sensor_readings, obs_lists).astype(jnp.float32)[None]
        error_part = jnp.take(sensor_noise_spread, obs_lists).astype(jnp.float32)[None]
        picked = jnp.concatenate([ens_part, value_part, error_part], axis=0)
        return prepare(picked, trial_lines, obs_lists - col_ids[:, None], tier_ids, obs_count)

    def block_sums(block_no):
        anomaly, innovation, weight = block_data(block_no)
        return spread_terms(anomaly, innovation, weight, trial_lines)
    fits, spreads = lax.map(block_sums, jnp.arange(block_count, dtype=jnp.int32))
    inflation = jnp.sum(fits) / jnp.sum(spreads)

    def block_analysis(block_no):
        anomaly, innovation, weight = block_data(block_no)
        trans_w = transform(anomaly, innovation, weight, inflation, trial_lines, NS_STEPS)
        trans_w = lax.optimization_barrier(trans_w).astype(jnp.float32)
        patch_start_index = (block_no * PATCH_CELLS).astype(jnp.int32)
        quantity_lines = lax.dynamic_slice_in_dim(prior_trials, patch_start_index, PATCH_CELLS, 1).astype(jnp.float32)
        updated = jnp.einsum('inc,ijn->jnc', quantity_lines, trans_w, precision=lax.Precision.HIGHEST)
        return updated.astype(jnp.bfloat16)
    piled_pieces = lax.map(block_analysis, jnp.arange(block_count, dtype=jnp.int32))
    return jnp.transpose(piled_pieces, (1, 0, 2, 3)).reshape(trial_lines, AREA_CELLS, prior_trials.shape[2])
```

```python
import functools

import jax
import jax.numpy as jnp
from jax import lax
from jax.experimental import pallas as pl
from jax.experimental.pallas import tpu as pltpu
from jax.sharding import PartitionSpec as P

NS_STEPS = 4
LANES = 128
GROUP = 4
CHUNK = 16
MESH = pl.DeviceIdType.MESH
F32 = jnp.float32
BF16 = jnp.bfloat16


def partner(me, k, n):
    if n & (n - 1):
        return lax.rem(me + k, n)
    other, bit = me, 1
    while bit < n:
        if k & bit:
            other = other + bit * (1 - 2 * lax.rem(me // bit, 2))
        bit *= 2
    return other


def split(value):
    high = value.astype(BF16)
    return high, (value - high.astype(F32)).astype(BF16)


def times(left, right):
    lh, ll = split(left)
    rh, rl = split(right)
    rows, k = left.shape[0], right.shape[0]
    lhs = jnp.concatenate([lh, ll], axis=0)[:, :k]
    rhs = jnp.concatenate([rh, rl], axis=1)
    out = jnp.dot(lhs, rhs, preferred_element_type=F32)
    width = right.shape[1]
    return out[:rows, :width] + out[:rows, width:] + out[rows:, :width]


def analyse_kernel(
    n, spaces, halo, obs_count, x, sensors_in, readings_in, noises_in, lists_in, tiers_in,
    out,
    sensors, readings, noises, lists, tiers, small_sem, pack, incoming, updated, gathered, full, anoms, anoms_t, marks, weights, gram, target, trans,
    moved, sums,
    in_send, in_recv, out_send, out_recv, local_sem, side_send, side_recv, sum_send, sum_recv,
):
    me = lax.axis_index("member")
    space = lax.axis_index("space")
    members, patch, _ = x.shape
    domains = patch // n
    lines = members * n
    width = anoms.shape[1]
    chunks = domains // CHUNK
    peers = n * spaces

    small = [
        pltpu.make_async_copy(source, place, small_sem.at[i])
        for i, (source, place) in enumerate(
            [
                (sensors_in, sensors), (readings_in, readings), (noises_in, noises),
                (lists_in.at[pl.ds(pl.multiple_of(me * domains, 8), domains)], lists),
                (tiers_in, tiers),
            ]
        )
    ]
    for copy in small:
        copy.start()

    def peer(k):
        other = lax.rem(me + space * n + k, peers)
        return {"member": lax.rem(other, n), "space": other // n}

    barrier = pltpu.get_barrier_semaphore()

    def greet(k, carry):
        pl.semaphore_signal(barrier, inc=1, device_id=peer(k), device_id_type=MESH)
        return carry

    lax.fori_loop(1, peers, greet, 0)
    for copy in small:
        copy.wait()
    rows = pack.shape[0]
    pack[...] = jnp.concatenate(
        [
            sensors[...].astype(F32), readings[...].astype(F32)[None],
            noises[...].astype(F32)[None], jnp.ones((rows - members - 2, patch), F32),
        ],
        axis=0,
    ).astype(BF16)
    gathered[1, me] = pack[...]

    lane = lax.broadcasted_iota(jnp.int32, (obs_count, width), 1)

    def mark(group, carry):
        start = pl.multiple_of(group * 8, 8)
        columns = jnp.transpose(lists[pl.ds(start, 8), :] - me * domains)
        found = []
        for d in range(8):
            hit = columns[:, d : d + 1] == lane
            found.append(jnp.sum(jnp.where(hit, 1.0, 0.0), axis=0, keepdims=True))
        marks[pl.ds(start, 8), :] = jnp.concatenate(found, axis=0)
        return carry

    pl.semaphore_wait(barrier, peers - 1)

    def side_copy(side, k):
        to_space = lax.rem(space + 1 - side + spaces, spaces)
        return pltpu.make_async_remote_copy(
            pack, gathered.at[side, me], side_send.at[side, k], side_recv.at[side, k],
            device_id={"member": partner(me, k, n), "space": to_space}, device_id_type=MESH,
        )

    has_left, has_right = space > 0, space < spaces - 1
    for k in range(1, n):
        side_copy(1, k).start()

    @pl.when(has_right)
    def _():
        for k in range(n):
            side_copy(0, k).start()

    @pl.when(has_left)
    def _():
        for k in range(n):
            side_copy(2, k).start()

    def in_views(to, g):
        return (
            x.at[:, pl.ds(pl.multiple_of(to * domains + g * CHUNK, 16), CHUNK), :],
            incoming.at[pl.ds(me * members, members), pl.ds(g * CHUNK, CHUNK), :],
        )

    def in_copy(g, k):
        to = partner(me, k, n)
        source, place = in_views(to, g)
        return pltpu.make_async_remote_copy(
            source, place, in_send.at[g, k], in_recv.at[g, k],
            device_id={"member": to}, device_id_type=MESH,
        )

    far_first = list(range(n // 2, n)) + list(range(1, n // 2))
    pairs = [(g, k) for g in range(chunks) for k in far_first]
    early = n - 1
    for g, k in pairs[:early]:
        in_copy(g, k).start()
    own = []
    for g in range(chunks):
        source, place = in_views(me, g)
        copy = pltpu.make_async_copy(source, place, local_sem.at[0, g])
        copy.start()
        own.append(copy)

    @pl.when(space == 0)
    def _():
        gathered[0] = jnp.ones(gathered.shape[1:], BF16)

    @pl.when(space == spaces - 1)
    def _():
        gathered[2] = jnp.ones(gathered.shape[1:], BF16)

    lax.fori_loop(0, domains // 8, mark, 0)

    for k in range(1, n):
        side_copy(1, k).wait()

    @pl.when(has_right)
    def _():
        for k in range(n):
            side_copy(0, k).wait_send()
            side_copy(2, k).wait_recv()

    @pl.when(has_left)
    def _():
        for k in range(n):
            side_copy(2, k).wait_send()
            side_copy(0, k).wait_recv()

    for side in range(3):
        for s in range(n):
            full[members * s : members * (s + 1), patch * side : patch * (side + 1)] = (
                gathered[side, s, :members, :].astype(F32)
            )
        full[lines : lines + 2, patch * side : patch * (side + 1)] = (
            gathered[side, 0, members : members + 2, :].astype(F32)
        )
    total = 3 * patch
    shift = lax.rem(2 * total - (patch - halo) - me * domains, total)
    turned = pltpu.roll(full[...], shift, 1)[:, :width]
    values = turned[:lines]
    mean = jnp.sum(values, axis=0, keepdims=True) * (1.0 / lines)
    anomaly = values - mean
    anoms[...] = anomaly
    innov = turned[lines : lines + 1] - mean
    noise = turned[lines + 1 : lines + 2]
    squares = jnp.sum(anomaly * anomaly, axis=0, keepdims=True)

    own_tier = lax.broadcasted_iota(jnp.int32, (domains, patch), 1) == (
        lax.broadcasted_iota(jnp.int32, (domains, patch), 0) + me * domains
    )
    tier = jnp.sum(jnp.where(own_tier, tiers[...].astype(F32)[None], 0.0), axis=1, keepdims=True)
    radius = (tier + 2.0) * (0.5 * obs_count)
    place = lax.broadcasted_iota(jnp.int32, (domains, width), 1)
    row = lax.broadcasted_iota(jnp.int32, (domains, width), 0)
    distance = jnp.abs(place - halo - row).astype(F32) / radius
    weight = marks[...] * jnp.exp(-2.0 * distance * distance) / noise
    weights[...] = weight
    fit = jnp.sum(weight * (innov * innov))
    spread = jnp.sum(weight * squares)
    first = lax.broadcasted_iota(jnp.int32, (1, LANES), 1) == 0
    moved[...] = jnp.where(first, fit, spread)

    high, low = split(anomaly)
    pad = jnp.zeros((LANES - lines, width), F32)
    anoms_t[...] = jnp.concatenate(
        [
            jnp.transpose(jnp.concatenate([high.astype(F32), pad], axis=0)),
            jnp.transpose(jnp.concatenate([low.astype(F32), pad], axis=0)),
        ],
        axis=1,
    ).astype(BF16)

    def sum_copy(k):
        return pltpu.make_async_remote_copy(
            moved, sums.at[k], sum_send.at[k], sum_recv.at[k],
            device_id=peer(k), device_id_type=MESH,
        )

    def start_sum(k, carry):
        sum_copy(k).start()
        return carry

    def end_sum(k, carry):
        sum_copy(k).wait()
        return carry + sums[k]

    lax.fori_loop(1, peers, start_sum, 0)
    for g, k in pairs[early:]:
        in_copy(g, k).start()

    hi, lo = split(weight * innov)
    aims = jnp.dot(jnp.concatenate([hi, lo], axis=0), anoms_t[...], preferred_element_type=F32)
    target[...] = aims[:domains, :LANES] + aims[:domains, LANES:] + aims[domains:, :LANES]

    def gram_group(g, carry):
        for d in range(2):
            c = g * 2 + d
            hi, lo = split(anoms[...] * weights[pl.ds(c, 1), :])
            prod = jnp.dot(
                jnp.concatenate([hi, lo], axis=0), anoms_t[...], preferred_element_type=F32
            )
            gram[c] = prod[:lines, :LANES] + prod[:lines, LANES:] + prod[lines:, :LANES]
        return carry

    lax.fori_loop(0, domains // 2, gram_group, 0)

    sums_all = lax.fori_loop(1, peers, end_sum, moved[...])
    scale = sums_all[:, 1:2] / sums_all[:, 0:1]
    eye = jnp.where(
        lax.broadcasted_iota(jnp.int32, (lines, LANES), 0)
        == lax.broadcasted_iota(jnp.int32, (lines, LANES), 1),
        1.0, 0.0,
    )
    diagonal = eye * scale

    def solve_group(g, carry):
        ids = [g * GROUP + d for d in range(GROUP)]
        mats = [gram[c] + diagonal for c in ids]
        bounds = [
            jnp.max(jnp.sum(jnp.abs(m), axis=0, keepdims=True), axis=1, keepdims=True)
            for m in mats
        ]
        ys = [m / b for m, b in zip(mats, bounds)]
        zs = [1.5 * eye - 0.5 * y for y in ys]
        ys = [times(y, z) for y, z in zip(ys, zs)]
        for step in range(1, NS_STEPS):
            ps = [1.5 * eye - 0.5 * times(z, y) for z, y in zip(zs, ys)]
            if step < NS_STEPS - 1:
                both = [
                    times(jnp.concatenate([y, z], axis=0), p) for y, z, p in zip(ys, zs, ps)
                ]
                ys = [b[:lines] for b in both]
                zs = [b[lines:] for b in both]
            else:
                zs = [times(z, p) for z, p in zip(zs, ps)]
        roots = [z * lax.rsqrt(b) for z, b in zip(zs, bounds)]
        for c, root in zip(ids, roots):
            half_gain = jnp.sum(root * target[pl.ds(c, 1), :], axis=1, keepdims=True)
            gain = jnp.sum(root * half_gain, axis=0, keepdims=True)
            w = (lines - 1.0) ** 0.5 * root + gain
            w = w - jnp.sum(w, axis=1, keepdims=True) * (1.0 / lines) + 1.0 / lines
            trans[c] = w.astype(BF16)
        return carry

    def out_views(to, g):
        return (
            updated.at[pl.ds(to * members, members), pl.ds(g * CHUNK, CHUNK), :],
            out.at[:, pl.ds(pl.multiple_of(me * domains + g * CHUNK, 16), CHUNK), :],
        )

    def out_copy(g, k):
        to = partner(me, k, n)
        source, place = out_views(to, g)
        return pltpu.make_async_remote_copy(
            source, place, out_send.at[g, k], out_recv.at[g, k],
            device_id={"member": to}, device_id_type=MESH,
        )

    for g in range(chunks):
        lax.fori_loop(g * CHUNK // GROUP, (g + 1) * CHUNK // GROUP, solve_group, 0)
        own[g].wait()
        for k in range(1, n):
            in_copy(g, k).wait()
        states = jnp.swapaxes(incoming[:, g * CHUNK : (g + 1) * CHUNK, :].astype(F32), 0, 1)
        states = states.astype(BF16)
        results = [
            jnp.dot(trans[g * CHUNK + c][:, :lines], states[c], preferred_element_type=F32)
            for c in range(CHUNK)
        ]
        results = jnp.stack(results, axis=0)
        updated[:, g * CHUNK : (g + 1) * CHUNK, :] = jnp.swapaxes(results, 0, 1).astype(BF16)
        for k in far_first:
            out_copy(g, k).start()
        source, place = out_views(me, g)
        copy = pltpu.make_async_copy(source, place, local_sem.at[1, g])
        copy.start()
        own.append(copy)

    for g in range(chunks):
        own[chunks + g].wait()
        for k in range(1, n):
            out_copy(g, k).wait()


def per_device(trials, sensors, readings, noises, lists, tiers):
    n, spaces = lax.axis_size("member"), lax.axis_size("space")
    members, patch, quantities = trials.shape
    obs_count = lists.shape[1]
    halo = 5 * obs_count // 2
    domains = patch // n
    chunks = domains // CHUNK
    lines = members * n
    width = -(-(domains + 2 * halo) // 256) * 256
    rows = -(-(members + 2) // 16) * 16
    vmem = pl.BlockSpec(memory_space=pltpu.VMEM)
    anywhere = pl.BlockSpec(memory_space=pltpu.HBM)
    full_rows = -(-(lines + 2) // 8) * 8
    dma = pltpu.SemaphoreType.DMA
    return pl.pallas_call(
        functools.partial(analyse_kernel, n, spaces, halo, obs_count),
        out_shape=pltpu.VMEM((members, patch, quantities), BF16),
        in_specs=[anywhere] * 6,
        out_specs=vmem,
        scratch_shapes=[
            pltpu.VMEM((members, patch), BF16),
            pltpu.VMEM((patch,), BF16),
            pltpu.VMEM((patch,), BF16),
            pltpu.VMEM((domains, obs_count), jnp.int32),
            pltpu.VMEM((patch,), jnp.int32),
            dma((5,)),
            pltpu.VMEM((rows, patch), BF16),
            pltpu.VMEM((lines, domains, quantities), BF16),
            pltpu.VMEM((lines, domains, quantities), BF16),
            pltpu.VMEM((3, n, rows, patch), BF16),
            pltpu.VMEM((full_rows, 3 * patch), F32),
            pltpu.VMEM((lines, width), F32),
            pltpu.VMEM((width, 2 * LANES), BF16),
            pltpu.VMEM((domains, width), F32),
            pltpu.VMEM((domains, width), F32),
            pltpu.VMEM((domains, lines, LANES), F32),
            pltpu.VMEM((domains, LANES), F32),
            pltpu.VMEM((domains, lines, LANES), BF16),
            pltpu.VMEM((1, LANES), F32),
            pltpu.VMEM((n * spaces, 1, LANES), F32),
            dma((chunks, n)), dma((chunks, n)), dma((chunks, n)), dma((chunks, n)),
            dma((2, chunks)), dma((3, n)), dma((3, n)), dma((n * spaces,)), dma((n * spaces,)),
        ],
        compiler_params=pltpu.CompilerParams(
            collective_id=0, has_side_effects=True, vmem_limit_bytes=40 << 20
        ),
        name="analyse",
    )(*[pltpu.with_memory_space_constraint(a, pltpu.HBM) for a in (trials, sensors, readings, noises, lists, tiers)])


def solution(mesh):
    return jax.shard_map(
        per_device,
        mesh=mesh,
        in_specs=(
            P("member", ("region", "space"), None),
            P("member", ("region", "space")),
            P(("region", "space")),
            P(("region", "space")),
            P(("region", "space"), None),
            P(("region", "space")),
        ),
        out_specs=P("member", ("region", "space"), None),
        check_vma=False,
    )
```

```python
import functools

import jax
import jax.numpy as jnp
from jax import lax
from jax.experimental import pallas as pl
from jax.experimental.pallas import tpu as pltpu
from jax.sharding import PartitionSpec as P

NS_STEPS = 4
LANES = 128
GROUP = 4
CHUNK = 16
MESH = pl.DeviceIdType.MESH
F32 = jnp.float32
BF16 = jnp.bfloat16


def partner(me, k, n):
    if n & (n - 1):
        return lax.rem(me + k, n)
    other, bit = me, 1
    while bit < n:
        if k & bit:
            other = other + bit * (1 - 2 * lax.rem(me // bit, 2))
        bit *= 2
    return other


def split(value):
    high = value.astype(BF16)
    return high, (value - high.astype(F32)).astype(BF16)


def times(left, right):
    lh, ll = split(left)
    rh, rl = split(right)
    rows, k = left.shape[0], right.shape[0]
    lhs = jnp.concatenate([lh, ll], axis=0)[:, :k]
    rhs = jnp.concatenate([rh, rl], axis=1)
    out = jnp.dot(lhs, rhs, preferred_element_type=F32)
    width = right.shape[1]
    return out[:rows, :width] + out[:rows, width:] + out[rows:, :width]


def analyse_kernel(
    n, spaces, halo, obs_count, x, sensors_in, readings_in, noises_in, lists_in, tiers_in,
    out,
    readings, noises, left_readings, left_noises, right_readings, right_noises, lists, tiers, small_sem, incoming, updated, gathered, full, anoms, anoms_t, marks, weights, gram, target, trans,
    moved, sums,
    in_send, in_recv, out_send, out_recv, local_sem, near_send, near_recv, chip_send, chip_recv, side_send, side_recv, sum_send, sum_recv,
):
    me = lax.axis_index("member")
    space = lax.axis_index("space")
    members, patch, _ = x.shape
    domains = patch // n
    lines = members * n
    width = anoms.shape[1]
    chunks = domains // CHUNK
    peers = n * spaces
    cores = 2 - n % 2
    chips = n // cores
    core, chip = lax.rem(me, cores), me // cores

    def slot(member):
        return lax.rem(member, cores) * chips + member // cores

    small = [
        pltpu.make_async_copy(source, place, small_sem.at[i])
        for i, (source, place) in enumerate(
            [
                (sensors_in, gathered.at[1, slot(me)]), (readings_in, readings), (noises_in, noises),
                (lists_in.at[pl.ds(pl.multiple_of(me * domains, 8), domains)], lists),
                (tiers_in, tiers),
            ]
        )
    ]
    for copy in small:
        copy.start()

    def peer(k):
        other = lax.rem(me + space * n + k, peers)
        return {"member": lax.rem(other, n), "space": other // n}

    barrier = pltpu.get_barrier_semaphore()

    def greet(k, carry):
        pl.semaphore_signal(barrier, inc=1, device_id=peer(k), device_id_type=MESH)
        return carry

    lax.fori_loop(1, peers, greet, 0)
    small[0].wait()

    lane = lax.broadcasted_iota(jnp.int32, (obs_count, width), 1)

    def mark(group, carry):
        start = pl.multiple_of(group * 8, 8)
        columns = jnp.transpose(lists[pl.ds(start, 8), :] - me * domains)
        found = []
        for d in range(8):
            hit = columns[:, d : d + 1] == lane
            found.append(jnp.sum(jnp.where(hit, 1.0, 0.0), axis=0, keepdims=True))
        marks[pl.ds(start, 8), :] = jnp.concatenate(found, axis=0)
        return carry

    with jax.named_scope("w_barrier"):
        pl.semaphore_wait(barrier, peers - 1)

    has_left, has_right = space > 0, space < spaces - 1

    def to_space(side):
        return lax.rem(space + 1 - side + spaces, spaces)

    def chip_copy(j):
        place = gathered.at[1, slot(me)]
        other = partner(chip, j, chips) * cores + core
        return pltpu.make_async_remote_copy(
            place, place, chip_send.at[j], chip_recv.at[j],
            device_id={"member": other}, device_id_type=MESH,
        )

    singles = [(left_readings, left_noises), (readings, noises), (right_readings, right_noises)]

    def near_copies(side):
        index = side // 2
        return [
            pltpu.make_async_remote_copy(
                source, place, near_send.at[index, i], near_recv.at[index, i],
                device_id={"space": to_space(side)}, device_id_type=MESH,
            )
            for i, (source, place) in enumerate(zip((readings_in, noises_in), singles[side]))
        ]

    def side_copy(side, t):
        rows = pl.ds(core * chips, chips)
        return pltpu.make_async_remote_copy(
            gathered.at[1, rows], gathered.at[side, rows],
            side_send.at[side, t], side_recv.at[side, t],
            device_id={"member": chip * cores + lax.rem(core + t, cores), "space": to_space(side)},
            device_id_type=MESH,
        )

    for j in range(1, chips):
        chip_copy(j).start()

    @pl.when(has_right)
    def _():
        for copy in near_copies(0):
            copy.start()

    @pl.when(has_left)
    def _():
        for copy in near_copies(2):
            copy.start()

    def in_views(to, g):
        return (
            x.at[:, pl.ds(pl.multiple_of(to * domains + g * CHUNK, 16), CHUNK), :],
            incoming.at[pl.ds(me * members, members), pl.ds(g * CHUNK, CHUNK), :],
        )

    def in_copy(g, k):
        to = partner(me, k, n)
        source, place = in_views(to, g)
        return pltpu.make_async_remote_copy(
            source, place, in_send.at[g, k], in_recv.at[g, k],
            device_id={"member": to}, device_id_type=MESH,
        )

    far = list(range(n // 2, n))
    close = list(range(1, n // 2))
    far_first = far + close
    middle = (me >= n // 2 - cores) & (me < n // 2 + cores)
    pairs = [(g, k) for g in range(chunks) for k in far_first]
    middle_early = [(0, k) for k in far_first]
    outer_early = [(g, k) for g in range(chunks) for k in close]

    @pl.when(middle)
    def _():
        for g, k in middle_early:
            in_copy(g, k).start()

    @pl.when(jnp.logical_not(middle))
    def _():
        for g, k in outer_early:
            in_copy(g, k).start()

    own = []
    for g in range(chunks):
        source, place = in_views(me, g)
        copy = pltpu.make_async_copy(source, place, local_sem.at[0, g])
        copy.start()
        own.append(copy)

    for side, missing in ((0, space == 0), (2, space == spaces - 1)):
        @pl.when(missing)
        def _():
            gathered[side] = jnp.ones(gathered.shape[1:], BF16)
            for single in singles[side]:
                single[...] = jnp.ones(single.shape, BF16)

    for copy in small[1:]:
        copy.wait()
    with jax.named_scope("marks"):
        lax.fori_loop(0, domains // 8, mark, 0)

    with jax.named_scope("w_chip"):
        for j in range(1, chips):
            chip_copy(j).wait()

    for t in range(1, cores):
        side_copy(1, t).start()

    @pl.when(has_right)
    def _():
        for t in range(cores):
            side_copy(0, t).start()

    @pl.when(has_left)
    def _():
        for t in range(cores):
            side_copy(2, t).start()

    with jax.named_scope("w_side"):
        for t in range(1, cores):
            side_copy(1, t).wait()

        @pl.when(has_right)
        def _():
            for copy in near_copies(0):
                copy.wait_send()
            for copy in near_copies(2):
                copy.wait_recv()
            for t in range(cores):
                side_copy(0, t).wait_send()
                side_copy(2, t).wait_recv()

        @pl.when(has_left)
        def _():
            for copy in near_copies(2):
                copy.wait_send()
            for copy in near_copies(0):
                copy.wait_recv()
            for t in range(cores):
                side_copy(2, t).wait_send()
                side_copy(0, t).wait_recv()

    for side in range(3):
        for s in range(n):
            full[members * s : members * (s + 1), patch * side : patch * (side + 1)] = (
                gathered[side, s % cores * chips + s // cores].astype(F32)
            )
        for i, single in enumerate(singles[side]):
            full[lines + i : lines + i + 1, patch * side : patch * (side + 1)] = (
                single[...].astype(F32)[None]
            )
    total = 3 * patch
    shift = lax.rem(2 * total - (patch - halo) - me * domains, total)
    turned = pltpu.roll(full[...], shift, 1)[:, :width]
    values = turned[:lines]
    mean = jnp.sum(values, axis=0, keepdims=True) * (1.0 / lines)
    anomaly = values - mean
    anoms[...] = anomaly
    innov = turned[lines : lines + 1] - mean
    noise = turned[lines + 1 : lines + 2]
    squares = jnp.sum(anomaly * anomaly, axis=0, keepdims=True)

    own_tier = lax.broadcasted_iota(jnp.int32, (domains, patch), 1) == (
        lax.broadcasted_iota(jnp.int32, (domains, patch), 0) + me * domains
    )
    tier = jnp.sum(jnp.where(own_tier, tiers[...].astype(F32)[None], 0.0), axis=1, keepdims=True)
    radius = (tier + 2.0) * (0.5 * obs_count)
    place = lax.broadcasted_iota(jnp.int32, (domains, width), 1)
    row = lax.broadcasted_iota(jnp.int32, (domains, width), 0)
    distance = jnp.abs(place - halo - row).astype(F32) / radius
    weight = marks[...] * jnp.exp(-2.0 * distance * distance) / noise
    weights[...] = weight
    fit = jnp.sum(weight * (innov * innov))
    spread = jnp.sum(weight * squares)
    first = lax.broadcasted_iota(jnp.int32, (1, LANES), 1) == 0
    moved[...] = jnp.where(first, fit, spread)

    high, low = split(anomaly)
    pad = jnp.zeros((LANES - lines, width), F32)
    anoms_t[...] = jnp.concatenate(
        [
            jnp.transpose(jnp.concatenate([high.astype(F32), pad], axis=0)),
            jnp.transpose(jnp.concatenate([low.astype(F32), pad], axis=0)),
        ],
        axis=1,
    ).astype(BF16)

    def sum_copy(k):
        return pltpu.make_async_remote_copy(
            moved, sums.at[k], sum_send.at[k], sum_recv.at[k],
            device_id=peer(k), device_id_type=MESH,
        )

    def start_sum(k, carry):
        sum_copy(k).start()
        return carry

    def end_sum(k, carry):
        sum_copy(k).wait()
        return carry + sums[k]

    lax.fori_loop(1, peers, start_sum, 0)

    @pl.when(middle)
    def _():
        for g, k in pairs:
            if (g, k) not in middle_early:
                in_copy(g, k).start()

    hi, lo = split(weight * innov)
    aims = jnp.dot(jnp.concatenate([hi, lo], axis=0), anoms_t[...], preferred_element_type=F32)
    target[...] = aims[:domains, :LANES] + aims[:domains, LANES:] + aims[domains:, :LANES]

    def gram_group(g, carry):
        for d in range(2):
            c = g * 2 + d
            hi, lo = split(anoms[...] * weights[pl.ds(c, 1), :])
            prod = jnp.dot(
                jnp.concatenate([hi, lo], axis=0), anoms_t[...], preferred_element_type=F32
            )
            gram[c] = prod[:lines, :LANES] + prod[:lines, LANES:] + prod[lines:, :LANES]
        return carry

    with jax.named_scope('gram'):
        lax.fori_loop(0, domains // 2, gram_group, 0)

    with jax.named_scope("w_sums"):
        sums_all = lax.fori_loop(1, peers, end_sum, moved[...])

    @pl.when(jnp.logical_not(middle))
    def _():
        for g, k in pairs:
            if (g, k) not in outer_early:
                in_copy(g, k).start()

    scale = sums_all[:, 1:2] / sums_all[:, 0:1]
    eye = jnp.where(
        lax.broadcasted_iota(jnp.int32, (lines, LANES), 0)
        == lax.broadcasted_iota(jnp.int32, (lines, LANES), 1),
        1.0, 0.0,
    )
    diagonal = eye * scale

    def solve_group(g, carry):
        ids = [g * GROUP + d for d in range(GROUP)]
        mats = [gram[c] + diagonal for c in ids]
        bounds = [
            jnp.max(jnp.sum(jnp.abs(m), axis=0, keepdims=True), axis=1, keepdims=True)
            for m in mats
        ]
        ys = [m / b for m, b in zip(mats, bounds)]
        zs = [1.5 * eye - 0.5 * y for y in ys]
        ys = [times(y, z) for y, z in zip(ys, zs)]
        for step in range(1, NS_STEPS):
            ps = [1.5 * eye - 0.5 * times(z, y) for z, y in zip(zs, ys)]
            if step < NS_STEPS - 1:
                both = [
                    times(jnp.concatenate([y, z], axis=0), p) for y, z, p in zip(ys, zs, ps)
                ]
                ys = [b[:lines] for b in both]
                zs = [b[lines:] for b in both]
            else:
                zs = [times(z, p) for z, p in zip(zs, ps)]
        roots = [z * lax.rsqrt(b) for z, b in zip(zs, bounds)]
        for c, root in zip(ids, roots):
            half_gain = jnp.sum(root * target[pl.ds(c, 1), :], axis=1, keepdims=True)
            gain = jnp.sum(root * half_gain, axis=0, keepdims=True)
            w = (lines - 1.0) ** 0.5 * root + gain
            w = w - jnp.sum(w, axis=1, keepdims=True) * (1.0 / lines) + 1.0 / lines
            trans[c] = w.astype(BF16)
        return carry

    def out_views(to, g):
        return (
            updated.at[pl.ds(to * members, members), pl.ds(g * CHUNK, CHUNK), :],
            out.at[:, pl.ds(pl.multiple_of(me * domains + g * CHUNK, 16), CHUNK), :],
        )

    def out_copy(g, k):
        to = partner(me, k, n)
        source, place = out_views(to, g)
        return pltpu.make_async_remote_copy(
            source, place, out_send.at[g, k], out_recv.at[g, k],
            device_id={"member": to}, device_id_type=MESH,
        )

    for g in range(chunks):
        with jax.named_scope(f'solve{g}'):
            lax.fori_loop(g * CHUNK // GROUP, (g + 1) * CHUNK // GROUP, solve_group, 0)
        with jax.named_scope(f'w_in{g}'):
            own[g].wait()
            for k in range(1, n):
                in_copy(g, k).wait()
        states = jnp.swapaxes(incoming[:, g * CHUNK : (g + 1) * CHUNK, :].astype(F32), 0, 1)
        states = states.astype(BF16)
        results = [
            jnp.dot(trans[g * CHUNK + c][:, :lines], states[c], preferred_element_type=F32)
            for c in range(CHUNK)
        ]
        results = jnp.stack(results, axis=0)
        updated[:, g * CHUNK : (g + 1) * CHUNK, :] = jnp.swapaxes(results, 0, 1).astype(BF16)
        for k in far_first:
            out_copy(g, k).start()
        source, place = out_views(me, g)
        copy = pltpu.make_async_copy(source, place, local_sem.at[1, g])
        copy.start()
        own.append(copy)

    for g in range(chunks):
        with jax.named_scope(f'w_out{g}'):
            own[chunks + g].wait()
            for k in range(1, n):
                out_copy(g, k).wait()


def per_device(trials, sensors, readings, noises, lists, tiers):
    n, spaces = lax.axis_size("member"), lax.axis_size("space")
    members, patch, quantities = trials.shape
    obs_count = lists.shape[1]
    halo = 5 * obs_count // 2
    domains = patch // n
    chunks = domains // CHUNK
    lines = members * n
    width = -(-(domains + 2 * halo) // 256) * 256
    vmem = pl.BlockSpec(memory_space=pltpu.VMEM)
    anywhere = pl.BlockSpec(memory_space=pltpu.HBM)
    full_rows = -(-(lines + 2) // 8) * 8
    dma = pltpu.SemaphoreType.DMA
    return pl.pallas_call(
        functools.partial(analyse_kernel, n, spaces, halo, obs_count),
        out_shape=pltpu.VMEM((members, patch, quantities), BF16),
        in_specs=[anywhere] * 6,
        out_specs=vmem,
        scratch_shapes=[
            pltpu.VMEM((patch,), BF16),
            pltpu.VMEM((patch,), BF16),
            pltpu.VMEM((patch,), BF16),
            pltpu.VMEM((patch,), BF16),
            pltpu.VMEM((patch,), BF16),
            pltpu.VMEM((patch,), BF16),
            pltpu.VMEM((domains, obs_count), jnp.int32),
            pltpu.VMEM((patch,), jnp.int32),
            dma((5,)),
            pltpu.VMEM((lines, domains, quantities), BF16),
            pltpu.VMEM((lines, domains, quantities), BF16),
            pltpu.VMEM((3, n, members, patch), BF16),
            pltpu.VMEM((full_rows, 3 * patch), F32),
            pltpu.VMEM((lines, width), F32),
            pltpu.VMEM((width, 2 * LANES), BF16),
            pltpu.VMEM((domains, width), F32),
            pltpu.VMEM((domains, width), F32),
            pltpu.VMEM((domains, lines, LANES), F32),
            pltpu.VMEM((domains, LANES), F32),
            pltpu.VMEM((domains, lines, LANES), BF16),
            pltpu.VMEM((1, LANES), F32),
            pltpu.VMEM((n * spaces, 1, LANES), F32),
            dma((chunks, n)), dma((chunks, n)), dma((chunks, n)), dma((chunks, n)),
            dma((2, chunks)), dma((2, 2)), dma((2, 2)), dma((n,)), dma((n,)), dma((3, 2)), dma((3, 2)),
            dma((n * spaces,)), dma((n * spaces,)),
        ],
        compiler_params=pltpu.CompilerParams(
            collective_id=0, has_side_effects=True, vmem_limit_bytes=40 << 20
        ),
        name="analyse",
    )(*[pltpu.with_memory_space_constraint(a, pltpu.HBM) for a in (trials, sensors, readings, noises, lists, tiers)])


def solution(mesh):
    return jax.shard_map(
        per_device,
        mesh=mesh,
        in_specs=(
            P("member", ("region", "space"), None),
            P("member", ("region", "space")),
            P(("region", "space")),
            P(("region", "space")),
            P(("region", "space"), None),
            P(("region", "space")),
        ),
        out_specs=P("member", ("region", "space"), None),
        check_vma=False,
    )
```

```python
import functools

import jax
import jax.numpy as jnp
from jax import lax
from jax.experimental import pallas as pl
from jax.experimental.pallas import tpu as pltpu
from jax.sharding import PartitionSpec as P

NS_STEPS = 4
LANES = 128
GROUP = 4
CHUNK = 16
MESH = pl.DeviceIdType.MESH
F32 = jnp.float32
BF16 = jnp.bfloat16


def partner(me, k, n):
    if n & (n - 1):
        return lax.rem(me + k, n)
    other, bit = me, 1
    while bit < n:
        if k & bit:
            other = other + bit * (1 - 2 * lax.rem(me // bit, 2))
        bit *= 2
    return other


def split(value):
    high = value.astype(BF16)
    return high, (value - high.astype(F32)).astype(BF16)


def times(left, right):
    lh, ll = split(left)
    rh, rl = split(right)
    rows, k = left.shape[0], right.shape[0]
    lhs = jnp.concatenate([lh, ll], axis=0)[:, :k]
    rhs = jnp.concatenate([rh, rl], axis=1)
    out = jnp.dot(lhs, rhs, preferred_element_type=F32)
    width = right.shape[1]
    return out[:rows, :width] + out[:rows, width:] + out[rows:, :width]


def analyse_kernel(
    n, spaces, halo, obs_count, x, sensors_in, readings_in, noises_in, lists_in, tiers_in,
    out,
    readings, noises, left_readings, left_noises, right_readings, right_noises, lists, tiers, small_sem, incoming, updated, gathered, full, anoms, anoms_t, marks, weights, gram, target, trans,
    moved, sums,
    in_send, in_recv, out_send, out_recv, near_send, near_recv, chip_send, chip_recv, side_send, side_recv, sum_send, sum_recv,
):
    me = lax.axis_index("member")
    space = lax.axis_index("space")
    members, patch, _ = x.shape
    domains = patch // n
    lines = members * n
    width = anoms.shape[1]
    chunks = domains // CHUNK
    peers = n * spaces
    cores = 2 - n % 2
    chips = n // cores
    core, chip = lax.rem(me, cores), me // cores

    def landed(ref, sem):
        pltpu.make_async_copy(ref, ref, sem).wait()

    def slot(member):
        return lax.rem(member, cores) * chips + member // cores

    small = [
        pltpu.make_async_copy(source, place, small_sem.at[i])
        for i, (source, place) in enumerate(
            [
                (sensors_in, gathered.at[1, slot(me)]), (readings_in, readings), (noises_in, noises),
                (lists_in.at[pl.ds(pl.multiple_of(me * domains, 8), domains)], lists),
                (tiers_in, tiers),
            ]
        )
    ]
    for copy in small:
        copy.start()

    def peer(k):
        other = lax.rem(me + space * n + k, peers)
        return {"member": lax.rem(other, n), "space": other // n}

    barrier = pltpu.get_barrier_semaphore()

    def greet(k, carry):
        pl.semaphore_signal(barrier, inc=1, device_id=peer(k), device_id_type=MESH)
        return carry

    lax.fori_loop(1, peers, greet, 0)
    small[0].wait()

    lane = lax.broadcasted_iota(jnp.int32, (obs_count, width), 1)

    def mark(group, carry):
        start = pl.multiple_of(group * 8, 8)
        columns = jnp.transpose(lists[pl.ds(start, 8), :] - me * domains)
        found = []
        for d in range(8):
            hit = columns[:, d : d + 1] == lane
            found.append(jnp.sum(jnp.where(hit, 1.0, 0.0), axis=0, keepdims=True))
        marks[pl.ds(start, 8), :] = jnp.concatenate(found, axis=0)
        return carry

    with jax.named_scope("w_barrier"):
        pl.semaphore_wait(barrier, peers - 1)

    has_left, has_right = space > 0, space < spaces - 1

    def to_space(side):
        return lax.rem(space + 1 - side + spaces, spaces)

    def chip_copy(j):
        place = gathered.at[1, slot(me)]
        other = partner(chip, j, chips) * cores + core
        return pltpu.make_async_remote_copy(
            place, place, chip_send.at[0], chip_recv.at[0],
            device_id={"member": other}, device_id_type=MESH,
        )

    singles = [(left_readings, left_noises), (readings, noises), (right_readings, right_noises)]

    def near_copies(side):
        index = side // 2
        return [
            pltpu.make_async_remote_copy(
                source, place, near_send.at[index, i], near_recv.at[index, i],
                device_id={"space": to_space(side)}, device_id_type=MESH,
            )
            for i, (source, place) in enumerate(zip((readings_in, noises_in), singles[side]))
        ]

    def side_copy(side, t):
        rows = pl.ds(core * chips, chips)
        return pltpu.make_async_remote_copy(
            gathered.at[1, rows], gathered.at[side, rows],
            side_send.at[side], side_recv.at[side],
            device_id={"member": chip * cores + lax.rem(core + t, cores), "space": to_space(side)},
            device_id_type=MESH,
        )

    for j in range(1, chips):
        chip_copy(j).start()

    @pl.when(has_right)
    def _():
        for copy in near_copies(0):
            copy.start()

    @pl.when(has_left)
    def _():
        for copy in near_copies(2):
            copy.start()

    def in_views(to, g):
        return (
            x.at[:, pl.ds(pl.multiple_of(to * domains + g * CHUNK, 16), CHUNK), :],
            incoming.at[pl.ds(me * members, members), pl.ds(g * CHUNK, CHUNK), :],
        )

    def in_copy(g, k):
        to = partner(me, k, n)
        source, place = in_views(to, g)
        return pltpu.make_async_remote_copy(
            source, place, in_send.at[0], in_recv.at[g],
            device_id={"member": to}, device_id_type=MESH,
        )

    far = list(range(n // 2, n))
    close = list(range(1, n // 2))
    far_first = far + close
    middle = (me >= n // 2 - cores) & (me < n // 2 + cores)
    pairs = [(g, k) for g in range(chunks) for k in far_first]
    middle_early = [(0, k) for k in far_first]
    outer_early = [(g, k) for g in range(chunks) for k in close]

    @pl.when(middle)
    def _():
        for g, k in middle_early:
            in_copy(g, k).start()

    @pl.when(jnp.logical_not(middle))
    def _():
        for g, k in outer_early:
            in_copy(g, k).start()

    for g in range(chunks):
        source, place = in_views(me, g)
        pltpu.make_async_copy(source, place, in_recv.at[g]).start()

    for side, missing in ((0, space == 0), (2, space == spaces - 1)):
        @pl.when(missing)
        def _():
            gathered[side] = jnp.ones(gathered.shape[1:], BF16)
            for single in singles[side]:
                single[...] = jnp.ones(single.shape, BF16)

    for copy in small[1:]:
        copy.wait()
    with jax.named_scope("marks"):
        lax.fori_loop(0, domains // 8, mark, 0)

    with jax.named_scope("w_chip"):
        if chips > 1:
            others = gathered.at[1, pl.ds(0, chips - 1)]
            landed(others, chip_send.at[0])
            landed(others, chip_recv.at[0])

    for t in range(1, cores):
        side_copy(1, t).start()

    @pl.when(has_right)
    def _():
        for t in range(cores):
            side_copy(0, t).start()

    @pl.when(has_left)
    def _():
        for t in range(cores):
            side_copy(2, t).start()

    with jax.named_scope("w_side"):
        if cores > 1:
            others = gathered.at[1, pl.ds(0, n - chips)]
            landed(others, side_send.at[1])
            landed(others, side_recv.at[1])

        @pl.when(has_right)
        def _():
            for copy in near_copies(0):
                copy.wait_send()
            for copy in near_copies(2):
                copy.wait_recv()
            landed(gathered.at[1], side_send.at[0])
            landed(gathered.at[2], side_recv.at[2])

        @pl.when(has_left)
        def _():
            for copy in near_copies(2):
                copy.wait_send()
            for copy in near_copies(0):
                copy.wait_recv()
            landed(gathered.at[1], side_send.at[2])
            landed(gathered.at[0], side_recv.at[0])

    for side in range(3):
        for s in range(n):
            full[members * s : members * (s + 1), patch * side : patch * (side + 1)] = (
                gathered[side, s % cores * chips + s // cores].astype(F32)
            )
        for i, single in enumerate(singles[side]):
            full[lines + i : lines + i + 1, patch * side : patch * (side + 1)] = (
                single[...].astype(F32)[None]
            )
    total = 3 * patch
    shift = lax.rem(2 * total - (patch - halo) - me * domains, total)
    turned = pltpu.roll(full[...], shift, 1)[:, :width]
    values = turned[:lines]
    mean = jnp.sum(values, axis=0, keepdims=True) * (1.0 / lines)
    anomaly = values - mean
    anoms[...] = anomaly
    innov = turned[lines : lines + 1] - mean
    noise = turned[lines + 1 : lines + 2]
    squares = jnp.sum(anomaly * anomaly, axis=0, keepdims=True)

    own_tier = lax.broadcasted_iota(jnp.int32, (domains, patch), 1) == (
        lax.broadcasted_iota(jnp.int32, (domains, patch), 0) + me * domains
    )
    tier = jnp.sum(jnp.where(own_tier, tiers[...].astype(F32)[None], 0.0), axis=1, keepdims=True)
    radius = (tier + 2.0) * (0.5 * obs_count)
    place = lax.broadcasted_iota(jnp.int32, (domains, width), 1)
    row = lax.broadcasted_iota(jnp.int32, (domains, width), 0)
    distance = jnp.abs(place - halo - row).astype(F32) / radius
    weight = marks[...] * jnp.exp(-2.0 * distance * distance) / noise
    weights[...] = weight
    fit = jnp.sum(weight * (innov * innov))
    spread = jnp.sum(weight * squares)
    first = lax.broadcasted_iota(jnp.int32, (1, LANES), 1) == 0
    moved[...] = jnp.where(first, fit, spread)

    high, low = split(anomaly)
    pad = jnp.zeros((LANES - lines, width), F32)
    anoms_t[...] = jnp.concatenate(
        [
            jnp.transpose(jnp.concatenate([high.astype(F32), pad], axis=0)),
            jnp.transpose(jnp.concatenate([low.astype(F32), pad], axis=0)),
        ],
        axis=1,
    ).astype(BF16)

    def sum_copy(k):
        return pltpu.make_async_remote_copy(
            moved, sums.at[k], sum_send.at[0], sum_recv.at[0],
            device_id=peer(k), device_id_type=MESH,
        )

    def start_sum(k, carry):
        sum_copy(k).start()
        return carry

    def add_sum(k, carry):
        return carry + sums[k]

    lax.fori_loop(1, peers, start_sum, 0)

    @pl.when(middle)
    def _():
        for g, k in pairs:
            if (g, k) not in middle_early:
                in_copy(g, k).start()

    hi, lo = split(weight * innov)
    aims = jnp.dot(jnp.concatenate([hi, lo], axis=0), anoms_t[...], preferred_element_type=F32)
    target[...] = aims[:domains, :LANES] + aims[:domains, LANES:] + aims[domains:, :LANES]

    def gram_group(g, carry):
        for d in range(2):
            c = g * 2 + d
            hi, lo = split(anoms[...] * weights[pl.ds(c, 1), :])
            prod = jnp.dot(
                jnp.concatenate([hi, lo], axis=0), anoms_t[...], preferred_element_type=F32
            )
            gram[c] = prod[:lines, :LANES] + prod[:lines, LANES:] + prod[lines:, :LANES]
        return carry

    with jax.named_scope('gram'):
        lax.fori_loop(0, domains // 2, gram_group, 0)

    with jax.named_scope("w_sums"):
        if peers > 1:
            others = sums.at[pl.ds(1, peers - 1)]
            landed(others, sum_send.at[0])
            landed(others, sum_recv.at[0])
        sums_all = lax.fori_loop(1, peers, add_sum, moved[...])

    @pl.when(jnp.logical_not(middle))
    def _():
        for g, k in pairs:
            if (g, k) not in outer_early:
                in_copy(g, k).start()

    scale = sums_all[:, 1:2] / sums_all[:, 0:1]
    eye = jnp.where(
        lax.broadcasted_iota(jnp.int32, (lines, LANES), 0)
        == lax.broadcasted_iota(jnp.int32, (lines, LANES), 1),
        1.0, 0.0,
    )
    diagonal = eye * scale

    def solve_group(g, carry):
        ids = [g * GROUP + d for d in range(GROUP)]
        mats = [gram[c] + diagonal for c in ids]
        bounds = [
            jnp.max(jnp.sum(jnp.abs(m), axis=0, keepdims=True), axis=1, keepdims=True)
            for m in mats
        ]
        ys = [m / b for m, b in zip(mats, bounds)]
        zs = [1.5 * eye - 0.5 * y for y in ys]
        ys = [times(y, z) for y, z in zip(ys, zs)]
        for step in range(1, NS_STEPS):
            ps = [1.5 * eye - 0.5 * times(z, y) for z, y in zip(zs, ys)]
            if step < NS_STEPS - 1:
                both = [
                    times(jnp.concatenate([y, z], axis=0), p) for y, z, p in zip(ys, zs, ps)
                ]
                ys = [b[:lines] for b in both]
                zs = [b[lines:] for b in both]
            else:
                zs = [times(z, p) for z, p in zip(zs, ps)]
        roots = [z * lax.rsqrt(b) for z, b in zip(zs, bounds)]
        for c, root in zip(ids, roots):
            half_gain = jnp.sum(root * target[pl.ds(c, 1), :], axis=1, keepdims=True)
            gain = jnp.sum(root * half_gain, axis=0, keepdims=True)
            w = (lines - 1.0) ** 0.5 * root + gain
            w = w - jnp.sum(w, axis=1, keepdims=True) * (1.0 / lines) + 1.0 / lines
            trans[c] = w.astype(BF16)
        return carry

    def out_views(to, g):
        return (
            updated.at[pl.ds(to * members, members), pl.ds(g * CHUNK, CHUNK), :],
            out.at[:, pl.ds(pl.multiple_of(me * domains + g * CHUNK, 16), CHUNK), :],
        )

    def out_copy(g, k):
        to = partner(me, k, n)
        source, place = out_views(to, g)
        return pltpu.make_async_remote_copy(
            source, place, out_send.at[0], out_recv.at[0],
            device_id={"member": to}, device_id_type=MESH,
        )

    for g in range(chunks):
        with jax.named_scope(f'solve{g}'):
            lax.fori_loop(g * CHUNK // GROUP, (g + 1) * CHUNK // GROUP, solve_group, 0)
        with jax.named_scope(f'w_in{g}'):
            landed(incoming.at[:, pl.ds(g * CHUNK, CHUNK), :], in_recv.at[g])
        states = jnp.swapaxes(incoming[:, g * CHUNK : (g + 1) * CHUNK, :].astype(F32), 0, 1)
        states = states.astype(BF16)
        results = [
            jnp.dot(trans[g * CHUNK + c][:, :lines], states[c], preferred_element_type=F32)
            for c in range(CHUNK)
        ]
        results = jnp.stack(results, axis=0)
        updated[:, g * CHUNK : (g + 1) * CHUNK, :] = jnp.swapaxes(results, 0, 1).astype(BF16)
        for k in far_first:
            out_copy(g, k).start()
        source, place = out_views(me, g)
        pltpu.make_async_copy(source, place, out_recv.at[0]).start()

    with jax.named_scope("w_out"):
        if n > 1:
            landed(x.at[:, pl.ds(0, patch - domains), :], in_send.at[0])
            landed(updated.at[pl.ds(0, lines - members)], out_send.at[0])
        landed(out, out_recv.at[0])


def per_device(trials, sensors, readings, noises, lists, tiers):
    n, spaces = lax.axis_size("member"), lax.axis_size("space")
    members, patch, quantities = trials.shape
    obs_count = lists.shape[1]
    halo = 5 * obs_count // 2
    domains = patch // n
    chunks = domains // CHUNK
    lines = members * n
    width = -(-(domains + 2 * halo) // 256) * 256
    vmem = pl.BlockSpec(memory_space=pltpu.VMEM)
    anywhere = pl.BlockSpec(memory_space=pltpu.HBM)
    full_rows = -(-(lines + 2) // 8) * 8
    dma = pltpu.SemaphoreType.DMA
    return pl.pallas_call(
        functools.partial(analyse_kernel, n, spaces, halo, obs_count),
        out_shape=pltpu.VMEM((members, patch, quantities), BF16),
        in_specs=[anywhere] * 6,
        out_specs=vmem,
        scratch_shapes=[
            pltpu.VMEM((patch,), BF16),
            pltpu.VMEM((patch,), BF16),
            pltpu.VMEM((patch,), BF16),
            pltpu.VMEM((patch,), BF16),
            pltpu.VMEM((patch,), BF16),
            pltpu.VMEM((patch,), BF16),
            pltpu.VMEM((domains, obs_count), jnp.int32),
            pltpu.VMEM((patch,), jnp.int32),
            dma((5,)),
            pltpu.VMEM((lines, domains, quantities), BF16),
            pltpu.VMEM((lines, domains, quantities), BF16),
            pltpu.VMEM((3, n, members, patch), BF16),
            pltpu.VMEM((full_rows, 3 * patch), F32),
            pltpu.VMEM((lines, width), F32),
            pltpu.VMEM((width, 2 * LANES), BF16),
            pltpu.VMEM((domains, width), F32),
            pltpu.VMEM((domains, width), F32),
            pltpu.VMEM((domains, lines, LANES), F32),
            pltpu.VMEM((domains, LANES), F32),
            pltpu.VMEM((domains, lines, LANES), BF16),
            pltpu.VMEM((1, LANES), F32),
            pltpu.VMEM((n * spaces, 1, LANES), F32),
            dma((1,)), dma((chunks,)), dma((1,)), dma((1,)),
            dma((2, 2)), dma((2, 2)), dma((1,)), dma((1,)), dma((3,)), dma((3,)), dma((1,)), dma((1,)),
        ],
        compiler_params=pltpu.CompilerParams(
            collective_id=0, has_side_effects=True, vmem_limit_bytes=40 << 20
        ),
        name="analyse",
    )(*[pltpu.with_memory_space_constraint(a, pltpu.HBM) for a in (trials, sensors, readings, noises, lists, tiers)])


def solution(mesh):
    return jax.shard_map(
        per_device,
        mesh=mesh,
        in_specs=(
            P("member", ("region", "space"), None),
            P("member", ("region", "space")),
            P(("region", "space")),
            P(("region", "space")),
            P(("region", "space"), None),
            P(("region", "space")),
        ),
        out_specs=P("member", ("region", "space"), None),
        check_vma=False,
    )
```

```python
import functools

import jax
import jax.numpy as jnp
from jax import lax
from jax.experimental import pallas as pl
from jax.experimental.pallas import tpu as pltpu
from jax.sharding import PartitionSpec as P

NS_STEPS = 4
LANES = 128
GROUP = 4
CHUNK = 16
MESH = pl.DeviceIdType.MESH
F32 = jnp.float32
BF16 = jnp.bfloat16


def partner(me, k, n):
    if n & (n - 1):
        return lax.rem(me + k, n)
    other, bit = me, 1
    while bit < n:
        if k & bit:
            other = other + bit * (1 - 2 * lax.rem(me // bit, 2))
        bit *= 2
    return other


def split(value):
    high = value.astype(BF16)
    return high, (value - high.astype(F32)).astype(BF16)


def times(left, right):
    lh, ll = split(left)
    rh, rl = split(right)
    rows, k = left.shape[0], right.shape[0]
    lhs = jnp.concatenate([lh, ll], axis=0)[:, :k]
    rhs = jnp.concatenate([rh, rl], axis=1)
    out = jnp.dot(lhs, rhs, preferred_element_type=F32)
    width = right.shape[1]
    return out[:rows, :width] + out[:rows, width:] + out[rows:, :width]


def analyse_kernel(
    n, spaces, halo, obs_count, x, sensors_in, readings_in, noises_in, lists_in, tiers_in,
    out,
    entered, readings, noises, left_readings, left_noises, right_readings, right_noises, lists, tiers, small_sem, incoming, updated, gathered, full, anoms, anoms_t, marks, weights, gram, target, trans,
    moved, sums,
    in_send, in_recv, out_send, out_recv, near_send, near_recv, chip_send, chip_recv, side_send, side_recv, sum_send, sum_recv,
):
    me = lax.axis_index("member")
    space = lax.axis_index("space")
    members, patch, _ = x.shape
    domains = patch // n
    lines = members * n
    width = anoms.shape[1]
    chunks = domains // CHUNK
    peers = n * spaces
    cores = 2 - n % 2
    chips = n // cores
    core, chip = lax.rem(me, cores), me // cores

    def landed(ref, sem):
        pltpu.make_async_copy(ref, ref, sem).wait()

    def slot(member):
        return lax.rem(member, cores) * chips + member // cores

    staged = n > 2 * cores and n & (n - 1) == 0
    low = n // 2 - cores if staged else n
    span = 2 * cores

    def central(member):
        return (member >= low) & (member < low + span)

    middle = central(me)
    outer = jnp.logical_not(middle)
    barrier = pltpu.get_barrier_semaphore()

    def peer(k):
        other = lax.rem(me + space * n + k, peers)
        return {"member": lax.rem(other, n), "space": other // n}

    @pl.when(middle)
    def _():
        for k in range(1, span):
            other = low + lax.rem(me - low + k, span)
            pl.semaphore_signal(barrier, inc=1, device_id={"member": other}, device_id_type=MESH)

    small = [
        pltpu.make_async_copy(source, place, small_sem.at[i])
        for i, (source, place) in enumerate(
            [
                (sensors_in, gathered.at[1, slot(me)]), (readings_in, readings), (noises_in, noises),
                (lists_in.at[pl.ds(pl.multiple_of(me * domains, 8), domains)], lists),
                (tiers_in, tiers),
            ]
        )
    ]
    for copy in small:
        copy.start()

    def greet(k, carry):
        other = peer(k)

        @pl.when(jnp.logical_not(central(other["member"])))
        def _():
            pl.semaphore_signal(barrier, inc=1, device_id=other, device_id_type=MESH)

        return carry

    lax.fori_loop(1, peers, greet, 0)
    lane = lax.broadcasted_iota(jnp.int32, (obs_count, width), 1)

    def mark(group, carry):
        start = pl.multiple_of(group * 8, 8)
        columns = jnp.transpose(lists[pl.ds(start, 8), :] - me * domains)
        found = []
        for d in range(8):
            hit = columns[:, d : d + 1] == lane
            found.append(jnp.sum(jnp.where(hit, 1.0, 0.0), axis=0, keepdims=True))
        marks[pl.ds(start, 8), :] = jnp.concatenate(found, axis=0)
        return carry

    def marking(first, last):
        with jax.named_scope("marks"):
            lax.fori_loop(first, last, mark, 0)

    has_left, has_right = space > 0, space < spaces - 1

    def to_space(side):
        return lax.rem(space + 1 - side + spaces, spaces)

    def chip_copy(j):
        place = gathered.at[1, slot(me)]
        other = partner(chip, j, chips) * cores + core
        return pltpu.make_async_remote_copy(
            place, place, chip_send.at[0], chip_recv.at[0],
            device_id={"member": other}, device_id_type=MESH,
        )

    singles = [(left_readings, left_noises), (readings, noises), (right_readings, right_noises)]

    def near_copies(side):
        index = side // 2
        return [
            pltpu.make_async_remote_copy(
                source, place, near_send.at[index, i], near_recv.at[index, i],
                device_id={"space": to_space(side)}, device_id_type=MESH,
            )
            for i, (source, place) in enumerate(zip((readings_in, noises_in), singles[side]))
        ]

    def side_copy(side, t):
        rows = pl.ds(core * chips, chips)
        return pltpu.make_async_remote_copy(
            gathered.at[1, rows], gathered.at[side, rows],
            side_send.at[side], side_recv.at[side],
            device_id={"member": chip * cores + lax.rem(core + t, cores), "space": to_space(side)},
            device_id_type=MESH,
        )

    def in_views(to, g):
        return (
            x.at[:, pl.ds(pl.multiple_of(to * domains + g * CHUNK, 16), CHUNK), :],
            incoming.at[pl.ds(me * members, members), pl.ds(g * CHUNK, CHUNK), :],
        )

    def in_copy(g, k):
        to = partner(me, k, n)
        source, place = in_views(to, g)
        return pltpu.make_async_remote_copy(
            source, place, in_send.at[0], in_recv.at[g],
            device_id={"member": to}, device_id_type=MESH,
        )

    far = list(range(n // 2, n))
    close = list(range(1, n // 2))
    far_first = far + close
    pairs = [(g, k) for g in range(chunks) for k in far_first]
    first_pairs = [(0, k) for k in reversed(range(n - cores, n))]
    middle_early = first_pairs + [(0, k) for k in far_first if k < n - cores]
    middle_early += [(1, k) for k in range(n - cores, n) if chunks > 1]
    outer_early = [(g, k) for g in range(chunks) for k in close]
    half = domains // 16

    def start_near():
        @pl.when(has_right)
        def _():
            for copy in near_copies(0):
                copy.start()

        @pl.when(has_left)
        def _():
            for copy in near_copies(2):
                copy.start()

    def start_own():
        for g in range(chunks):
            source, place = in_views(me, g)
            pltpu.make_async_copy(source, place, in_recv.at[g]).start()

    @pl.when(middle)
    def _():
        small[0].wait()
        with jax.named_scope("w_middle"):
            pl.semaphore_wait(barrier, span - 1)
        if staged:
            chip_copy(chips - 1).start()
        for g, k in first_pairs:
            in_copy(g, k).start()
        start_own()
        for copy in small[1:]:
            copy.wait()
        marking(0, half)
        with jax.named_scope("w_entered"):
            pl.semaphore_wait(entered, 1)
        for j in range(1, chips - 1):
            chip_copy(j).start()
        start_near()
        for g, k in middle_early[len(first_pairs):]:
            in_copy(g, k).start()

    @pl.when(outer)
    def _():
        with jax.named_scope("w_barrier"):
            pl.semaphore_wait(barrier, peers - 1)
        if staged:
            @pl.when((me >= low + span) & (me < low + span + cores))
            def _():
                for j in range(1, 3):
                    pl.semaphore_signal(
                        entered, inc=1, device_id={"member": me - j * cores}, device_id_type=MESH
                    )
        small[0].wait()
        for j in range(1, chips):
            chip_copy(j).start()
        start_near()
        for g, k in outer_early:
            in_copy(g, k).start()
        start_own()
        for copy in small[1:]:
            copy.wait()
        marking(0, half)

    for side, missing in ((0, space == 0), (2, space == spaces - 1)):
        @pl.when(missing)
        def _():
            gathered[side] = jnp.ones(gathered.shape[1:], BF16)
            for single in singles[side]:
                single[...] = jnp.ones(single.shape, BF16)

    marking(half, domains // 8)

    with jax.named_scope("w_chip"):
        if chips > 1:
            others = gathered.at[1, pl.ds(0, chips - 1)]
            landed(others, chip_send.at[0])
            landed(others, chip_recv.at[0])

    for t in range(1, cores):
        side_copy(1, t).start()

    @pl.when(has_right)
    def _():
        for t in range(cores):
            side_copy(0, t).start()

    @pl.when(has_left)
    def _():
        for t in range(cores):
            side_copy(2, t).start()

    with jax.named_scope("w_side"):
        if cores > 1:
            others = gathered.at[1, pl.ds(0, n - chips)]
            landed(others, side_send.at[1])
            landed(others, side_recv.at[1])

        @pl.when(has_right)
        def _():
            for copy in near_copies(0):
                copy.wait_send()
            for copy in near_copies(2):
                copy.wait_recv()
            landed(gathered.at[1], side_send.at[0])
            landed(gathered.at[2], side_recv.at[2])

        @pl.when(has_left)
        def _():
            for copy in near_copies(2):
                copy.wait_send()
            for copy in near_copies(0):
                copy.wait_recv()
            landed(gathered.at[1], side_send.at[2])
            landed(gathered.at[0], side_recv.at[0])

    for side in range(3):
        for s in range(n):
            full[members * s : members * (s + 1), patch * side : patch * (side + 1)] = (
                gathered[side, s % cores * chips + s // cores].astype(F32)
            )
        for i, single in enumerate(singles[side]):
            full[lines + i : lines + i + 1, patch * side : patch * (side + 1)] = (
                single[...].astype(F32)[None]
            )
    total = 3 * patch
    shift = lax.rem(2 * total - (patch - halo) - me * domains, total)
    turned = pltpu.roll(full[...], shift, 1)[:, :width]
    values = turned[:lines]
    mean = jnp.sum(values, axis=0, keepdims=True) * (1.0 / lines)
    anomaly = values - mean
    anoms[...] = anomaly
    innov = turned[lines : lines + 1] - mean
    noise = turned[lines + 1 : lines + 2]
    squares = jnp.sum(anomaly * anomaly, axis=0, keepdims=True)

    own_tier = lax.broadcasted_iota(jnp.int32, (domains, patch), 1) == (
        lax.broadcasted_iota(jnp.int32, (domains, patch), 0) + me * domains
    )
    tier = jnp.sum(jnp.where(own_tier, tiers[...].astype(F32)[None], 0.0), axis=1, keepdims=True)
    radius = (tier + 2.0) * (0.5 * obs_count)
    place = lax.broadcasted_iota(jnp.int32, (domains, width), 1)
    row = lax.broadcasted_iota(jnp.int32, (domains, width), 0)
    distance = jnp.abs(place - halo - row).astype(F32) / radius
    weight = marks[...] * jnp.exp(-2.0 * distance * distance) / noise
    weights[...] = weight
    fit = jnp.sum(weight * (innov * innov))
    spread = jnp.sum(weight * squares)
    first = lax.broadcasted_iota(jnp.int32, (1, LANES), 1) == 0
    moved[...] = jnp.where(first, fit, spread)

    high, low = split(anomaly)
    pad = jnp.zeros((LANES - lines, width), F32)
    anoms_t[...] = jnp.concatenate(
        [
            jnp.transpose(jnp.concatenate([high.astype(F32), pad], axis=0)),
            jnp.transpose(jnp.concatenate([low.astype(F32), pad], axis=0)),
        ],
        axis=1,
    ).astype(BF16)

    def sum_copy(k):
        return pltpu.make_async_remote_copy(
            moved, sums.at[k], sum_send.at[0], sum_recv.at[0],
            device_id=peer(k), device_id_type=MESH,
        )

    def start_sum(k, carry):
        sum_copy(k).start()
        return carry

    def add_sum(k, carry):
        return carry + sums[k]

    lax.fori_loop(1, peers, start_sum, 0)

    @pl.when(middle)
    def _():
        for g, k in pairs:
            if (g, k) not in middle_early:
                in_copy(g, k).start()

    hi, lo = split(weight * innov)
    aims = jnp.dot(jnp.concatenate([hi, lo], axis=0), anoms_t[...], preferred_element_type=F32)
    target[...] = aims[:domains, :LANES] + aims[:domains, LANES:] + aims[domains:, :LANES]

    def gram_group(g, carry):
        for d in range(2):
            c = g * 2 + d
            hi, lo = split(anoms[...] * weights[pl.ds(c, 1), :])
            prod = jnp.dot(
                jnp.concatenate([hi, lo], axis=0), anoms_t[...], preferred_element_type=F32
            )
            gram[c] = prod[:lines, :LANES] + prod[:lines, LANES:] + prod[lines:, :LANES]
        return carry

    with jax.named_scope('gram'):
        lax.fori_loop(0, domains // 2, gram_group, 0)

    with jax.named_scope("w_sums"):
        if peers > 1:
            others = sums.at[pl.ds(1, peers - 1)]
            landed(others, sum_send.at[0])
            landed(others, sum_recv.at[0])
        sums_all = lax.fori_loop(1, peers, add_sum, moved[...])

    @pl.when(outer)
    def _():
        for g, k in pairs:
            if (g, k) not in outer_early:
                in_copy(g, k).start()

    scale = sums_all[:, 1:2] / sums_all[:, 0:1]
    eye = jnp.where(
        lax.broadcasted_iota(jnp.int32, (lines, LANES), 0)
        == lax.broadcasted_iota(jnp.int32, (lines, LANES), 1),
        1.0, 0.0,
    )
    diagonal = eye * scale

    def solve_group(g, carry):
        ids = [g * GROUP + d for d in range(GROUP)]
        mats = [gram[c] + diagonal for c in ids]
        bounds = [
            jnp.max(jnp.sum(jnp.abs(m), axis=0, keepdims=True), axis=1, keepdims=True)
            for m in mats
        ]
        ys = [m / b for m, b in zip(mats, bounds)]
        zs = [1.5 * eye - 0.5 * y for y in ys]
        ys = [times(y, z) for y, z in zip(ys, zs)]
        for step in range(1, NS_STEPS):
            ps = [1.5 * eye - 0.5 * times(z, y) for z, y in zip(zs, ys)]
            if step < NS_STEPS - 1:
                both = [
                    times(jnp.concatenate([y, z], axis=0), p) for y, z, p in zip(ys, zs, ps)
                ]
                ys = [b[:lines] for b in both]
                zs = [b[lines:] for b in both]
            else:
                zs = [times(z, p) for z, p in zip(zs, ps)]
        roots = [z * lax.rsqrt(b) for z, b in zip(zs, bounds)]
        for c, root in zip(ids, roots):
            half_gain = jnp.sum(root * target[pl.ds(c, 1), :], axis=1, keepdims=True)
            gain = jnp.sum(root * half_gain, axis=0, keepdims=True)
            w = (lines - 1.0) ** 0.5 * root + gain
            w = w - jnp.sum(w, axis=1, keepdims=True) * (1.0 / lines) + 1.0 / lines
            trans[c] = w.astype(BF16)
        return carry

    def out_views(to, g):
        return (
            updated.at[pl.ds(to * members, members), pl.ds(g * CHUNK, CHUNK), :],
            out.at[:, pl.ds(pl.multiple_of(me * domains + g * CHUNK, 16), CHUNK), :],
        )

    def out_copy(g, k):
        to = partner(me, k, n)
        source, place = out_views(to, g)
        return pltpu.make_async_remote_copy(
            source, place, out_send.at[0], out_recv.at[0],
            device_id={"member": to}, device_id_type=MESH,
        )

    for g in range(chunks):
        with jax.named_scope(f'solve{g}'):
            lax.fori_loop(g * CHUNK // GROUP, (g + 1) * CHUNK // GROUP, solve_group, 0)
        with jax.named_scope(f'w_in{g}'):
            landed(incoming.at[:, pl.ds(g * CHUNK, CHUNK), :], in_recv.at[g])
        states = jnp.swapaxes(incoming[:, g * CHUNK : (g + 1) * CHUNK, :].astype(F32), 0, 1)
        states = states.astype(BF16)
        results = [
            jnp.dot(trans[g * CHUNK + c][:, :lines], states[c], preferred_element_type=F32)
            for c in range(CHUNK)
        ]
        results = jnp.stack(results, axis=0)
        updated[:, g * CHUNK : (g + 1) * CHUNK, :] = jnp.swapaxes(results, 0, 1).astype(BF16)
        for k in far_first:
            out_copy(g, k).start()
        source, place = out_views(me, g)
        pltpu.make_async_copy(source, place, out_recv.at[0]).start()

    with jax.named_scope("w_out"):
        if n > 1:
            landed(x.at[:, pl.ds(0, patch - domains), :], in_send.at[0])
            landed(updated.at[pl.ds(0, lines - members)], out_send.at[0])
        landed(out, out_recv.at[0])


def per_device(trials, sensors, readings, noises, lists, tiers):
    n, spaces = lax.axis_size("member"), lax.axis_size("space")
    members, patch, quantities = trials.shape
    obs_count = lists.shape[1]
    halo = 5 * obs_count // 2
    domains = patch // n
    chunks = domains // CHUNK
    lines = members * n
    width = -(-(domains + 2 * halo) // 256) * 256
    vmem = pl.BlockSpec(memory_space=pltpu.VMEM)
    anywhere = pl.BlockSpec(memory_space=pltpu.HBM)
    full_rows = -(-(lines + 2) // 8) * 8
    dma = pltpu.SemaphoreType.DMA
    return pl.pallas_call(
        functools.partial(analyse_kernel, n, spaces, halo, obs_count),
        out_shape=pltpu.VMEM((members, patch, quantities), BF16),
        in_specs=[anywhere] * 6,
        out_specs=vmem,
        scratch_shapes=[
            pltpu.SemaphoreType.REGULAR,
            pltpu.VMEM((patch,), BF16),
            pltpu.VMEM((patch,), BF16),
            pltpu.VMEM((patch,), BF16),
            pltpu.VMEM((patch,), BF16),
            pltpu.VMEM((patch,), BF16),
            pltpu.VMEM((patch,), BF16),
            pltpu.VMEM((domains, obs_count), jnp.int32),
            pltpu.VMEM((patch,), jnp.int32),
            dma((5,)),
            pltpu.VMEM((lines, domains, quantities), BF16),
            pltpu.VMEM((lines, domains, quantities), BF16),
            pltpu.VMEM((3, n, members, patch), BF16),
            pltpu.VMEM((full_rows, 3 * patch), F32),
            pltpu.VMEM((lines, width), F32),
            pltpu.VMEM((width, 2 * LANES), BF16),
            pltpu.VMEM((domains, width), F32),
            pltpu.VMEM((domains, width), F32),
            pltpu.VMEM((domains, lines, LANES), F32),
            pltpu.VMEM((domains, LANES), F32),
            pltpu.VMEM((domains, lines, LANES), BF16),
            pltpu.VMEM((1, LANES), F32),
            pltpu.VMEM((n * spaces, 1, LANES), F32),
            dma((1,)), dma((chunks,)), dma((1,)), dma((1,)),
            dma((2, 2)), dma((2, 2)), dma((1,)), dma((1,)), dma((3,)), dma((3,)), dma((1,)), dma((1,)),
        ],
        compiler_params=pltpu.CompilerParams(
            collective_id=0, has_side_effects=True, vmem_limit_bytes=40 << 20
        ),
        name="analyse",
    )(*[pltpu.with_memory_space_constraint(a, pltpu.HBM) for a in (trials, sensors, readings, noises, lists, tiers)])


def solution(mesh):
    return jax.shard_map(
        per_device,
        mesh=mesh,
        in_specs=(
            P("member", ("region", "space"), None),
            P("member", ("region", "space")),
            P(("region", "space")),
            P(("region", "space")),
            P(("region", "space"), None),
            P(("region", "space")),
        ),
        out_specs=P("member", ("region", "space"), None),
        check_vma=False,
    )
```

```python
import functools

import jax
import jax.numpy as jnp
from jax import lax
from jax.experimental import pallas as pl
from jax.experimental.pallas import tpu as pltpu
from jax.sharding import PartitionSpec as P

NS_STEPS = 4
LANES = 128
GROUP = 4
CHUNK = 16
MESH = pl.DeviceIdType.MESH
F32 = jnp.float32
BF16 = jnp.bfloat16


def partner(me, k, n):
    if n & (n - 1):
        return lax.rem(me + k, n)
    other, bit = me, 1
    while bit < n:
        if k & bit:
            other = other + bit * (1 - 2 * lax.rem(me // bit, 2))
        bit *= 2
    return other


def split(value):
    high = value.astype(BF16)
    return high, (value - high.astype(F32)).astype(BF16)


def times(left, right):
    lh, ll = split(left)
    rh, rl = split(right)
    rows, k = left.shape[0], right.shape[0]
    lhs = jnp.concatenate([lh, ll], axis=0)[:, :k]
    rhs = jnp.concatenate([rh, rl], axis=1)
    out = jnp.dot(lhs, rhs, preferred_element_type=F32)
    width = right.shape[1]
    return out[:rows, :width] + out[:rows, width:] + out[rows:, :width]


def analyse_kernel(
    n, spaces, halo, obs_count, x, sensors_in, readings_in, noises_in, lists_in, tiers_in,
    out,
    entered, readings, noises, left_readings, left_noises, right_readings, right_noises, lists, tiers, small_sem, stage_sem, stage, incoming, updated, gathered, full, anoms, anoms_t, marks, weights, gram, target, trans,
    moved, sums,
    in_send, in_recv, out_send, out_recv, near_send, near_recv, chip_send, chip_recv, side_send, side_recv, sum_send, sum_recv,
):
    me = lax.axis_index("member")
    space = lax.axis_index("space")
    members, patch, _ = x.shape
    domains = patch // n
    lines = members * n
    width = anoms.shape[1]
    chunks = domains // CHUNK
    peers = n * spaces
    cores = 2 - n % 2
    chips = n // cores
    core, chip = lax.rem(me, cores), me // cores

    def landed(ref, sem):
        pltpu.make_async_copy(ref, ref, sem).wait()

    def slot(member):
        return lax.rem(member, cores) * chips + member // cores

    staged = n > 2 * cores and n & (n - 1) == 0
    low = n // 2 - cores if staged else n
    span = 2 * cores

    def central(member):
        return (member >= low) & (member < low + span)

    def in_views(to, g):
        return (
            x.at[:, pl.ds(pl.multiple_of(to * domains + g * CHUNK, 16), CHUNK), :],
            incoming.at[pl.ds(me * members, members), pl.ds(g * CHUNK, CHUNK), :],
        )

    middle = central(me)
    outer = jnp.logical_not(middle)
    barrier = pltpu.get_barrier_semaphore()

    def peer(k):
        other = lax.rem(me + space * n + k, peers)
        return {"member": lax.rem(other, n), "space": other // n}

    @pl.when(middle)
    def _():
        for k in range(1, span):
            other = low + lax.rem(me - low + k, span)
            pl.semaphore_signal(barrier, inc=1, device_id={"member": other}, device_id_type=MESH)
        for i in range(cores):
            source, _ = in_views(partner(me, n - 1 - i, n), 0)
            pltpu.make_async_copy(source, stage.at[i], stage_sem.at[0]).start()

    half_chips = chips // 2
    upper = chip >= half_chips

    small = [
        pltpu.make_async_copy(source, place, small_sem.at[i])
        for i, (source, place) in enumerate(
            [
                (sensors_in, gathered.at[1, slot(me)]), (readings_in, readings), (noises_in, noises),
                (lists_in.at[pl.ds(pl.multiple_of(me * domains, 8), domains)], lists),
                (tiers_in, tiers),
            ]
        )
    ]
    for copy in small:
        copy.start()

    def greet(k, carry):
        other = peer(k)

        @pl.when(jnp.logical_not(central(other["member"])))
        def _():
            pl.semaphore_signal(barrier, inc=1, device_id=other, device_id_type=MESH)

        return carry

    lax.fori_loop(1, peers, greet, 0)
    lane = lax.broadcasted_iota(jnp.int32, (obs_count, width), 1)

    def mark(group, carry):
        start = pl.multiple_of(group * 8, 8)
        columns = jnp.transpose(lists[pl.ds(start, 8), :] - me * domains)
        found = []
        for d in range(8):
            hit = columns[:, d : d + 1] == lane
            found.append(jnp.sum(jnp.where(hit, 1.0, 0.0), axis=0, keepdims=True))
        marks[pl.ds(start, 8), :] = jnp.concatenate(found, axis=0)
        return carry

    def marking(first, last):
        with jax.named_scope("marks"):
            lax.fori_loop(first, last, mark, 0)

    has_left, has_right = space > 0, space < spaces - 1

    def to_space(side):
        return lax.rem(space + 1 - side + spaces, spaces)

    def slot_copy(other, half):
        place = gathered.at[1, slot(me)]
        return pltpu.make_async_remote_copy(
            place, place, chip_send.at[0], chip_recv.at[half],
            device_id={"member": other * cores + core}, device_id_type=MESH,
        )

    def near_slots():
        for j in range(1, half_chips if staged else chips):
            slot_copy(partner(chip, j, chips), 0).start()

    def cross_slot():
        if staged:
            slot_copy(half_chips - upper.astype(jnp.int32), 1).start()

    def relay_copy(j):
        rows = pl.ds(core * chips + (1 - upper.astype(jnp.int32)) * half_chips, half_chips)
        return pltpu.make_async_remote_copy(
            gathered.at[1, rows], gathered.at[1, rows], chip_send.at[j], chip_recv.at[1],
            device_id={"member": partner(chip, j, chips) * cores + core}, device_id_type=MESH,
        )

    singles = [(left_readings, left_noises), (readings, noises), (right_readings, right_noises)]

    def near_copies(side):
        index = side // 2
        return [
            pltpu.make_async_remote_copy(
                source, place, near_send.at[index, i], near_recv.at[index, i],
                device_id={"space": to_space(side)}, device_id_type=MESH,
            )
            for i, (source, place) in enumerate(zip((readings_in, noises_in), singles[side]))
        ]

    def side_copy(side, t):
        rows = pl.ds(core * chips, chips)
        return pltpu.make_async_remote_copy(
            gathered.at[1, rows], gathered.at[side, rows],
            side_send.at[side], side_recv.at[side],
            device_id={"member": chip * cores + lax.rem(core + t, cores), "space": to_space(side)},
            device_id_type=MESH,
        )

    def in_copy(g, k, copied=None):
        to = partner(me, k, n)
        source, place = in_views(to, g)
        source = source if copied is None else copied
        return pltpu.make_async_remote_copy(
            source, place, in_send.at[0], in_recv.at[g],
            device_id={"member": to}, device_id_type=MESH,
        )

    far = list(range(n // 2, n))
    close = list(range(1, n // 2))
    far_first = far + close
    pairs = [(g, k) for g in range(chunks) for k in far_first]
    first_pairs = [(0, k) for k in reversed(range(n - cores, n))]
    opposite = [(g, k) for g in range(1, chunks) for k in range(n - cores, n)]
    relayed = [(0, k) for k in close]
    middle_early = first_pairs + opposite + relayed
    outer_early = [(g, k) for g in range(chunks) for k in close]
    half = domains // 16

    def start_near():
        @pl.when(has_right)
        def _():
            for copy in near_copies(0):
                copy.start()

        @pl.when(has_left)
        def _():
            for copy in near_copies(2):
                copy.start()

    def start_own():
        for g in range(chunks):
            source, place = in_views(me, g)
            pltpu.make_async_copy(source, place, in_recv.at[g]).start()

    @pl.when(middle)
    def _():
        with jax.named_scope("w_middle"):
            pl.semaphore_wait(barrier, span - 1)
        with jax.named_scope("w_stage"):
            landed(stage, stage_sem.at[0])
        for i, (g, k) in enumerate(first_pairs):
            in_copy(g, k, stage.at[i]).start()
            if i == 0:
                small[0].wait()
                cross_slot()
        start_own()
        for copy in small[1:]:
            copy.wait()
        marking(0, half)
        with jax.named_scope("w_entered"):
            pl.semaphore_wait(entered, 1)
        near_slots()
        start_near()
        for g, k in opposite:
            in_copy(g, k).start()

    @pl.when(outer)
    def _():
        with jax.named_scope("w_barrier"):
            pl.semaphore_wait(barrier, peers - 1)
        if staged:
            @pl.when((me >= low + span) & (me < low + span + cores))
            def _():
                for j in range(1, 3):
                    pl.semaphore_signal(
                        entered, inc=1, device_id={"member": me - j * cores}, device_id_type=MESH
                    )
        small[0].wait()
        cross_slot()
        near_slots()
        start_near()
        for g, k in outer_early:
            in_copy(g, k).start()
        start_own()
        for copy in small[1:]:
            copy.wait()
        marking(0, half)

    for side, missing in ((0, space == 0), (2, space == spaces - 1)):
        @pl.when(missing)
        def _():
            gathered[side] = jnp.ones(gathered.shape[1:], BF16)
            for single in singles[side]:
                single[...] = jnp.ones(single.shape, BF16)

    marking(half, domains // 8)

    with jax.named_scope("w_chip"):
        if staged:
            landed(gathered.at[1, pl.ds(0, half_chips)], chip_recv.at[1])

            @pl.when(middle)
            def _():
                for j in range(1, half_chips):
                    relay_copy(j).start()
                for g, k in relayed:
                    in_copy(g, k).start()
        near = half_chips - 1 if staged else chips - 1
        if near:
            landed(gathered.at[1, pl.ds(0, near)], chip_recv.at[0])

    for t in range(1, cores):
        side_copy(1, t).start()

    @pl.when(has_right)
    def _():
        for t in range(cores):
            side_copy(0, t).start()

    @pl.when(has_left)
    def _():
        for t in range(cores):
            side_copy(2, t).start()

    with jax.named_scope("w_side"):
        sent = half_chips if staged else chips - 1
        if sent:
            landed(gathered.at[1, pl.ds(0, sent)], chip_send.at[0])
        if staged:
            @pl.when(middle)
            def _():
                for j in range(1, half_chips):
                    relay_copy(j).wait_send()
        if cores > 1:
            others = gathered.at[1, pl.ds(0, n - chips)]
            landed(others, side_send.at[1])
            landed(others, side_recv.at[1])

        @pl.when(has_right)
        def _():
            for copy in near_copies(0):
                copy.wait_send()
            for copy in near_copies(2):
                copy.wait_recv()
            landed(gathered.at[1], side_send.at[0])
            landed(gathered.at[2], side_recv.at[2])

        @pl.when(has_left)
        def _():
            for copy in near_copies(2):
                copy.wait_send()
            for copy in near_copies(0):
                copy.wait_recv()
            landed(gathered.at[1], side_send.at[2])
            landed(gathered.at[0], side_recv.at[0])

    for side in range(3):
        for s in range(n):
            full[members * s : members * (s + 1), patch * side : patch * (side + 1)] = (
                gathered[side, s % cores * chips + s // cores].astype(F32)
            )
        for i, single in enumerate(singles[side]):
            full[lines + i : lines + i + 1, patch * side : patch * (side + 1)] = (
                single[...].astype(F32)[None]
            )
    total = 3 * patch
    shift = lax.rem(2 * total - (patch - halo) - me * domains, total)
    turned = pltpu.roll(full[...], shift, 1)[:, :width]
    values = turned[:lines]
    mean = jnp.sum(values, axis=0, keepdims=True) * (1.0 / lines)
    anomaly = values - mean
    anoms[...] = anomaly
    innov = turned[lines : lines + 1] - mean
    noise = turned[lines + 1 : lines + 2]
    squares = jnp.sum(anomaly * anomaly, axis=0, keepdims=True)

    own_tier = lax.broadcasted_iota(jnp.int32, (domains, patch), 1) == (
        lax.broadcasted_iota(jnp.int32, (domains, patch), 0) + me * domains
    )
    tier = jnp.sum(jnp.where(own_tier, tiers[...].astype(F32)[None], 0.0), axis=1, keepdims=True)
    radius = (tier + 2.0) * (0.5 * obs_count)
    place = lax.broadcasted_iota(jnp.int32, (domains, width), 1)
    row = lax.broadcasted_iota(jnp.int32, (domains, width), 0)
    distance = jnp.abs(place - halo - row).astype(F32) / radius
    weight = marks[...] * jnp.exp(-2.0 * distance * distance) / noise
    weights[...] = weight
    fit = jnp.sum(weight * (innov * innov))
    spread = jnp.sum(weight * squares)
    first = lax.broadcasted_iota(jnp.int32, (1, LANES), 1) == 0
    moved[...] = jnp.where(first, fit, spread)

    high, low = split(anomaly)
    pad = jnp.zeros((LANES - lines, width), F32)
    anoms_t[...] = jnp.concatenate(
        [
            jnp.transpose(jnp.concatenate([high.astype(F32), pad], axis=0)),
            jnp.transpose(jnp.concatenate([low.astype(F32), pad], axis=0)),
        ],
        axis=1,
    ).astype(BF16)

    def sum_copy(k):
        return pltpu.make_async_remote_copy(
            moved, sums.at[k], sum_send.at[0], sum_recv.at[0],
            device_id=peer(k), device_id_type=MESH,
        )

    def start_sum(k, carry):
        sum_copy(k).start()
        return carry

    def add_sum(k, carry):
        return carry + sums[k]

    lax.fori_loop(1, peers, start_sum, 0)

    @pl.when(middle)
    def _():
        for g, k in pairs:
            if (g, k) not in middle_early:
                in_copy(g, k).start()

    hi, lo = split(weight * innov)
    aims = jnp.dot(jnp.concatenate([hi, lo], axis=0), anoms_t[...], preferred_element_type=F32)
    target[...] = aims[:domains, :LANES] + aims[:domains, LANES:] + aims[domains:, :LANES]

    def gram_group(g, carry):
        for d in range(2):
            c = g * 2 + d
            hi, lo = split(anoms[...] * weights[pl.ds(c, 1), :])
            prod = jnp.dot(
                jnp.concatenate([hi, lo], axis=0), anoms_t[...], preferred_element_type=F32
            )
            gram[c] = prod[:lines, :LANES] + prod[:lines, LANES:] + prod[lines:, :LANES]
        return carry

    with jax.named_scope('gram'):
        lax.fori_loop(0, domains // 2, gram_group, 0)

    with jax.named_scope("w_sums"):
        if peers > 1:
            others = sums.at[pl.ds(1, peers - 1)]
            landed(others, sum_send.at[0])
            landed(others, sum_recv.at[0])
        sums_all = lax.fori_loop(1, peers, add_sum, moved[...])

    @pl.when(outer)
    def _():
        for g, k in pairs:
            if (g, k) not in outer_early:
                in_copy(g, k).start()

    scale = sums_all[:, 1:2] / sums_all[:, 0:1]
    eye = jnp.where(
        lax.broadcasted_iota(jnp.int32, (lines, LANES), 0)
        == lax.broadcasted_iota(jnp.int32, (lines, LANES), 1),
        1.0, 0.0,
    )
    diagonal = eye * scale

    def solve_group(g, carry):
        ids = [g * GROUP + d for d in range(GROUP)]
        mats = [gram[c] + diagonal for c in ids]
        bounds = [
            jnp.max(jnp.sum(jnp.abs(m), axis=0, keepdims=True), axis=1, keepdims=True)
            for m in mats
        ]
        ys = [m / b for m, b in zip(mats, bounds)]
        zs = [1.5 * eye - 0.5 * y for y in ys]
        ys = [times(y, z) for y, z in zip(ys, zs)]
        for step in range(1, NS_STEPS):
            ps = [1.5 * eye - 0.5 * times(z, y) for z, y in zip(zs, ys)]
            if step < NS_STEPS - 1:
                both = [
                    times(jnp.concatenate([y, z], axis=0), p) for y, z, p in zip(ys, zs, ps)
                ]
                ys = [b[:lines] for b in both]
                zs = [b[lines:] for b in both]
            else:
                zs = [times(z, p) for z, p in zip(zs, ps)]
        roots = [z * lax.rsqrt(b) for z, b in zip(zs, bounds)]
        for c, root in zip(ids, roots):
            half_gain = jnp.sum(root * target[pl.ds(c, 1), :], axis=1, keepdims=True)
            gain = jnp.sum(root * half_gain, axis=0, keepdims=True)
            w = (lines - 1.0) ** 0.5 * root + gain
            w = w - jnp.sum(w, axis=1, keepdims=True) * (1.0 / lines) + 1.0 / lines
            trans[c] = w.astype(BF16)
        return carry

    def out_views(to, g):
        return (
            updated.at[pl.ds(to * members, members), pl.ds(g * CHUNK, CHUNK), :],
            out.at[:, pl.ds(pl.multiple_of(me * domains + g * CHUNK, 16), CHUNK), :],
        )

    def out_copy(g, k):
        to = partner(me, k, n)
        source, place = out_views(to, g)
        return pltpu.make_async_remote_copy(
            source, place, out_send.at[0], out_recv.at[0],
            device_id={"member": to}, device_id_type=MESH,
        )

    for g in range(chunks):
        with jax.named_scope(f'solve{g}'):
            lax.fori_loop(g * CHUNK // GROUP, (g + 1) * CHUNK // GROUP, solve_group, 0)
        with jax.named_scope(f'w_in{g}'):
            landed(incoming.at[:, pl.ds(g * CHUNK, CHUNK), :], in_recv.at[g])
        states = jnp.swapaxes(incoming[:, g * CHUNK : (g + 1) * CHUNK, :].astype(F32), 0, 1)
        states = states.astype(BF16)
        results = [
            jnp.dot(trans[g * CHUNK + c][:, :lines], states[c], preferred_element_type=F32)
            for c in range(CHUNK)
        ]
        results = jnp.stack(results, axis=0)
        updated[:, g * CHUNK : (g + 1) * CHUNK, :] = jnp.swapaxes(results, 0, 1).astype(BF16)
        for k in far_first:
            out_copy(g, k).start()
        source, place = out_views(me, g)
        pltpu.make_async_copy(source, place, out_recv.at[0]).start()

    with jax.named_scope("w_out"):
        if n > 1:
            landed(x.at[:, pl.ds(0, patch - domains), :], in_send.at[0])
            landed(updated.at[pl.ds(0, lines - members)], out_send.at[0])
        landed(out, out_recv.at[0])


def per_device(trials, sensors, readings, noises, lists, tiers):
    n, spaces = lax.axis_size("member"), lax.axis_size("space")
    members, patch, quantities = trials.shape
    obs_count = lists.shape[1]
    halo = 5 * obs_count // 2
    domains = patch // n
    chunks = domains // CHUNK
    lines = members * n
    width = -(-(domains + 2 * halo) // 256) * 256
    vmem = pl.BlockSpec(memory_space=pltpu.VMEM)
    anywhere = pl.BlockSpec(memory_space=pltpu.HBM)
    full_rows = -(-(lines + 2) // 8) * 8
    dma = pltpu.SemaphoreType.DMA
    return pl.pallas_call(
        functools.partial(analyse_kernel, n, spaces, halo, obs_count),
        out_shape=pltpu.VMEM((members, patch, quantities), BF16),
        in_specs=[anywhere] * 6,
        out_specs=vmem,
        scratch_shapes=[
            pltpu.SemaphoreType.REGULAR,
            pltpu.VMEM((patch,), BF16),
            pltpu.VMEM((patch,), BF16),
            pltpu.VMEM((patch,), BF16),
            pltpu.VMEM((patch,), BF16),
            pltpu.VMEM((patch,), BF16),
            pltpu.VMEM((patch,), BF16),
            pltpu.VMEM((domains, obs_count), jnp.int32),
            pltpu.VMEM((patch,), jnp.int32),
            dma((5,)), dma((1,)),
            pltpu.VMEM((2 - n % 2, members, CHUNK, quantities), BF16),
            pltpu.VMEM((lines, domains, quantities), BF16),
            pltpu.VMEM((lines, domains, quantities), BF16),
            pltpu.VMEM((3, n, members, patch), BF16),
            pltpu.VMEM((full_rows, 3 * patch), F32),
            pltpu.VMEM((lines, width), F32),
            pltpu.VMEM((width, 2 * LANES), BF16),
            pltpu.VMEM((domains, width), F32),
            pltpu.VMEM((domains, width), F32),
            pltpu.VMEM((domains, lines, LANES), F32),
            pltpu.VMEM((domains, LANES), F32),
            pltpu.VMEM((domains, lines, LANES), BF16),
            pltpu.VMEM((1, LANES), F32),
            pltpu.VMEM((n * spaces, 1, LANES), F32),
            dma((1,)), dma((chunks,)), dma((1,)), dma((1,)),
            dma((2, 2)), dma((2, 2)), dma((max(n // 4, 1),)), dma((2,)), dma((3,)), dma((3,)), dma((1,)), dma((1,)),
        ],
        compiler_params=pltpu.CompilerParams(
            collective_id=0, has_side_effects=True, vmem_limit_bytes=40 << 20
        ),
        name="analyse",
    )(*[pltpu.with_memory_space_constraint(a, pltpu.HBM) for a in (trials, sensors, readings, noises, lists, tiers)])


def solution(mesh):
    return jax.shard_map(
        per_device,
        mesh=mesh,
        in_specs=(
            P("member", ("region", "space"), None),
            P("member", ("region", "space")),
            P(("region", "space")),
            P(("region", "space")),
            P(("region", "space"), None),
            P(("region", "space")),
        ),
        out_specs=P("member", ("region", "space"), None),
        check_vma=False,
    )
```

```python
import functools

import jax
import jax.numpy as jnp
from jax import lax
from jax.experimental import pallas as pl
from jax.experimental.pallas import tpu as pltpu
from jax.sharding import PartitionSpec as P

NS_STEPS = 4
LANES = 128
GROUP = 4
CHUNK = 16
MESH = pl.DeviceIdType.MESH
F32 = jnp.float32
BF16 = jnp.bfloat16


def partner(me, k, n):
    if n & (n - 1):
        return lax.rem(me + k, n)
    other, bit = me, 1
    while bit < n:
        if k & bit:
            other = other + bit * (1 - 2 * lax.rem(me // bit, 2))
        bit *= 2
    return other


def split(value):
    high = value.astype(BF16)
    return high, (value - high.astype(F32)).astype(BF16)


def times(left, right):
    lh, ll = split(left)
    rh, rl = split(right)
    rows, k = left.shape[0], right.shape[0]
    lhs = jnp.concatenate([lh, ll], axis=0)[:, :k]
    rhs = jnp.concatenate([rh, rl], axis=1)
    out = jnp.dot(lhs, rhs, preferred_element_type=F32)
    width = right.shape[1]
    return out[:rows, :width] + out[:rows, width:] + out[rows:, :width]


def analyse_kernel(
    n, spaces, halo, obs_count, x, sensors_in, readings_in, noises_in, lists_in, tiers_in,
    out,
    entered, readings, noises, left_readings, left_noises, right_readings, right_noises, lists, tiers, small_sem, stage_sem, stage, incoming, updated, gathered, full, anoms, anoms_t, marks, weights, gram, target, trans,
    moved, sums,
    in_send, in_recv, out_send, out_recv, near_send, near_recv, chip_send, chip_recv, side_send, side_recv, sum_send, sum_recv,
):
    me = lax.axis_index("member")
    space = lax.axis_index("space")
    members, patch, _ = x.shape
    domains = patch // n
    lines = members * n
    width = anoms.shape[1]
    chunks = domains // CHUNK
    peers = n * spaces
    cores = 2 - n % 2
    chips = n // cores
    core, chip = lax.rem(me, cores), me // cores

    def landed(ref, sem):
        pltpu.make_async_copy(ref, ref, sem).wait()

    def slot(member):
        return lax.rem(member, cores) * chips + member // cores

    staged = n > 2 * cores and n & (n - 1) == 0
    low = n // 2 - cores if staged else n
    span = 2 * cores

    def central(member):
        return (member >= low) & (member < low + span)

    def in_views(to, g):
        return (
            x.at[:, pl.ds(pl.multiple_of(to * domains + g * CHUNK, 16), CHUNK), :],
            incoming.at[pl.ds(me * members, members), pl.ds(g * CHUNK, CHUNK), :],
        )

    middle = central(me)
    outer = jnp.logical_not(middle)
    barrier = pltpu.get_barrier_semaphore()

    def peer(k):
        other = lax.rem(me + space * n + k, peers)
        return {"member": lax.rem(other, n), "space": other // n}

    @pl.when(middle)
    def _():
        other = partner(me, n - cores, n)
        pl.semaphore_signal(barrier, inc=1, device_id={"member": other}, device_id_type=MESH)
        source, _ = in_views(other, 0)
        pltpu.make_async_copy(source, stage, stage_sem.at[0]).start()

    half_chips = chips // 2
    upper = chip >= half_chips

    small = [
        pltpu.make_async_copy(source, place, small_sem.at[i])
        for i, (source, place) in enumerate(
            [
                (sensors_in, gathered.at[1, slot(me)]), (readings_in, readings), (noises_in, noises),
                (lists_in.at[pl.ds(pl.multiple_of(me * domains, 8), domains)], lists),
                (tiers_in, tiers),
            ]
        )
    ]
    for copy in small:
        copy.start()

    def greet(k, carry):
        other = peer(k)

        @pl.when(jnp.logical_not(central(other["member"])))
        def _():
            pl.semaphore_signal(barrier, inc=1, device_id=other, device_id_type=MESH)

        return carry

    lax.fori_loop(1, peers, greet, 0)
    lane = lax.broadcasted_iota(jnp.int32, (obs_count, width), 1)

    def mark(group, carry):
        start = pl.multiple_of(group * 8, 8)
        columns = jnp.transpose(lists[pl.ds(start, 8), :] - me * domains)
        found = []
        for d in range(8):
            hit = columns[:, d : d + 1] == lane
            found.append(jnp.sum(jnp.where(hit, 1.0, 0.0), axis=0, keepdims=True))
        marks[pl.ds(start, 8), :] = jnp.concatenate(found, axis=0)
        return carry

    def marking(first, last):
        with jax.named_scope("marks"):
            lax.fori_loop(first, last, mark, 0)

    has_left, has_right = space > 0, space < spaces - 1

    def to_space(side):
        return lax.rem(space + 1 - side + spaces, spaces)

    def slot_copy(other, half):
        place = gathered.at[1, slot(me)]
        return pltpu.make_async_remote_copy(
            place, place, chip_send.at[0], chip_recv.at[half],
            device_id={"member": other * cores + core}, device_id_type=MESH,
        )

    def near_slots():
        for j in range(1, half_chips if staged else chips):
            slot_copy(partner(chip, j, chips), 0).start()

    def cross_slot():
        if staged:
            slot_copy(half_chips - upper.astype(jnp.int32), 1).start()

    def relay_copy(j):
        rows = pl.ds(core * chips + (1 - upper.astype(jnp.int32)) * half_chips, half_chips)
        return pltpu.make_async_remote_copy(
            gathered.at[1, rows], gathered.at[1, rows], chip_send.at[j], chip_recv.at[1],
            device_id={"member": partner(chip, j, chips) * cores + core}, device_id_type=MESH,
        )

    singles = [(left_readings, left_noises), (readings, noises), (right_readings, right_noises)]

    def near_copies(side):
        index = side // 2
        return [
            pltpu.make_async_remote_copy(
                source, place, near_send.at[index, i], near_recv.at[index, i],
                device_id={"space": to_space(side)}, device_id_type=MESH,
            )
            for i, (source, place) in enumerate(zip((readings_in, noises_in), singles[side]))
        ]

    def side_copy(side, t):
        rows = pl.ds(core * chips, chips)
        return pltpu.make_async_remote_copy(
            gathered.at[1, rows], gathered.at[side, rows],
            side_send.at[side], side_recv.at[side],
            device_id={"member": chip * cores + lax.rem(core + t, cores), "space": to_space(side)},
            device_id_type=MESH,
        )

    def in_copy(g, k, copied=None):
        to = partner(me, k, n)
        source, place = in_views(to, g)
        source = source if copied is None else copied
        return pltpu.make_async_remote_copy(
            source, place, in_send.at[0], in_recv.at[g],
            device_id={"member": to}, device_id_type=MESH,
        )

    far = list(range(n // 2, n))
    close = list(range(1, n // 2))
    far_first = far + close
    pairs = [(g, k) for g in range(chunks) for k in far_first]
    facing = [(g, n - cores) for g in range(chunks)]
    crossed = [(g, k) for g in range(chunks) for k in range(n - cores + 1, n)]
    relayed = [(0, k) for k in close]
    middle_early = facing + crossed + relayed
    outer_early = [(g, k) for g in range(chunks) for k in close]
    half = domains // 16

    def start_near():
        @pl.when(has_right)
        def _():
            for copy in near_copies(0):
                copy.start()

        @pl.when(has_left)
        def _():
            for copy in near_copies(2):
                copy.start()

    def start_own():
        for g in range(chunks):
            source, place = in_views(me, g)
            pltpu.make_async_copy(source, place, in_recv.at[g]).start()

    @pl.when(middle)
    def _():
        with jax.named_scope("w_middle"):
            pl.semaphore_wait(barrier, 1)
        with jax.named_scope("w_stage"):
            landed(stage, stage_sem.at[0])
        in_copy(*facing[0], stage).start()
        small[0].wait()
        cross_slot()
        for g, k in facing[1:]:
            in_copy(g, k).start()
        start_own()
        for copy in small[1:]:
            copy.wait()
        marking(0, half)
        with jax.named_scope("w_entered"):
            pl.semaphore_wait(entered, 1)
        near_slots()
        start_near()
        for g, k in crossed:
            in_copy(g, k).start()

    @pl.when(outer)
    def _():
        with jax.named_scope("w_barrier"):
            pl.semaphore_wait(barrier, peers - 1)
        if staged:
            @pl.when((me >= low + span) & (me < low + span + cores))
            def _():
                for j in range(1, 3):
                    pl.semaphore_signal(
                        entered, inc=1, device_id={"member": me - j * cores}, device_id_type=MESH
                    )
        small[0].wait()
        cross_slot()
        near_slots()
        start_near()
        for g, k in outer_early:
            in_copy(g, k).start()
        start_own()
        for copy in small[1:]:
            copy.wait()
        marking(0, half)

    for side, missing in ((0, space == 0), (2, space == spaces - 1)):
        @pl.when(missing)
        def _():
            gathered[side] = jnp.ones(gathered.shape[1:], BF16)
            for single in singles[side]:
                single[...] = jnp.ones(single.shape, BF16)

    marking(half, domains // 8)

    with jax.named_scope("w_chip"):
        if staged:
            landed(gathered.at[1, pl.ds(0, half_chips)], chip_recv.at[1])

            @pl.when(middle)
            def _():
                for j in range(1, half_chips):
                    relay_copy(j).start()
                for g, k in relayed:
                    in_copy(g, k).start()
        near = half_chips - 1 if staged else chips - 1
        if near:
            landed(gathered.at[1, pl.ds(0, near)], chip_recv.at[0])

    for t in range(1, cores):
        side_copy(1, t).start()

    @pl.when(has_right)
    def _():
        for t in range(cores):
            side_copy(0, t).start()

    @pl.when(has_left)
    def _():
        for t in range(cores):
            side_copy(2, t).start()

    with jax.named_scope("w_side"):
        sent = half_chips if staged else chips - 1
        if sent:
            landed(gathered.at[1, pl.ds(0, sent)], chip_send.at[0])
        if staged:
            @pl.when(middle)
            def _():
                for j in range(1, half_chips):
                    relay_copy(j).wait_send()
        if cores > 1:
            others = gathered.at[1, pl.ds(0, n - chips)]
            landed(others, side_send.at[1])
            landed(others, side_recv.at[1])

        @pl.when(has_right)
        def _():
            for copy in near_copies(0):
                copy.wait_send()
            for copy in near_copies(2):
                copy.wait_recv()
            landed(gathered.at[1], side_send.at[0])
            landed(gathered.at[2], side_recv.at[2])

        @pl.when(has_left)
        def _():
            for copy in near_copies(2):
                copy.wait_send()
            for copy in near_copies(0):
                copy.wait_recv()
            landed(gathered.at[1], side_send.at[2])
            landed(gathered.at[0], side_recv.at[0])

    for side in range(3):
        for s in range(n):
            full[members * s : members * (s + 1), patch * side : patch * (side + 1)] = (
                gathered[side, s % cores * chips + s // cores].astype(F32)
            )
        for i, single in enumerate(singles[side]):
            full[lines + i : lines + i + 1, patch * side : patch * (side + 1)] = (
                single[...].astype(F32)[None]
            )
    total = 3 * patch
    shift = lax.rem(2 * total - (patch - halo) - me * domains, total)
    turned = pltpu.roll(full[...], shift, 1)[:, :width]
    values = turned[:lines]
    mean = jnp.sum(values, axis=0, keepdims=True) * (1.0 / lines)
    anomaly = values - mean
    anoms[...] = anomaly
    innov = turned[lines : lines + 1] - mean
    noise = turned[lines + 1 : lines + 2]
    squares = jnp.sum(anomaly * anomaly, axis=0, keepdims=True)

    own_tier = lax.broadcasted_iota(jnp.int32, (domains, patch), 1) == (
        lax.broadcasted_iota(jnp.int32, (domains, patch), 0) + me * domains
    )
    tier = jnp.sum(jnp.where(own_tier, tiers[...].astype(F32)[None], 0.0), axis=1, keepdims=True)
    radius = (tier + 2.0) * (0.5 * obs_count)
    place = lax.broadcasted_iota(jnp.int32, (domains, width), 1)
    row = lax.broadcasted_iota(jnp.int32, (domains, width), 0)
    distance = jnp.abs(place - halo - row).astype(F32) / radius
    weight = marks[...] * jnp.exp(-2.0 * distance * distance) / noise
    weights[...] = weight
    fit = jnp.sum(weight * (innov * innov))
    spread = jnp.sum(weight * squares)
    first = lax.broadcasted_iota(jnp.int32, (1, LANES), 1) == 0
    moved[...] = jnp.where(first, fit, spread)

    high, low = split(anomaly)
    pad = jnp.zeros((LANES - lines, width), F32)
    anoms_t[...] = jnp.concatenate(
        [
            jnp.transpose(jnp.concatenate([high.astype(F32), pad], axis=0)),
            jnp.transpose(jnp.concatenate([low.astype(F32), pad], axis=0)),
        ],
        axis=1,
    ).astype(BF16)

    def sum_copy(k):
        return pltpu.make_async_remote_copy(
            moved, sums.at[k], sum_send.at[0], sum_recv.at[0],
            device_id=peer(k), device_id_type=MESH,
        )

    def start_sum(k, carry):
        sum_copy(k).start()
        return carry

    def add_sum(k, carry):
        return carry + sums[k]

    lax.fori_loop(1, peers, start_sum, 0)

    @pl.when(middle)
    def _():
        for g, k in pairs:
            if (g, k) not in middle_early:
                in_copy(g, k).start()

    hi, lo = split(weight * innov)
    aims = jnp.dot(jnp.concatenate([hi, lo], axis=0), anoms_t[...], preferred_element_type=F32)
    target[...] = aims[:domains, :LANES] + aims[:domains, LANES:] + aims[domains:, :LANES]

    def gram_group(g, carry):
        for d in range(2):
            c = g * 2 + d
            hi, lo = split(anoms[...] * weights[pl.ds(c, 1), :])
            prod = jnp.dot(
                jnp.concatenate([hi, lo], axis=0), anoms_t[...], preferred_element_type=F32
            )
            gram[c] = prod[:lines, :LANES] + prod[:lines, LANES:] + prod[lines:, :LANES]
        return carry

    with jax.named_scope("gram"):
        lax.fori_loop(0, domains // 4, gram_group, 0)

    @pl.when(outer)
    def _():
        for g, k in pairs:
            if (g, k) not in outer_early:
                in_copy(g, k).start()

    with jax.named_scope("gram"):
        lax.fori_loop(domains // 4, domains // 2, gram_group, 0)

    with jax.named_scope("w_sums"):
        if peers > 1:
            others = sums.at[pl.ds(1, peers - 1)]
            landed(others, sum_send.at[0])
            landed(others, sum_recv.at[0])
        sums_all = lax.fori_loop(1, peers, add_sum, moved[...])

    scale = sums_all[:, 1:2] / sums_all[:, 0:1]
    eye = jnp.where(
        lax.broadcasted_iota(jnp.int32, (lines, LANES), 0)
        == lax.broadcasted_iota(jnp.int32, (lines, LANES), 1),
        1.0, 0.0,
    )
    diagonal = eye * scale

    def solve_group(g, carry):
        ids = [g * GROUP + d for d in range(GROUP)]
        mats = [gram[c] + diagonal for c in ids]
        bounds = [
            jnp.max(jnp.sum(jnp.abs(m), axis=0, keepdims=True), axis=1, keepdims=True)
            for m in mats
        ]
        ys = [m / b for m, b in zip(mats, bounds)]
        zs = [1.5 * eye - 0.5 * y for y in ys]
        ys = [times(y, z) for y, z in zip(ys, zs)]
        for step in range(1, NS_STEPS):
            ps = [1.5 * eye - 0.5 * times(z, y) for z, y in zip(zs, ys)]
            if step < NS_STEPS - 1:
                both = [
                    times(jnp.concatenate([y, z], axis=0), p) for y, z, p in zip(ys, zs, ps)
                ]
                ys = [b[:lines] for b in both]
                zs = [b[lines:] for b in both]
            else:
                zs = [times(z, p) for z, p in zip(zs, ps)]
        roots = [z * lax.rsqrt(b) for z, b in zip(zs, bounds)]
        for c, root in zip(ids, roots):
            half_gain = jnp.sum(root * target[pl.ds(c, 1), :], axis=1, keepdims=True)
            gain = jnp.sum(root * half_gain, axis=0, keepdims=True)
            w = (lines - 1.0) ** 0.5 * root + gain
            w = w - jnp.sum(w, axis=1, keepdims=True) * (1.0 / lines) + 1.0 / lines
            trans[c] = w.astype(BF16)
        return carry

    if staged:
        beyond = list(range(half_chips, chips)) + list(range(1, half_chips))
        receivers = [
            partner(chip, j, chips) * cores + c for j in beyond for c in reversed(range(cores))
        ] + [chip * cores + lax.rem(core + t, cores) for t in range(1, cores)]
    else:
        receivers = [partner(me, k, n) for k in far_first]

    def out_views(to, g):
        return (
            updated.at[pl.ds(to * members, members), pl.ds(g * CHUNK, CHUNK), :],
            out.at[:, pl.ds(pl.multiple_of(me * domains + g * CHUNK, 16), CHUNK), :],
        )

    def out_copy(g, to):
        source, place = out_views(to, g)
        return pltpu.make_async_remote_copy(
            source, place, out_send.at[0], out_recv.at[0],
            device_id={"member": to}, device_id_type=MESH,
        )

    for g in range(chunks):
        with jax.named_scope(f'solve{g}'):
            lax.fori_loop(g * CHUNK // GROUP, (g + 1) * CHUNK // GROUP, solve_group, 0)
        with jax.named_scope(f'w_in{g}'):
            landed(incoming.at[:, pl.ds(g * CHUNK, CHUNK), :], in_recv.at[g])
        states = jnp.swapaxes(incoming[:, g * CHUNK : (g + 1) * CHUNK, :].astype(F32), 0, 1)
        states = states.astype(BF16)
        results = [
            jnp.dot(trans[g * CHUNK + c][:, :lines], states[c], preferred_element_type=F32)
            for c in range(CHUNK)
        ]
        results = jnp.stack(results, axis=0)
        updated[:, g * CHUNK : (g + 1) * CHUNK, :] = jnp.swapaxes(results, 0, 1).astype(BF16)
        for to in receivers:
            out_copy(g, to).start()
        source, place = out_views(me, g)
        pltpu.make_async_copy(source, place, out_recv.at[0]).start()

    with jax.named_scope("w_out"):
        landed(out, out_recv.at[0])
    with jax.named_scope("w_sent"):
        if n > 1:
            landed(x.at[:, pl.ds(0, patch - domains), :], in_send.at[0])
            landed(updated.at[pl.ds(0, lines - members)], out_send.at[0])


def per_device(trials, sensors, readings, noises, lists, tiers):
    n, spaces = lax.axis_size("member"), lax.axis_size("space")
    members, patch, quantities = trials.shape
    obs_count = lists.shape[1]
    halo = 5 * obs_count // 2
    domains = patch // n
    chunks = domains // CHUNK
    lines = members * n
    width = -(-(domains + 2 * halo) // 256) * 256
    vmem = pl.BlockSpec(memory_space=pltpu.VMEM)
    anywhere = pl.BlockSpec(memory_space=pltpu.HBM)
    full_rows = -(-(lines + 2) // 8) * 8
    dma = pltpu.SemaphoreType.DMA
    return pl.pallas_call(
        functools.partial(analyse_kernel, n, spaces, halo, obs_count),
        out_shape=pltpu.VMEM((members, patch, quantities), BF16),
        in_specs=[anywhere] * 6,
        out_specs=vmem,
        scratch_shapes=[
            pltpu.SemaphoreType.REGULAR,
            pltpu.VMEM((patch,), BF16),
            pltpu.VMEM((patch,), BF16),
            pltpu.VMEM((patch,), BF16),
            pltpu.VMEM((patch,), BF16),
            pltpu.VMEM((patch,), BF16),
            pltpu.VMEM((patch,), BF16),
            pltpu.VMEM((domains, obs_count), jnp.int32),
            pltpu.VMEM((patch,), jnp.int32),
            dma((5,)), dma((1,)),
            pltpu.VMEM((members, CHUNK, quantities), BF16),
            pltpu.VMEM((lines, domains, quantities), BF16),
            pltpu.VMEM((lines, domains, quantities), BF16),
            pltpu.VMEM((3, n, members, patch), BF16),
            pltpu.VMEM((full_rows, 3 * patch), F32),
            pltpu.VMEM((lines, width), F32),
            pltpu.VMEM((width, 2 * LANES), BF16),
            pltpu.VMEM((domains, width), F32),
            pltpu.VMEM((domains, width), F32),
            pltpu.VMEM((domains, lines, LANES), F32),
            pltpu.VMEM((domains, LANES), F32),
            pltpu.VMEM((domains, lines, LANES), BF16),
            pltpu.VMEM((1, LANES), F32),
            pltpu.VMEM((n * spaces, 1, LANES), F32),
            dma((1,)), dma((chunks,)), dma((1,)), dma((1,)),
            dma((2, 2)), dma((2, 2)), dma((max(n // 4, 1),)), dma((2,)), dma((3,)), dma((3,)), dma((1,)), dma((1,)),
        ],
        compiler_params=pltpu.CompilerParams(
            collective_id=0, has_side_effects=True, vmem_limit_bytes=40 << 20
        ),
        name="analyse",
    )(*[pltpu.with_memory_space_constraint(a, pltpu.HBM) for a in (trials, sensors, readings, noises, lists, tiers)])


def solution(mesh):
    return jax.shard_map(
        per_device,
        mesh=mesh,
        in_specs=(
            P("member", ("region", "space"), None),
            P("member", ("region", "space")),
            P(("region", "space")),
            P(("region", "space")),
            P(("region", "space"), None),
            P(("region", "space")),
        ),
        out_specs=P("member", ("region", "space"), None),
        check_vma=False,
    )
```

```python
import functools

import jax
import jax.numpy as jnp
from jax import lax
from jax.experimental import pallas as pl
from jax.experimental.pallas import tpu as pltpu
from jax.sharding import PartitionSpec as P

NS_STEPS = 4
LANES = 128
GROUP = 4
CHUNK = 16
MESH = pl.DeviceIdType.MESH
F32 = jnp.float32
BF16 = jnp.bfloat16


def partner(me, k, n):
    if n & (n - 1):
        return lax.rem(me + k, n)
    other, bit = me, 1
    while bit < n:
        if k & bit:
            other = other + bit * (1 - 2 * lax.rem(me // bit, 2))
        bit *= 2
    return other


def split(value):
    high = value.astype(BF16)
    return high, (value - high.astype(F32)).astype(BF16)


def times(left, right):
    lh, ll = split(left)
    rh, rl = split(right)
    rows, k = left.shape[0], right.shape[0]
    lhs = jnp.concatenate([lh, ll], axis=0)[:, :k]
    rhs = jnp.concatenate([rh, rl], axis=1)
    out = jnp.dot(lhs, rhs, preferred_element_type=F32)
    width = right.shape[1]
    return out[:rows, :width] + out[:rows, width:] + out[rows:, :width]


def analyse_kernel(
    n, spaces, halo, obs_count, x, sensors_in, readings_in, noises_in, lists_in, tiers_in,
    out,
    entered, readings, noises, left_readings, left_noises, right_readings, right_noises, lists, tiers, small_sem, stage_sem, stage, incoming, updated, gathered, full, anoms, anoms_t, marks, weights, gram, target, trans,
    moved, sums,
    in_send, in_recv, out_send, out_recv, near_send, near_recv, chip_send, chip_recv, side_send, side_recv, sum_send, sum_recv,
):
    me = lax.axis_index("member")
    space = lax.axis_index("space")
    members, patch, _ = x.shape
    domains = patch // n
    lines = members * n
    width = anoms.shape[1]
    chunks = domains // CHUNK
    peers = n * spaces
    cores = 2 - n % 2
    chips = n // cores
    core, chip = lax.rem(me, cores), me // cores

    def landed(ref, sem):
        pltpu.make_async_copy(ref, ref, sem).wait()

    def slot(member):
        return lax.rem(member, cores) * chips + member // cores

    staged = n > 2 * cores and n & (n - 1) == 0
    low = n // 2 - cores if staged else n
    span = 2 * cores

    def central(member):
        return (member >= low) & (member < low + span)

    def in_views(to, g):
        return (
            x.at[:, pl.ds(pl.multiple_of(to * domains + g * CHUNK, 16), CHUNK), :],
            incoming.at[pl.ds(me * members, members), pl.ds(g * CHUNK, CHUNK), :],
        )

    lead = max(members // 5, 1)
    stage_parts = [pl.ds(0, lead), pl.ds(lead, members - lead)]
    middle = central(me)
    outer = jnp.logical_not(middle)
    barrier = pltpu.get_barrier_semaphore()

    def peer(k):
        other = lax.rem(me + space * n + k, peers)
        return {"member": lax.rem(other, n), "space": other // n}

    @pl.when(middle)
    def _():
        other = partner(me, n - cores, n)
        pl.semaphore_signal(barrier, inc=1, device_id={"member": other}, device_id_type=MESH)
        source, _ = in_views(other, 0)
        for i, rows in enumerate(stage_parts):
            pltpu.make_async_copy(source.at[rows], stage.at[rows], stage_sem.at[i]).start()

    half_chips = chips // 2
    upper = chip >= half_chips

    small = [
        pltpu.make_async_copy(source, place, small_sem.at[i])
        for i, (source, place) in enumerate(
            [
                (sensors_in, gathered.at[1, slot(me)]), (readings_in, readings), (noises_in, noises),
                (lists_in.at[pl.ds(pl.multiple_of(me * domains, 8), domains)], lists),
                (tiers_in, tiers),
            ]
        )
    ]
    for copy in small:
        copy.start()

    def greet(k, carry):
        other = peer(k)

        @pl.when(jnp.logical_not(central(other["member"])))
        def _():
            pl.semaphore_signal(barrier, inc=1, device_id=other, device_id_type=MESH)

        return carry

    lax.fori_loop(1, peers, greet, 0)
    lane = lax.broadcasted_iota(jnp.int32, (obs_count, width), 1)

    def mark(group, carry):
        start = pl.multiple_of(group * 8, 8)
        columns = jnp.transpose(lists[pl.ds(start, 8), :] - me * domains)
        found = []
        for d in range(8):
            hit = columns[:, d : d + 1] == lane
            found.append(jnp.sum(jnp.where(hit, 1.0, 0.0), axis=0, keepdims=True))
        marks[pl.ds(start, 8), :] = jnp.concatenate(found, axis=0)
        return carry

    def marking(first, last):
        with jax.named_scope("marks"):
            lax.fori_loop(first, last, mark, 0)

    has_left, has_right = space > 0, space < spaces - 1

    def to_space(side):
        return lax.rem(space + 1 - side + spaces, spaces)

    def slot_copy(other, half):
        place = gathered.at[1, slot(me)]
        return pltpu.make_async_remote_copy(
            place, place, chip_send.at[0], chip_recv.at[half],
            device_id={"member": other * cores + core}, device_id_type=MESH,
        )

    def near_slots():
        for j in range(1, half_chips if staged else chips):
            slot_copy(partner(chip, j, chips), 0).start()

    def cross_slot():
        if staged:
            slot_copy(half_chips - upper.astype(jnp.int32), 1).start()

    def relay_copy(j):
        rows = pl.ds(core * chips + (1 - upper.astype(jnp.int32)) * half_chips, half_chips)
        return pltpu.make_async_remote_copy(
            gathered.at[1, rows], gathered.at[1, rows], chip_send.at[j], chip_recv.at[1],
            device_id={"member": partner(chip, j, chips) * cores + core}, device_id_type=MESH,
        )

    singles = [(left_readings, left_noises), (readings, noises), (right_readings, right_noises)]

    def near_copies(side):
        index = side // 2
        return [
            pltpu.make_async_remote_copy(
                source, place, near_send.at[index, i], near_recv.at[index, i],
                device_id={"space": to_space(side)}, device_id_type=MESH,
            )
            for i, (source, place) in enumerate(zip((readings_in, noises_in), singles[side]))
        ]

    def side_copy(side, t):
        rows = pl.ds(core * chips, chips)
        return pltpu.make_async_remote_copy(
            gathered.at[1, rows], gathered.at[side, rows],
            side_send.at[side], side_recv.at[side],
            device_id={"member": chip * cores + lax.rem(core + t, cores), "space": to_space(side)},
            device_id_type=MESH,
        )

    def in_copy(g, k, rows=None):
        to = partner(me, k, n)
        source, place = in_views(to, g)
        if rows is not None:
            source, place = stage.at[rows], place.at[rows]
        return pltpu.make_async_remote_copy(
            source, place, in_send.at[0], in_recv.at[g],
            device_id={"member": to}, device_id_type=MESH,
        )

    far = list(range(n // 2, n))
    close = list(range(1, n // 2))
    far_first = far + close
    pairs = [(g, k) for g in range(chunks) for k in far_first]
    facing = [(g, n - cores) for g in range(chunks)]
    crossed = [(g, k) for g in range(chunks) for k in range(n - cores + 1, n)]
    relayed = [(0, k) for k in close]
    middle_early = facing + crossed + relayed
    outer_early = [(g, k) for g in range(chunks) for k in close]
    half = domains // 16

    def start_near():
        @pl.when(has_right)
        def _():
            for copy in near_copies(0):
                copy.start()

        @pl.when(has_left)
        def _():
            for copy in near_copies(2):
                copy.start()

    def start_own():
        for g in range(chunks):
            source, place = in_views(me, g)
            pltpu.make_async_copy(source, place, in_recv.at[g]).start()

    @pl.when(middle)
    def _():
        with jax.named_scope("w_middle"):
            pl.semaphore_wait(barrier, 1)
        for i, rows in enumerate(stage_parts):
            landed(stage.at[rows], stage_sem.at[i])
            in_copy(*facing[0], rows).start()
        small[0].wait()
        cross_slot()
        for g, k in facing[1:]:
            in_copy(g, k).start()
        start_own()
        for copy in small[1:]:
            copy.wait()
        marking(0, half)
        with jax.named_scope("w_entered"):
            pl.semaphore_wait(entered, 1)
        near_slots()
        start_near()
        for g, k in crossed:
            in_copy(g, k).start()

    @pl.when(outer)
    def _():
        with jax.named_scope("w_barrier"):
            pl.semaphore_wait(barrier, peers - 1)
        if staged:
            @pl.when((me >= low + span) & (me < low + span + cores))
            def _():
                for j in range(1, 3):
                    pl.semaphore_signal(
                        entered, inc=1, device_id={"member": me - j * cores}, device_id_type=MESH
                    )
        small[0].wait()
        cross_slot()
        near_slots()
        start_near()
        for g, k in outer_early:
            in_copy(g, k).start()
        start_own()
        for copy in small[1:]:
            copy.wait()
        marking(0, half)

    for side, missing in ((0, space == 0), (2, space == spaces - 1)):
        @pl.when(missing)
        def _():
            gathered[side] = jnp.ones(gathered.shape[1:], BF16)
            for single in singles[side]:
                single[...] = jnp.ones(single.shape, BF16)

    marking(half, domains // 8)

    with jax.named_scope("w_chip"):
        if staged:
            landed(gathered.at[1, pl.ds(0, half_chips)], chip_recv.at[1])

            @pl.when(middle)
            def _():
                for j in range(1, half_chips):
                    relay_copy(j).start()
                for g, k in relayed:
                    in_copy(g, k).start()
        near = half_chips - 1 if staged else chips - 1
        if near:
            landed(gathered.at[1, pl.ds(0, near)], chip_recv.at[0])

    for t in range(1, cores):
        side_copy(1, t).start()

    @pl.when(has_right)
    def _():
        for t in range(cores):
            side_copy(0, t).start()

    @pl.when(has_left)
    def _():
        for t in range(cores):
            side_copy(2, t).start()

    with jax.named_scope("w_side"):
        sent = half_chips if staged else chips - 1
        if sent:
            landed(gathered.at[1, pl.ds(0, sent)], chip_send.at[0])
        if staged:
            @pl.when(middle)
            def _():
                for j in range(1, half_chips):
                    relay_copy(j).wait_send()
        if cores > 1:
            others = gathered.at[1, pl.ds(0, n - chips)]
            landed(others, side_send.at[1])
            landed(others, side_recv.at[1])

        @pl.when(has_right)
        def _():
            for copy in near_copies(0):
                copy.wait_send()
            for copy in near_copies(2):
                copy.wait_recv()
            landed(gathered.at[1], side_send.at[0])
            landed(gathered.at[2], side_recv.at[2])

        @pl.when(has_left)
        def _():
            for copy in near_copies(2):
                copy.wait_send()
            for copy in near_copies(0):
                copy.wait_recv()
            landed(gathered.at[1], side_send.at[2])
            landed(gathered.at[0], side_recv.at[0])

    for side in range(3):
        for s in range(n):
            full[members * s : members * (s + 1), patch * side : patch * (side + 1)] = (
                gathered[side, s % cores * chips + s // cores].astype(F32)
            )
        for i, single in enumerate(singles[side]):
            full[lines + i : lines + i + 1, patch * side : patch * (side + 1)] = (
                single[...].astype(F32)[None]
            )
    total = 3 * patch
    shift = lax.rem(2 * total - (patch - halo) - me * domains, total)
    turned = pltpu.roll(full[...], shift, 1)[:, :width]
    values = turned[:lines]
    mean = jnp.sum(values, axis=0, keepdims=True) * (1.0 / lines)
    anomaly = values - mean
    anoms[...] = anomaly
    innov = turned[lines : lines + 1] - mean
    noise = turned[lines + 1 : lines + 2]
    squares = jnp.sum(anomaly * anomaly, axis=0, keepdims=True)

    own_tier = lax.broadcasted_iota(jnp.int32, (domains, patch), 1) == (
        lax.broadcasted_iota(jnp.int32, (domains, patch), 0) + me * domains
    )
    tier = jnp.sum(jnp.where(own_tier, tiers[...].astype(F32)[None], 0.0), axis=1, keepdims=True)
    radius = (tier + 2.0) * (0.5 * obs_count)
    place = lax.broadcasted_iota(jnp.int32, (domains, width), 1)
    row = lax.broadcasted_iota(jnp.int32, (domains, width), 0)
    distance = jnp.abs(place - halo - row).astype(F32) / radius
    weight = marks[...] * jnp.exp(-2.0 * distance * distance) / noise
    weights[...] = weight
    fit = jnp.sum(weight * (innov * innov))
    spread = jnp.sum(weight * squares)
    first = lax.broadcasted_iota(jnp.int32, (1, LANES), 1) == 0
    moved[...] = jnp.where(first, fit, spread)

    high, low = split(anomaly)
    pad = jnp.zeros((LANES - lines, width), F32)
    anoms_t[...] = jnp.concatenate(
        [
            jnp.transpose(jnp.concatenate([high.astype(F32), pad], axis=0)),
            jnp.transpose(jnp.concatenate([low.astype(F32), pad], axis=0)),
        ],
        axis=1,
    ).astype(BF16)

    def sum_copy(k):
        return pltpu.make_async_remote_copy(
            moved, sums.at[k], sum_send.at[0], sum_recv.at[0],
            device_id=peer(k), device_id_type=MESH,
        )

    def start_sum(k, carry):
        sum_copy(k).start()
        return carry

    def add_sum(k, carry):
        return carry + sums[k]

    lax.fori_loop(1, peers, start_sum, 0)

    @pl.when(middle)
    def _():
        for g, k in pairs:
            if (g, k) not in middle_early:
                in_copy(g, k).start()

    hi, lo = split(weight * innov)
    aims = jnp.dot(jnp.concatenate([hi, lo], axis=0), anoms_t[...], preferred_element_type=F32)
    target[...] = aims[:domains, :LANES] + aims[:domains, LANES:] + aims[domains:, :LANES]

    def gram_group(g, carry):
        for d in range(2):
            c = g * 2 + d
            hi, lo = split(anoms[...] * weights[pl.ds(c, 1), :])
            prod = jnp.dot(
                jnp.concatenate([hi, lo], axis=0), anoms_t[...], preferred_element_type=F32
            )
            gram[c] = prod[:lines, :LANES] + prod[:lines, LANES:] + prod[lines:, :LANES]
        return carry

    with jax.named_scope("gram"):
        lax.fori_loop(0, domains // 4, gram_group, 0)

    @pl.when(outer)
    def _():
        for g, k in pairs:
            if (g, k) not in outer_early:
                in_copy(g, k).start()

    with jax.named_scope("gram"):
        lax.fori_loop(domains // 4, domains // 2, gram_group, 0)

    with jax.named_scope("w_sums"):
        if peers > 1:
            others = sums.at[pl.ds(1, peers - 1)]
            landed(others, sum_send.at[0])
            landed(others, sum_recv.at[0])
        sums_all = lax.fori_loop(1, peers, add_sum, moved[...])

    scale = sums_all[:, 1:2] / sums_all[:, 0:1]
    eye = jnp.where(
        lax.broadcasted_iota(jnp.int32, (lines, LANES), 0)
        == lax.broadcasted_iota(jnp.int32, (lines, LANES), 1),
        1.0, 0.0,
    )
    diagonal = eye * scale

    def solve_group(g, carry):
        ids = [g * GROUP + d for d in range(GROUP)]
        mats = [gram[c] + diagonal for c in ids]
        bounds = [
            jnp.max(jnp.sum(jnp.abs(m), axis=0, keepdims=True), axis=1, keepdims=True)
            for m in mats
        ]
        ys = [m / b for m, b in zip(mats, bounds)]
        zs = [1.5 * eye - 0.5 * y for y in ys]
        ys = [times(y, z) for y, z in zip(ys, zs)]
        for step in range(1, NS_STEPS):
            ps = [1.5 * eye - 0.5 * times(z, y) for z, y in zip(zs, ys)]
            if step < NS_STEPS - 1:
                both = [
                    times(jnp.concatenate([y, z], axis=0), p) for y, z, p in zip(ys, zs, ps)
                ]
                ys = [b[:lines] for b in both]
                zs = [b[lines:] for b in both]
            else:
                zs = [times(z, p) for z, p in zip(zs, ps)]
        roots = [z * lax.rsqrt(b) for z, b in zip(zs, bounds)]
        for c, root in zip(ids, roots):
            half_gain = jnp.sum(root * target[pl.ds(c, 1), :], axis=1, keepdims=True)
            gain = jnp.sum(root * half_gain, axis=0, keepdims=True)
            w = (lines - 1.0) ** 0.5 * root + gain
            w = w - jnp.sum(w, axis=1, keepdims=True) * (1.0 / lines) + 1.0 / lines
            trans[c] = w.astype(BF16)
        return carry

    if staged:
        beyond = list(range(half_chips, chips)) + list(range(1, half_chips))
        receivers = [
            partner(chip, j, chips) * cores + c for j in beyond for c in reversed(range(cores))
        ] + [chip * cores + lax.rem(core + t, cores) for t in range(1, cores)]
    else:
        receivers = [partner(me, k, n) for k in far_first]

    def out_views(to, g):
        return (
            updated.at[pl.ds(to * members, members), pl.ds(g * CHUNK, CHUNK), :],
            out.at[:, pl.ds(pl.multiple_of(me * domains + g * CHUNK, 16), CHUNK), :],
        )

    def out_copy(g, to):
        source, place = out_views(to, g)
        return pltpu.make_async_remote_copy(
            source, place, out_send.at[0], out_recv.at[0],
            device_id={"member": to}, device_id_type=MESH,
        )

    for g in range(chunks):
        with jax.named_scope(f'solve{g}'):
            lax.fori_loop(g * CHUNK // GROUP, (g + 1) * CHUNK // GROUP, solve_group, 0)
        with jax.named_scope(f'w_in{g}'):
            landed(incoming.at[:, pl.ds(g * CHUNK, CHUNK), :], in_recv.at[g])
        states = jnp.swapaxes(incoming[:, g * CHUNK : (g + 1) * CHUNK, :].astype(F32), 0, 1)
        states = states.astype(BF16)
        results = [
            jnp.dot(trans[g * CHUNK + c][:, :lines], states[c], preferred_element_type=F32)
            for c in range(CHUNK)
        ]
        results = jnp.stack(results, axis=0)
        updated[:, g * CHUNK : (g + 1) * CHUNK, :] = jnp.swapaxes(results, 0, 1).astype(BF16)
        for to in receivers:
            out_copy(g, to).start()
        source, place = out_views(me, g)
        pltpu.make_async_copy(source, place, out_recv.at[0]).start()

    with jax.named_scope("w_out"):
        landed(out, out_recv.at[0])
    with jax.named_scope("w_sent"):
        if n > 1:
            landed(x.at[:, pl.ds(0, patch - domains), :], in_send.at[0])
            landed(updated.at[pl.ds(0, lines - members)], out_send.at[0])


def per_device(trials, sensors, readings, noises, lists, tiers):
    n, spaces = lax.axis_size("member"), lax.axis_size("space")
    members, patch, quantities = trials.shape
    obs_count = lists.shape[1]
    halo = 5 * obs_count // 2
    domains = patch // n
    chunks = domains // CHUNK
    lines = members * n
    width = -(-(domains + 2 * halo) // 256) * 256
    vmem = pl.BlockSpec(memory_space=pltpu.VMEM)
    anywhere = pl.BlockSpec(memory_space=pltpu.HBM)
    full_rows = -(-(lines + 2) // 8) * 8
    dma = pltpu.SemaphoreType.DMA
    return pl.pallas_call(
        functools.partial(analyse_kernel, n, spaces, halo, obs_count),
        out_shape=pltpu.VMEM((members, patch, quantities), BF16),
        in_specs=[anywhere] * 6,
        out_specs=vmem,
        scratch_shapes=[
            pltpu.SemaphoreType.REGULAR,
            pltpu.VMEM((patch,), BF16),
            pltpu.VMEM((patch,), BF16),
            pltpu.VMEM((patch,), BF16),
            pltpu.VMEM((patch,), BF16),
            pltpu.VMEM((patch,), BF16),
            pltpu.VMEM((patch,), BF16),
            pltpu.VMEM((domains, obs_count), jnp.int32),
            pltpu.VMEM((patch,), jnp.int32),
            dma((5,)), dma((2,)),
            pltpu.VMEM((members, CHUNK, quantities), BF16),
            pltpu.VMEM((lines, domains, quantities), BF16),
            pltpu.VMEM((lines, domains, quantities), BF16),
            pltpu.VMEM((3, n, members, patch), BF16),
            pltpu.VMEM((full_rows, 3 * patch), F32),
            pltpu.VMEM((lines, width), F32),
            pltpu.VMEM((width, 2 * LANES), BF16),
            pltpu.VMEM((domains, width), F32),
            pltpu.VMEM((domains, width), F32),
            pltpu.VMEM((domains, lines, LANES), F32),
            pltpu.VMEM((domains, LANES), F32),
            pltpu.VMEM((domains, lines, LANES), BF16),
            pltpu.VMEM((1, LANES), F32),
            pltpu.VMEM((n * spaces, 1, LANES), F32),
            dma((1,)), dma((chunks,)), dma((1,)), dma((1,)),
            dma((2, 2)), dma((2, 2)), dma((max(n // 4, 1),)), dma((2,)), dma((3,)), dma((3,)), dma((1,)), dma((1,)),
        ],
        compiler_params=pltpu.CompilerParams(
            collective_id=0, has_side_effects=True, vmem_limit_bytes=40 << 20
        ),
        name="analyse",
    )(*[pltpu.with_memory_space_constraint(a, pltpu.HBM) for a in (trials, sensors, readings, noises, lists, tiers)])


def solution(mesh):
    return jax.shard_map(
        per_device,
        mesh=mesh,
        in_specs=(
            P("member", ("region", "space"), None),
            P("member", ("region", "space")),
            P(("region", "space")),
            P(("region", "space")),
            P(("region", "space"), None),
            P(("region", "space")),
        ),
        out_specs=P("member", ("region", "space"), None),
        check_vma=False,
    )
```

```python
import functools

import jax
import jax.numpy as jnp
from jax import lax
from jax.experimental import pallas as pl
from jax.experimental.pallas import tpu as pltpu
from jax.sharding import PartitionSpec as P

NS_STEPS = 4
LANES = 128
GROUP = 4
CHUNK = 16
MESH = pl.DeviceIdType.MESH
F32 = jnp.float32
BF16 = jnp.bfloat16


def partner(me, k, n):
    if n & (n - 1):
        return lax.rem(me + k, n)
    other, bit = me, 1
    while bit < n:
        if k & bit:
            other = other + bit * (1 - 2 * lax.rem(me // bit, 2))
        bit *= 2
    return other


def split(value):
    high = value.astype(BF16)
    return high, (value - high.astype(F32)).astype(BF16)


def times(left, right):
    lh, ll = split(left)
    rh, rl = split(right)
    rows, k = left.shape[0], right.shape[0]
    lhs = jnp.concatenate([lh, ll], axis=0)[:, :k]
    rhs = jnp.concatenate([rh, rl], axis=1)
    out = jnp.dot(lhs, rhs, preferred_element_type=F32)
    width = right.shape[1]
    return out[:rows, :width] + out[:rows, width:] + out[rows:, :width]


def analyse_kernel(
    n, spaces, halo, obs_count, x, sensors_in, readings_in, noises_in, lists_in, tiers_in,
    out,
    entered, sensors, readings, noises, left_readings, left_noises, right_readings, right_noises, lists, tiers, small_sem, stage_sem, stage, incoming, updated, gathered, full, anoms, anoms_t, marks, weights, gram, target, trans,
    moved, sums,
    in_send, in_recv, out_send, out_recv, near_send, near_recv, chip_send, chip_recv, side_send, side_recv, sum_send, sum_recv,
):
    me = lax.axis_index("member")
    space = lax.axis_index("space")
    members, patch, _ = x.shape
    domains = patch // n
    lines = members * n
    width = anoms.shape[1]
    chunks = domains // CHUNK
    peers = n * spaces
    cores = 2 - n % 2
    chips = n // cores
    core, chip = lax.rem(me, cores), me // cores

    def landed(ref, sem):
        pltpu.make_async_copy(ref, ref, sem).wait()

    def slot(member):
        return lax.rem(member, cores) * chips + member // cores

    staged = n > 2 * cores and n & (n - 1) == 0
    low = n // 2 - cores if staged else n
    span = 2 * cores

    def central(member):
        return (member >= low) & (member < low + span)

    def in_views(to, g):
        return (
            x.at[:, pl.ds(pl.multiple_of(to * domains + g * CHUNK, 16), CHUNK), :],
            incoming.at[pl.ds(me * members, members), pl.ds(g * CHUNK, CHUNK), :],
        )

    lead = max(members // 5, 1)
    stage_parts = [pl.ds(0, lead), pl.ds(lead, members - lead)]
    middle = central(me)
    outer = jnp.logical_not(middle)
    barrier = pltpu.get_barrier_semaphore()

    def peer(k):
        other = lax.rem(me + space * n + k, peers)
        return {"member": lax.rem(other, n), "space": other // n}

    @pl.when(middle)
    def _():
        other = partner(me, n - cores, n)
        pl.semaphore_signal(barrier, inc=1, device_id={"member": other}, device_id_type=MESH)
        source, _ = in_views(other, 0)
        for i, rows in enumerate(stage_parts):
            pltpu.make_async_copy(source.at[rows], stage.at[rows], stage_sem.at[i]).start()

    half_chips = chips // 2
    upper = chip >= half_chips

    small = [
        pltpu.make_async_copy(source, place, small_sem.at[i])
        for i, (source, place) in enumerate(
            [
                (sensors_in, sensors), (readings_in, readings), (noises_in, noises),
                (lists_in.at[pl.ds(pl.multiple_of(me * domains, 8), domains)], lists),
                (tiers_in, tiers),
            ]
        )
    ]
    for copy in small:
        copy.start()

    def greet(k, carry):
        other = peer(k)

        @pl.when(jnp.logical_not(central(other["member"])))
        def _():
            pl.semaphore_signal(barrier, inc=1, device_id=other, device_id_type=MESH)

        return carry

    lax.fori_loop(1, peers, greet, 0)
    lane = lax.broadcasted_iota(jnp.int32, (obs_count, width), 1)

    def mark(group, carry):
        start = pl.multiple_of(group * 8, 8)
        columns = jnp.transpose(lists[pl.ds(start, 8), :] - me * domains)
        found = []
        for d in range(8):
            hit = columns[:, d : d + 1] == lane
            found.append(jnp.sum(jnp.where(hit, 1.0, 0.0), axis=0, keepdims=True))
        marks[pl.ds(start, 8), :] = jnp.concatenate(found, axis=0)
        return carry

    def marking(first, last):
        with jax.named_scope("marks"):
            lax.fori_loop(first, last, mark, 0)

    has_left, has_right = space > 0, space < spaces - 1

    def to_space(side):
        return lax.rem(space + 1 - side + spaces, spaces)

    strips = patch // LANES

    def pack():
        small[0].wait()
        values = sensors[...].astype(F32)
        rows = [values[:, LANES * t : LANES * (t + 1)] for t in range(strips)]
        spare = gathered.shape[2] - members * strips
        if spare:
            rows.append(jnp.zeros((spare, LANES), F32))
        gathered[1, slot(me)] = jnp.concatenate(rows, axis=0).astype(BF16)

    def slot_copy(other, half):
        place = gathered.at[1, slot(me)]
        return pltpu.make_async_remote_copy(
            place, place, chip_send.at[0], chip_recv.at[half],
            device_id={"member": other * cores + core}, device_id_type=MESH,
        )

    def near_slots():
        for j in range(1, half_chips if staged else chips):
            slot_copy(partner(chip, j, chips), 0).start()

    def cross_slot():
        if staged:
            slot_copy(half_chips - upper.astype(jnp.int32), 1).start()

    def relay_copy(j):
        rows = pl.ds(core * chips + (1 - upper.astype(jnp.int32)) * half_chips, half_chips)
        return pltpu.make_async_remote_copy(
            gathered.at[1, rows], gathered.at[1, rows], chip_send.at[j], chip_recv.at[1],
            device_id={"member": partner(chip, j, chips) * cores + core}, device_id_type=MESH,
        )

    singles = [(left_readings, left_noises), (readings, noises), (right_readings, right_noises)]

    def near_copies(side):
        index = side // 2
        return [
            pltpu.make_async_remote_copy(
                source, place, near_send.at[index, i], near_recv.at[index, i],
                device_id={"space": to_space(side)}, device_id_type=MESH,
            )
            for i, (source, place) in enumerate(zip((readings_in, noises_in), singles[side]))
        ]

    def side_copy(side, t):
        rows = pl.ds(core * chips, chips)
        return pltpu.make_async_remote_copy(
            gathered.at[1, rows], gathered.at[side, rows],
            side_send.at[side], side_recv.at[side],
            device_id={"member": chip * cores + lax.rem(core + t, cores), "space": to_space(side)},
            device_id_type=MESH,
        )

    def in_copy(g, k, rows=None):
        to = partner(me, k, n)
        source, place = in_views(to, g)
        if rows is not None:
            source, place = stage.at[rows], place.at[rows]
        return pltpu.make_async_remote_copy(
            source, place, in_send.at[0], in_recv.at[g],
            device_id={"member": to}, device_id_type=MESH,
        )

    far = list(range(n // 2, n))
    close = list(range(1, n // 2))
    far_first = far + close
    pairs = [(g, k) for g in range(chunks) for k in far_first]
    facing = [(g, n - cores) for g in range(chunks)]
    crossed = [(g, k) for g in range(chunks) for k in range(n - cores + 1, n)]
    relayed = [(0, k) for k in close]
    middle_early = facing + crossed + relayed
    outer_early = [(g, k) for g in range(chunks) for k in close]
    half = domains // 16

    def start_near():
        @pl.when(has_right)
        def _():
            for copy in near_copies(0):
                copy.start()

        @pl.when(has_left)
        def _():
            for copy in near_copies(2):
                copy.start()

    def start_own():
        for g in range(chunks):
            source, place = in_views(me, g)
            pltpu.make_async_copy(source, place, in_recv.at[g]).start()

    @pl.when(middle)
    def _():
        with jax.named_scope("w_middle"):
            pl.semaphore_wait(barrier, 1)
        for i, rows in enumerate(stage_parts):
            landed(stage.at[rows], stage_sem.at[i])
            in_copy(*facing[0], rows).start()
        pack()
        cross_slot()
        for g, k in facing[1:]:
            in_copy(g, k).start()
        start_own()
        for copy in small[1:]:
            copy.wait()
        marking(0, half)
        with jax.named_scope("w_entered"):
            pl.semaphore_wait(entered, 1)
        near_slots()
        start_near()
        for g, k in crossed:
            in_copy(g, k).start()

    @pl.when(outer)
    def _():
        pack()
        with jax.named_scope("w_barrier"):
            pl.semaphore_wait(barrier, peers - 1)
        if staged:
            @pl.when((me >= low + span) & (me < low + span + cores))
            def _():
                for j in range(1, 3):
                    pl.semaphore_signal(
                        entered, inc=1, device_id={"member": me - j * cores}, device_id_type=MESH
                    )
        cross_slot()
        near_slots()
        start_near()
        for g, k in outer_early:
            in_copy(g, k).start()
        start_own()
        for copy in small[1:]:
            copy.wait()
        marking(0, half)

    for side, missing in ((0, space == 0), (2, space == spaces - 1)):
        @pl.when(missing)
        def _():
            gathered[side] = jnp.ones(gathered.shape[1:], BF16)
            for single in singles[side]:
                single[...] = jnp.ones(single.shape, BF16)

    marking(half, domains // 8)

    with jax.named_scope("w_chip"):
        if staged:
            landed(gathered.at[1, pl.ds(0, half_chips)], chip_recv.at[1])

            @pl.when(middle)
            def _():
                for j in range(1, half_chips):
                    relay_copy(j).start()
                for g, k in relayed:
                    in_copy(g, k).start()
        near = half_chips - 1 if staged else chips - 1
        if near:
            landed(gathered.at[1, pl.ds(0, near)], chip_recv.at[0])

    for t in range(1, cores):
        side_copy(1, t).start()

    @pl.when(has_right)
    def _():
        for t in range(cores):
            side_copy(0, t).start()

    @pl.when(has_left)
    def _():
        for t in range(cores):
            side_copy(2, t).start()

    with jax.named_scope("w_side"):
        sent = half_chips if staged else chips - 1
        if sent:
            landed(gathered.at[1, pl.ds(0, sent)], chip_send.at[0])
        if staged:
            @pl.when(middle)
            def _():
                for j in range(1, half_chips):
                    relay_copy(j).wait_send()
        if cores > 1:
            others = gathered.at[1, pl.ds(0, n - chips)]
            landed(others, side_send.at[1])
            landed(others, side_recv.at[1])

        @pl.when(has_right)
        def _():
            for copy in near_copies(0):
                copy.wait_send()
            for copy in near_copies(2):
                copy.wait_recv()
            landed(gathered.at[1], side_send.at[0])
            landed(gathered.at[2], side_recv.at[2])

        @pl.when(has_left)
        def _():
            for copy in near_copies(2):
                copy.wait_send()
            for copy in near_copies(0):
                copy.wait_recv()
            landed(gathered.at[1], side_send.at[2])
            landed(gathered.at[0], side_recv.at[0])

    for side in range(3):
        for s in range(n):
            rows = gathered[side, s % cores * chips + s // cores].astype(F32)
            for t in range(strips):
                at = patch * side + LANES * t
                full[members * s : members * (s + 1), at : at + LANES] = (
                    rows[members * t : members * (t + 1)]
                )
        for i, single in enumerate(singles[side]):
            full[lines + i : lines + i + 1, patch * side : patch * (side + 1)] = (
                single[...].astype(F32)[None]
            )
    total = 3 * patch
    shift = lax.rem(2 * total - (patch - halo) - me * domains, total)
    turned = pltpu.roll(full[...], shift, 1)[:, :width]
    values = turned[:lines]
    mean = jnp.sum(values, axis=0, keepdims=True) * (1.0 / lines)
    anomaly = values - mean
    anoms[...] = anomaly
    innov = turned[lines : lines + 1] - mean
    noise = turned[lines + 1 : lines + 2]
    squares = jnp.sum(anomaly * anomaly, axis=0, keepdims=True)

    own_tier = lax.broadcasted_iota(jnp.int32, (domains, patch), 1) == (
        lax.broadcasted_iota(jnp.int32, (domains, patch), 0) + me * domains
    )
    tier = jnp.sum(jnp.where(own_tier, tiers[...].astype(F32)[None], 0.0), axis=1, keepdims=True)
    radius = (tier + 2.0) * (0.5 * obs_count)
    place = lax.broadcasted_iota(jnp.int32, (domains, width), 1)
    row = lax.broadcasted_iota(jnp.int32, (domains, width), 0)
    distance = jnp.abs(place - halo - row).astype(F32) / radius
    weight = marks[...] * jnp.exp(-2.0 * distance * distance) / noise
    weights[...] = weight
    fit = jnp.sum(weight * (innov * innov))
    spread = jnp.sum(weight * squares)
    first = lax.broadcasted_iota(jnp.int32, (1, LANES), 1) == 0
    moved[...] = jnp.where(first, fit, spread)

    high, low = split(anomaly)
    pad = jnp.zeros((LANES - lines, width), F32)
    anoms_t[...] = jnp.concatenate(
        [
            jnp.transpose(jnp.concatenate([high.astype(F32), pad], axis=0)),
            jnp.transpose(jnp.concatenate([low.astype(F32), pad], axis=0)),
        ],
        axis=1,
    ).astype(BF16)

    def sum_copy(k):
        return pltpu.make_async_remote_copy(
            moved, sums.at[k], sum_send.at[0], sum_recv.at[0],
            device_id=peer(k), device_id_type=MESH,
        )

    def start_sum(k, carry):
        sum_copy(k).start()
        return carry

    def add_sum(k, carry):
        return carry + sums[k]

    lax.fori_loop(1, peers, start_sum, 0)

    @pl.when(middle)
    def _():
        for g, k in pairs:
            if (g, k) not in middle_early:
                in_copy(g, k).start()

    hi, lo = split(weight * innov)
    aims = jnp.dot(jnp.concatenate([hi, lo], axis=0), anoms_t[...], preferred_element_type=F32)
    target[...] = aims[:domains, :LANES] + aims[:domains, LANES:] + aims[domains:, :LANES]

    def gram_group(g, carry):
        for d in range(2):
            c = g * 2 + d
            hi, lo = split(anoms[...] * weights[pl.ds(c, 1), :])
            prod = jnp.dot(
                jnp.concatenate([hi, lo], axis=0), anoms_t[...], preferred_element_type=F32
            )
            gram[c] = prod[:lines, :LANES] + prod[:lines, LANES:] + prod[lines:, :LANES]
        return carry

    with jax.named_scope("gram"):
        lax.fori_loop(0, domains // 4, gram_group, 0)

    @pl.when(outer)
    def _():
        for g, k in pairs:
            if (g, k) not in outer_early:
                in_copy(g, k).start()

    with jax.named_scope("gram"):
        lax.fori_loop(domains // 4, domains // 2, gram_group, 0)

    with jax.named_scope("w_sums"):
        if peers > 1:
            others = sums.at[pl.ds(1, peers - 1)]
            landed(others, sum_send.at[0])
            landed(others, sum_recv.at[0])
        sums_all = lax.fori_loop(1, peers, add_sum, moved[...])

    scale = sums_all[:, 1:2] / sums_all[:, 0:1]
    eye = jnp.where(
        lax.broadcasted_iota(jnp.int32, (lines, LANES), 0)
        == lax.broadcasted_iota(jnp.int32, (lines, LANES), 1),
        1.0, 0.0,
    )
    diagonal = eye * scale

    def solve_group(g, carry):
        ids = [g * GROUP + d for d in range(GROUP)]
        mats = [gram[c] + diagonal for c in ids]
        bounds = [
            jnp.max(jnp.sum(jnp.abs(m), axis=0, keepdims=True), axis=1, keepdims=True)
            for m in mats
        ]
        ys = [m / b for m, b in zip(mats, bounds)]
        zs = [1.5 * eye - 0.5 * y for y in ys]
        ys = [times(y, z) for y, z in zip(ys, zs)]
        for step in range(1, NS_STEPS):
            ps = [1.5 * eye - 0.5 * times(z, y) for z, y in zip(zs, ys)]
            if step < NS_STEPS - 1:
                both = [
                    times(jnp.concatenate([y, z], axis=0), p) for y, z, p in zip(ys, zs, ps)
                ]
                ys = [b[:lines] for b in both]
                zs = [b[lines:] for b in both]
            else:
                zs = [times(z, p) for z, p in zip(zs, ps)]
        roots = [z * lax.rsqrt(b) for z, b in zip(zs, bounds)]
        for c, root in zip(ids, roots):
            half_gain = jnp.sum(root * target[pl.ds(c, 1), :], axis=1, keepdims=True)
            gain = jnp.sum(root * half_gain, axis=0, keepdims=True)
            w = (lines - 1.0) ** 0.5 * root + gain
            w = w - jnp.sum(w, axis=1, keepdims=True) * (1.0 / lines) + 1.0 / lines
            trans[c] = w.astype(BF16)
        return carry

    if staged:
        beyond = list(range(half_chips, chips)) + list(range(1, half_chips))
        receivers = [
            partner(chip, j, chips) * cores + c for j in beyond for c in reversed(range(cores))
        ] + [chip * cores + lax.rem(core + t, cores) for t in range(1, cores)]
    else:
        receivers = [partner(me, k, n) for k in far_first]

    def out_views(to, g):
        return (
            updated.at[pl.ds(to * members, members), pl.ds(g * CHUNK, CHUNK), :],
            out.at[:, pl.ds(pl.multiple_of(me * domains + g * CHUNK, 16), CHUNK), :],
        )

    def out_copy(g, to):
        source, place = out_views(to, g)
        return pltpu.make_async_remote_copy(
            source, place, out_send.at[0], out_recv.at[0],
            device_id={"member": to}, device_id_type=MESH,
        )

    for g in range(chunks):
        with jax.named_scope(f'solve{g}'):
            lax.fori_loop(g * CHUNK // GROUP, (g + 1) * CHUNK // GROUP, solve_group, 0)
        with jax.named_scope(f'w_in{g}'):
            landed(incoming.at[:, pl.ds(g * CHUNK, CHUNK), :], in_recv.at[g])
        states = jnp.swapaxes(incoming[:, g * CHUNK : (g + 1) * CHUNK, :].astype(F32), 0, 1)
        states = states.astype(BF16)
        results = [
            jnp.dot(trans[g * CHUNK + c][:, :lines], states[c], preferred_element_type=F32)
            for c in range(CHUNK)
        ]
        results = jnp.stack(results, axis=0)
        updated[:, g * CHUNK : (g + 1) * CHUNK, :] = jnp.swapaxes(results, 0, 1).astype(BF16)
        for to in receivers:
            out_copy(g, to).start()
        source, place = out_views(me, g)
        pltpu.make_async_copy(source, place, out_recv.at[0]).start()

    with jax.named_scope("w_out"):
        landed(out, out_recv.at[0])
    with jax.named_scope("w_sent"):
        if n > 1:
            landed(x.at[:, pl.ds(0, patch - domains), :], in_send.at[0])
            landed(updated.at[pl.ds(0, lines - members)], out_send.at[0])


def per_device(trials, sensors, readings, noises, lists, tiers):
    n, spaces = lax.axis_size("member"), lax.axis_size("space")
    members, patch, quantities = trials.shape
    obs_count = lists.shape[1]
    halo = 5 * obs_count // 2
    domains = patch // n
    chunks = domains // CHUNK
    lines = members * n
    width = -(-(domains + 2 * halo) // 256) * 256
    vmem = pl.BlockSpec(memory_space=pltpu.VMEM)
    anywhere = pl.BlockSpec(memory_space=pltpu.HBM)
    packed = -(-members * (patch // LANES) // 16) * 16
    full_rows = -(-(lines + 2) // 8) * 8
    dma = pltpu.SemaphoreType.DMA
    return pl.pallas_call(
        functools.partial(analyse_kernel, n, spaces, halo, obs_count),
        out_shape=pltpu.VMEM((members, patch, quantities), BF16),
        in_specs=[anywhere] * 6,
        out_specs=vmem,
        scratch_shapes=[
            pltpu.SemaphoreType.REGULAR,
            pltpu.VMEM((members, patch), BF16),
            pltpu.VMEM((patch,), BF16),
            pltpu.VMEM((patch,), BF16),
            pltpu.VMEM((patch,), BF16),
            pltpu.VMEM((patch,), BF16),
            pltpu.VMEM((patch,), BF16),
            pltpu.VMEM((patch,), BF16),
            pltpu.VMEM((domains, obs_count), jnp.int32),
            pltpu.VMEM((patch,), jnp.int32),
            dma((5,)), dma((2,)),
            pltpu.VMEM((members, CHUNK, quantities), BF16),
            pltpu.VMEM((lines, domains, quantities), BF16),
            pltpu.VMEM((lines, domains, quantities), BF16),
            pltpu.VMEM((3, n, packed, LANES), BF16),
            pltpu.VMEM((full_rows, 3 * patch), F32),
            pltpu.VMEM((lines, width), F32),
            pltpu.VMEM((width, 2 * LANES), BF16),
            pltpu.VMEM((domains, width), F32),
            pltpu.VMEM((domains, width), F32),
            pltpu.VMEM((domains, lines, LANES), F32),
            pltpu.VMEM((domains, LANES), F32),
            pltpu.VMEM((domains, lines, LANES), BF16),
            pltpu.VMEM((1, LANES), F32),
            pltpu.VMEM((n * spaces, 1, LANES), F32),
            dma((1,)), dma((chunks,)), dma((1,)), dma((1,)),
            dma((2, 2)), dma((2, 2)), dma((max(n // 4, 1),)), dma((2,)), dma((3,)), dma((3,)), dma((1,)), dma((1,)),
        ],
        compiler_params=pltpu.CompilerParams(
            collective_id=0, has_side_effects=True, vmem_limit_bytes=40 << 20
        ),
        name="analyse",
    )(*[pltpu.with_memory_space_constraint(a, pltpu.HBM) for a in (trials, sensors, readings, noises, lists, tiers)])


def solution(mesh):
    return jax.shard_map(
        per_device,
        mesh=mesh,
        in_specs=(
            P("member", ("region", "space"), None),
            P("member", ("region", "space")),
            P(("region", "space")),
            P(("region", "space")),
            P(("region", "space"), None),
            P(("region", "space")),
        ),
        out_specs=P("member", ("region", "space"), None),
        check_vma=False,
    )
```

```python
import functools

import jax
import jax.numpy as jnp
from jax import lax
from jax.experimental import pallas as pl
from jax.experimental.pallas import tpu as pltpu
from jax.sharding import PartitionSpec as P

NS_STEPS = 4
LANES = 128
GROUP = 4
CHUNK = 16
MESH = pl.DeviceIdType.MESH
F32 = jnp.float32
BF16 = jnp.bfloat16


def partner(me, k, n):
    if n & (n - 1):
        return lax.rem(me + k, n)
    other, bit = me, 1
    while bit < n:
        if k & bit:
            other = other + bit * (1 - 2 * lax.rem(me // bit, 2))
        bit *= 2
    return other


def split(value):
    high = value.astype(BF16)
    return high, (value - high.astype(F32)).astype(BF16)


def times(left, right):
    lh, ll = split(left)
    rh, rl = split(right)
    rows, k = left.shape[0], right.shape[0]
    lhs = jnp.concatenate([lh, ll], axis=0)[:, :k]
    rhs = jnp.concatenate([rh, rl], axis=1)
    out = jnp.dot(lhs, rhs, preferred_element_type=F32)
    width = right.shape[1]
    return out[:rows, :width] + out[:rows, width:] + out[rows:, :width]


def analyse_kernel(
    n, spaces, halo, obs_count, x, sensors_in, readings_in, noises_in, lists_in, tiers_in,
    out,
    entered, sensors, readings, noises, left_readings, left_noises, right_readings, right_noises, lists, tiers, small_sem, stage_sem, stage, incoming, updated, gathered, full, anoms, anoms_t, marks, weights, gram, target, trans,
    moved, sums,
    in_send, in_recv, out_recv, near_recv, chip_send, chip_recv, side_send, side_recv, sum_recv,
):
    me = lax.axis_index("member")
    space = lax.axis_index("space")
    members, patch, _ = x.shape
    domains = patch // n
    lines = members * n
    width = anoms.shape[1]
    chunks = domains // CHUNK
    peers = n * spaces
    cores = 2 - n % 2
    chips = n // cores
    core, chip = lax.rem(me, cores), me // cores

    def landed(ref, sem):
        pltpu.make_async_copy(ref, ref, sem).wait()

    def slot(member):
        return lax.rem(member, cores) * chips + member // cores

    staged = n > 2 * cores and n & (n - 1) == 0
    low = n // 2 - cores if staged else n
    span = 2 * cores

    def central(member):
        return (member >= low) & (member < low + span)

    def in_views(to, g):
        return (
            x.at[:, pl.ds(pl.multiple_of(to * domains + g * CHUNK, 16), CHUNK), :],
            incoming.at[pl.ds(me * members, members), pl.ds(g * CHUNK, CHUNK), :],
        )

    lead = max(members // 5, 1)
    stage_parts = [pl.ds(0, lead), pl.ds(lead, members - lead)]
    middle = central(me)
    outer = jnp.logical_not(middle)
    barrier = pltpu.get_barrier_semaphore()

    def peer(k):
        other = lax.rem(me + space * n + k, peers)
        return {"member": lax.rem(other, n), "space": other // n}

    @pl.when(middle)
    def _():
        other = partner(me, n - cores, n)
        pl.semaphore_signal(barrier, inc=1, device_id={"member": other}, device_id_type=MESH)
        source, _ = in_views(other, 0)
        for i, rows in enumerate(stage_parts):
            pltpu.make_async_copy(source.at[rows], stage.at[rows], stage_sem.at[i]).start()

    half_chips = chips // 2
    upper = chip >= half_chips

    small = [
        pltpu.make_async_copy(source, place, small_sem.at[i])
        for i, (source, place) in enumerate(
            [
                (sensors_in, sensors), (readings_in, readings), (noises_in, noises),
                (lists_in.at[pl.ds(pl.multiple_of(me * domains, 8), domains)], lists),
                (tiers_in, tiers),
            ]
        )
    ]
    for copy in small:
        copy.start()

    def greet(k, carry):
        other = peer(k)

        @pl.when(jnp.logical_not(central(other["member"])))
        def _():
            pl.semaphore_signal(barrier, inc=1, device_id=other, device_id_type=MESH)

        return carry

    lax.fori_loop(1, peers, greet, 0)
    lane = lax.broadcasted_iota(jnp.int32, (obs_count, width), 1)

    def mark(group, carry):
        start = pl.multiple_of(group * 8, 8)
        columns = jnp.transpose(lists[pl.ds(start, 8), :] - me * domains)
        found = []
        for d in range(8):
            hit = columns[:, d : d + 1] == lane
            found.append(jnp.sum(jnp.where(hit, 1.0, 0.0), axis=0, keepdims=True))
        marks[pl.ds(start, 8), :] = jnp.concatenate(found, axis=0)
        return carry

    def marking(first, last):
        with jax.named_scope("marks"):
            lax.fori_loop(first, last, mark, 0)

    has_left, has_right = space > 0, space < spaces - 1

    def to_space(side):
        return lax.rem(space + 1 - side + spaces, spaces)

    strips = patch // LANES

    def pack():
        small[0].wait()
        values = sensors[...].astype(F32)
        rows = [values[:, LANES * t : LANES * (t + 1)] for t in range(strips)]
        spare = gathered.shape[2] - members * strips
        if spare:
            rows.append(jnp.zeros((spare, LANES), F32))
        gathered[1, slot(me)] = jnp.concatenate(rows, axis=0).astype(BF16)

    def slot_copy(other, half):
        place = gathered.at[1, slot(me)]
        return pltpu.make_async_remote_copy(
            place, place, small_sem.at[0], chip_recv.at[half],
            device_id={"member": other * cores + core}, device_id_type=MESH,
        )

    def near_slots():
        for j in range(1, half_chips if staged else chips):
            slot_copy(partner(chip, j, chips), 0).start()

    def cross_slot():
        if staged:
            slot_copy(half_chips - upper.astype(jnp.int32), 1).start()

    def relay_copy(j):
        rows = pl.ds(core * chips + (1 - upper.astype(jnp.int32)) * half_chips, half_chips)
        return pltpu.make_async_remote_copy(
            gathered.at[1, rows], gathered.at[1, rows], chip_send.at[j - 1], chip_recv.at[1],
            device_id={"member": partner(chip, j, chips) * cores + core}, device_id_type=MESH,
        )

    singles = [(left_readings, left_noises), (readings, noises), (right_readings, right_noises)]

    def near_copies(side):
        index = side // 2
        return [
            pltpu.make_async_remote_copy(
                source, place, small_sem.at[1 + 2 * index + i], near_recv.at[index, i],
                device_id={"space": to_space(side)}, device_id_type=MESH,
            )
            for i, (source, place) in enumerate(zip((readings_in, noises_in), singles[side]))
        ]

    def side_copy(side, t):
        rows = pl.ds(core * chips, chips)
        return pltpu.make_async_remote_copy(
            gathered.at[1, rows], gathered.at[side, rows],
            side_send.at[side], side_recv.at[side],
            device_id={"member": chip * cores + lax.rem(core + t, cores), "space": to_space(side)},
            device_id_type=MESH,
        )

    def in_copy(g, k, rows=None):
        to = partner(me, k, n)
        source, place = in_views(to, g)
        if rows is not None:
            source, place = stage.at[rows], place.at[rows]
        return pltpu.make_async_remote_copy(
            source, place, in_send.at[0], in_recv.at[g],
            device_id={"member": to}, device_id_type=MESH,
        )

    far = list(range(n // 2, n))
    close = list(range(1, n // 2))
    far_first = far + close
    pairs = [(g, k) for g in range(chunks) for k in far_first]
    facing = [(g, n - cores) for g in range(chunks)]
    crossed = [(g, k) for g in range(chunks) for k in range(n - cores + 1, n)]
    relayed = [(0, k) for k in close]
    middle_early = facing + crossed + relayed
    outer_early = [(g, k) for g in range(chunks) for k in close]
    half = domains // 16

    def start_near():
        @pl.when(has_right)
        def _():
            for copy in near_copies(0):
                copy.start()

        @pl.when(has_left)
        def _():
            for copy in near_copies(2):
                copy.start()

    def start_own():
        for g in range(chunks):
            source, place = in_views(me, g)
            pltpu.make_async_copy(source, place, in_recv.at[g]).start()

    @pl.when(middle)
    def _():
        with jax.named_scope("w_middle"):
            pl.semaphore_wait(barrier, 1)
        for i, rows in enumerate(stage_parts):
            landed(stage.at[rows], stage_sem.at[i])
            in_copy(*facing[0], rows).start()
        pack()
        cross_slot()
        for g, k in facing[1:]:
            in_copy(g, k).start()
        start_own()
        for copy in small[1:]:
            copy.wait()
        marking(0, half)
        with jax.named_scope("w_entered"):
            pl.semaphore_wait(entered, 1)
        near_slots()
        start_near()
        for g, k in crossed:
            in_copy(g, k).start()

    @pl.when(outer)
    def _():
        pack()
        with jax.named_scope("w_barrier"):
            pl.semaphore_wait(barrier, peers - 1)
        if staged:
            @pl.when((me >= low + span) & (me < low + span + cores))
            def _():
                for j in range(1, 3):
                    pl.semaphore_signal(
                        entered, inc=1, device_id={"member": me - j * cores}, device_id_type=MESH
                    )
        cross_slot()
        near_slots()
        for g, k in outer_early:
            in_copy(g, k).start()
        start_own()
        for copy in small[1:]:
            copy.wait()
        start_near()
        marking(0, half)

    for side, missing in ((0, space == 0), (2, space == spaces - 1)):
        @pl.when(missing)
        def _():
            gathered[side] = jnp.ones(gathered.shape[1:], BF16)
            for single in singles[side]:
                single[...] = jnp.ones(single.shape, BF16)

    marking(half, domains // 8)

    with jax.named_scope("w_chip"):
        if staged:
            landed(gathered.at[1, pl.ds(0, half_chips)], chip_recv.at[1])

            @pl.when(middle)
            def _():
                for j in range(1, half_chips):
                    relay_copy(j).start()
                for g, k in relayed:
                    in_copy(g, k).start()
        near = half_chips - 1 if staged else chips - 1
        if near:
            landed(gathered.at[1, pl.ds(0, near)], chip_recv.at[0])

    for t in range(1, cores):
        side_copy(1, t).start()

    @pl.when(has_right)
    def _():
        for t in range(cores):
            side_copy(0, t).start()

    @pl.when(has_left)
    def _():
        for t in range(cores):
            side_copy(2, t).start()

    with jax.named_scope("w_side"):
        sent = half_chips if staged else chips - 1
        if sent:
            landed(gathered.at[1, pl.ds(0, sent)], small_sem.at[0])
        if staged:
            @pl.when(middle)
            def _():
                for j in range(1, half_chips):
                    relay_copy(j).wait_send()
        if cores > 1:
            others = gathered.at[1, pl.ds(0, n - chips)]
            landed(others, side_send.at[1])
            landed(others, side_recv.at[1])

        @pl.when(has_right)
        def _():
            for copy in near_copies(0):
                copy.wait_send()
            for copy in near_copies(2):
                copy.wait_recv()
            landed(gathered.at[1], side_send.at[0])
            landed(gathered.at[2], side_recv.at[2])

        @pl.when(has_left)
        def _():
            for copy in near_copies(2):
                copy.wait_send()
            for copy in near_copies(0):
                copy.wait_recv()
            landed(gathered.at[1], side_send.at[2])
            landed(gathered.at[0], side_recv.at[0])

    for side in range(3):
        for s in range(n):
            rows = gathered[side, s % cores * chips + s // cores].astype(F32)
            for t in range(strips):
                at = patch * side + LANES * t
                full[members * s : members * (s + 1), at : at + LANES] = (
                    rows[members * t : members * (t + 1)]
                )
        for i, single in enumerate(singles[side]):
            full[lines + i : lines + i + 1, patch * side : patch * (side + 1)] = (
                single[...].astype(F32)[None]
            )
    total = 3 * patch
    shift = lax.rem(2 * total - (patch - halo) - me * domains, total)
    turned = pltpu.roll(full[...], shift, 1)[:, :width]
    values = turned[:lines]
    mean = jnp.sum(values, axis=0, keepdims=True) * (1.0 / lines)
    anomaly = values - mean
    anoms[...] = anomaly
    innov = turned[lines : lines + 1] - mean
    noise = turned[lines + 1 : lines + 2]
    squares = jnp.sum(anomaly * anomaly, axis=0, keepdims=True)

    own_tier = lax.broadcasted_iota(jnp.int32, (domains, patch), 1) == (
        lax.broadcasted_iota(jnp.int32, (domains, patch), 0) + me * domains
    )
    tier = jnp.sum(jnp.where(own_tier, tiers[...].astype(F32)[None], 0.0), axis=1, keepdims=True)
    radius = (tier + 2.0) * (0.5 * obs_count)
    place = lax.broadcasted_iota(jnp.int32, (domains, width), 1)
    row = lax.broadcasted_iota(jnp.int32, (domains, width), 0)
    distance = jnp.abs(place - halo - row).astype(F32) / radius
    weight = marks[...] * jnp.exp(-2.0 * distance * distance) / noise
    weights[...] = weight
    fit = jnp.sum(weight * (innov * innov))
    spread = jnp.sum(weight * squares)
    first = lax.broadcasted_iota(jnp.int32, (1, LANES), 1) == 0
    moved[...] = jnp.where(first, fit, spread)

    high, low = split(anomaly)
    pad = jnp.zeros((LANES - lines, width), F32)
    anoms_t[...] = jnp.concatenate(
        [
            jnp.transpose(jnp.concatenate([high.astype(F32), pad], axis=0)),
            jnp.transpose(jnp.concatenate([low.astype(F32), pad], axis=0)),
        ],
        axis=1,
    ).astype(BF16)

    def sum_copy(k):
        return pltpu.make_async_remote_copy(
            moved, sums.at[k], side_send.at[1], sum_recv.at[0],
            device_id=peer(k), device_id_type=MESH,
        )

    def start_sum(k, carry):
        sum_copy(k).start()
        return carry

    def add_sum(k, carry):
        return carry + sums[k]

    lax.fori_loop(1, peers, start_sum, 0)

    @pl.when(middle)
    def _():
        for g, k in pairs:
            if (g, k) not in middle_early:
                in_copy(g, k).start()

    hi, lo = split(weight * innov)
    aims = jnp.dot(jnp.concatenate([hi, lo], axis=0), anoms_t[...], preferred_element_type=F32)
    target[...] = aims[:domains, :LANES] + aims[:domains, LANES:] + aims[domains:, :LANES]

    def gram_group(g, carry):
        for d in range(2):
            c = g * 2 + d
            hi, lo = split(anoms[...] * weights[pl.ds(c, 1), :])
            prod = jnp.dot(
                jnp.concatenate([hi, lo], axis=0), anoms_t[...], preferred_element_type=F32
            )
            gram[c] = prod[:lines, :LANES] + prod[:lines, LANES:] + prod[lines:, :LANES]
        return carry

    with jax.named_scope("gram"):
        lax.fori_loop(0, domains // 4, gram_group, 0)

    @pl.when(outer)
    def _():
        for g, k in pairs:
            if (g, k) not in outer_early:
                in_copy(g, k).start()

    with jax.named_scope("gram"):
        lax.fori_loop(domains // 4, domains // 2, gram_group, 0)

    with jax.named_scope("w_sums"):
        if peers > 1:
            others = sums.at[pl.ds(1, peers - 1)]
            landed(others, side_send.at[1])
            landed(others, sum_recv.at[0])
        sums_all = lax.fori_loop(1, peers, add_sum, moved[...])

    scale = sums_all[:, 1:2] / sums_all[:, 0:1]
    eye = jnp.where(
        lax.broadcasted_iota(jnp.int32, (lines, LANES), 0)
        == lax.broadcasted_iota(jnp.int32, (lines, LANES), 1),
        1.0, 0.0,
    )
    diagonal = eye * scale

    def solve_group(g, carry):
        ids = [g * GROUP + d for d in range(GROUP)]
        mats = [gram[c] + diagonal for c in ids]
        bounds = [
            jnp.max(jnp.sum(jnp.abs(m), axis=0, keepdims=True), axis=1, keepdims=True)
            for m in mats
        ]
        ys = [m / b for m, b in zip(mats, bounds)]
        zs = [1.5 * eye - 0.5 * y for y in ys]
        ys = [times(y, z) for y, z in zip(ys, zs)]
        for step in range(1, NS_STEPS):
            ps = [1.5 * eye - 0.5 * times(z, y) for z, y in zip(zs, ys)]
            if step < NS_STEPS - 1:
                both = [
                    times(jnp.concatenate([y, z], axis=0), p) for y, z, p in zip(ys, zs, ps)
                ]
                ys = [b[:lines] for b in both]
                zs = [b[lines:] for b in both]
            else:
                zs = [times(z, p) for z, p in zip(zs, ps)]
        roots = [z * lax.rsqrt(b) for z, b in zip(zs, bounds)]
        for c, root in zip(ids, roots):
            half_gain = jnp.sum(root * target[pl.ds(c, 1), :], axis=1, keepdims=True)
            gain = jnp.sum(root * half_gain, axis=0, keepdims=True)
            w = (lines - 1.0) ** 0.5 * root + gain
            w = w - jnp.sum(w, axis=1, keepdims=True) * (1.0 / lines) + 1.0 / lines
            trans[c] = w.astype(BF16)
        return carry

    if staged:
        beyond = list(range(half_chips, chips)) + list(range(1, half_chips))
        receivers = [
            partner(chip, j, chips) * cores + c for j in beyond for c in reversed(range(cores))
        ] + [chip * cores + lax.rem(core + t, cores) for t in range(1, cores)]
    else:
        receivers = [partner(me, k, n) for k in far_first]

    def out_views(to, g):
        return (
            updated.at[pl.ds(to * members, members), pl.ds(g * CHUNK, CHUNK), :],
            out.at[:, pl.ds(pl.multiple_of(me * domains + g * CHUNK, 16), CHUNK), :],
        )

    def out_copy(g, to):
        source, place = out_views(to, g)
        return pltpu.make_async_remote_copy(
            source, place, side_send.at[0], out_recv.at[0],
            device_id={"member": to}, device_id_type=MESH,
        )

    for g in range(chunks):
        with jax.named_scope(f'solve{g}'):
            lax.fori_loop(g * CHUNK // GROUP, (g + 1) * CHUNK // GROUP, solve_group, 0)
        with jax.named_scope(f'w_in{g}'):
            landed(incoming.at[:, pl.ds(g * CHUNK, CHUNK), :], in_recv.at[g])
        states = jnp.swapaxes(incoming[:, g * CHUNK : (g + 1) * CHUNK, :].astype(F32), 0, 1)
        states = states.astype(BF16)
        results = [
            jnp.dot(trans[g * CHUNK + c][:, :lines], states[c], preferred_element_type=F32)
            for c in range(CHUNK)
        ]
        results = jnp.stack(results, axis=0)
        updated[:, g * CHUNK : (g + 1) * CHUNK, :] = jnp.swapaxes(results, 0, 1).astype(BF16)
        for to in receivers:
            out_copy(g, to).start()
        source, place = out_views(me, g)
        pltpu.make_async_copy(source, place, out_recv.at[0]).start()

    with jax.named_scope("w_out"):
        landed(out, out_recv.at[0])
    with jax.named_scope("w_sent"):
        if n > 1:
            landed(x.at[:, pl.ds(0, patch - domains), :], in_send.at[0])
            landed(updated.at[pl.ds(0, lines - members)], side_send.at[0])


def per_device(trials, sensors, readings, noises, lists, tiers):
    n, spaces = lax.axis_size("member"), lax.axis_size("space")
    members, patch, quantities = trials.shape
    obs_count = lists.shape[1]
    halo = 5 * obs_count // 2
    domains = patch // n
    chunks = domains // CHUNK
    lines = members * n
    width = -(-(domains + 2 * halo) // 256) * 256
    vmem = pl.BlockSpec(memory_space=pltpu.VMEM)
    anywhere = pl.BlockSpec(memory_space=pltpu.HBM)
    packed = -(-members * (patch // LANES) // 16) * 16
    full_rows = -(-(lines + 2) // 8) * 8
    dma = pltpu.SemaphoreType.DMA
    return pl.pallas_call(
        functools.partial(analyse_kernel, n, spaces, halo, obs_count),
        out_shape=pltpu.VMEM((members, patch, quantities), BF16),
        in_specs=[anywhere] * 6,
        out_specs=vmem,
        scratch_shapes=[
            pltpu.SemaphoreType.REGULAR,
            pltpu.VMEM((members, patch), BF16),
            pltpu.VMEM((patch,), BF16),
            pltpu.VMEM((patch,), BF16),
            pltpu.VMEM((patch,), BF16),
            pltpu.VMEM((patch,), BF16),
            pltpu.VMEM((patch,), BF16),
            pltpu.VMEM((patch,), BF16),
            pltpu.VMEM((domains, obs_count), jnp.int32),
            pltpu.VMEM((patch,), jnp.int32),
            dma((5,)), dma((2,)),
            pltpu.VMEM((members, CHUNK, quantities), BF16),
            pltpu.VMEM((lines, domains, quantities), BF16),
            pltpu.VMEM((lines, domains, quantities), BF16),
            pltpu.VMEM((3, n, packed, LANES), BF16),
            pltpu.VMEM((full_rows, 3 * patch), F32),
            pltpu.VMEM((lines, width), F32),
            pltpu.VMEM((width, 2 * LANES), BF16),
            pltpu.VMEM((domains, width), F32),
            pltpu.VMEM((domains, width), F32),
            pltpu.VMEM((domains, lines, LANES), F32),
            pltpu.VMEM((domains, LANES), F32),
            pltpu.VMEM((domains, lines, LANES), BF16),
            pltpu.VMEM((1, LANES), F32),
            pltpu.VMEM((n * spaces, 1, LANES), F32),
            dma((1,)), dma((chunks,)), dma((1,)),
            dma((2, 2)), dma((max(n // 4 - 1, 1),)), dma((2,)), dma((3,)), dma((3,)), dma((1,)),
        ],
        compiler_params=pltpu.CompilerParams(
            collective_id=0, has_side_effects=True, vmem_limit_bytes=40 << 20
        ),
        name="analyse",
    )(*[pltpu.with_memory_space_constraint(a, pltpu.HBM) for a in (trials, sensors, readings, noises, lists, tiers)])


def solution(mesh):
    return jax.shard_map(
        per_device,
        mesh=mesh,
        in_specs=(
            P("member", ("region", "space"), None),
            P("member", ("region", "space")),
            P(("region", "space")),
            P(("region", "space")),
            P(("region", "space"), None),
            P(("region", "space")),
        ),
        out_specs=P("member", ("region", "space"), None),
        check_vma=False,
    )
```

```python
import functools

import jax
import jax.numpy as jnp
from jax import lax
from jax.experimental import pallas as pl
from jax.experimental.pallas import tpu as pltpu
from jax.sharding import PartitionSpec as P

NS_STEPS = 4
LANES = 128
GROUP = 4
CHUNK = 16
MESH = pl.DeviceIdType.MESH
F32 = jnp.float32
BF16 = jnp.bfloat16


def partner(me, k, n):
    if n & (n - 1):
        return lax.rem(me + k, n)
    other, bit = me, 1
    while bit < n:
        if k & bit:
            other = other + bit * (1 - 2 * lax.rem(me // bit, 2))
        bit *= 2
    return other


def split(value):
    high = value.astype(BF16)
    return high, (value - high.astype(F32)).astype(BF16)


def times(left, right):
    lh, ll = split(left)
    rh, rl = split(right)
    rows, k = left.shape[0], right.shape[0]
    lhs = jnp.concatenate([lh, ll], axis=0)[:, :k]
    rhs = jnp.concatenate([rh, rl], axis=1)
    out = jnp.dot(lhs, rhs, preferred_element_type=F32)
    width = right.shape[1]
    return out[:rows, :width] + out[:rows, width:] + out[rows:, :width]


def analyse_kernel(
    n, spaces, halo, obs_count, x, sensors_in, readings_in, noises_in, lists_in, tiers_in,
    out,
    entered, sensors, readings, noises, left_readings, left_noises, right_readings, right_noises, lists, tiers, small_sem, stage_sem, stage, incoming, updated, gathered, full, anoms, anoms_t, marks, weights, gram, target, trans,
    moved, sums,
    in_send, in_recv, out_recv, near_recv, chip_send, chip_recv, side_send, side_recv, sum_recv,
):
    me = lax.axis_index("member")
    space = lax.axis_index("space")
    members, patch, _ = x.shape
    domains = patch // n
    lines = members * n
    width = anoms.shape[1]
    chunks = domains // CHUNK
    peers = n * spaces
    cores = 2 - n % 2
    chips = n // cores
    core, chip = lax.rem(me, cores), me // cores

    def landed(ref, sem):
        pltpu.make_async_copy(ref, ref, sem).wait()

    def slot(member):
        return lax.rem(member, cores) * chips + member // cores

    staged = n > 2 * cores and n & (n - 1) == 0
    low = n // 2 - cores if staged else n
    span = 2 * cores

    def central(member):
        return (member >= low) & (member < low + span)

    def in_views(to, g):
        return (
            x.at[:, pl.ds(pl.multiple_of(to * domains + g * CHUNK, 16), CHUNK), :],
            incoming.at[pl.ds(me * members, members), pl.ds(g * CHUNK, CHUNK), :],
        )

    lead = 1
    stage_parts = [pl.ds(0, lead), pl.ds(lead, members - lead)]
    middle = central(me)
    outer = jnp.logical_not(middle)
    barrier = pltpu.get_barrier_semaphore()

    def peer(k):
        other = lax.rem(me + space * n + k, peers)
        return {"member": lax.rem(other, n), "space": other // n}

    @pl.when(middle)
    def _():
        other = partner(me, n - cores, n)
        pl.semaphore_signal(barrier, inc=1, device_id={"member": other}, device_id_type=MESH)
        source, _ = in_views(other, 0)
        for i, rows in enumerate(stage_parts):
            pltpu.make_async_copy(source.at[rows], stage.at[rows], stage_sem.at[i]).start()

    half_chips = chips // 2
    upper = chip >= half_chips

    small = [
        pltpu.make_async_copy(source, place, small_sem.at[i])
        for i, (source, place) in enumerate(
            [
                (sensors_in, sensors), (readings_in, readings), (noises_in, noises),
                (lists_in.at[pl.ds(pl.multiple_of(me * domains, 8), domains)], lists),
                (tiers_in, tiers),
            ]
        )
    ]
    for copy in small:
        copy.start()

    def greet(k, carry):
        other = peer(k)

        @pl.when(jnp.logical_not(central(other["member"])))
        def _():
            pl.semaphore_signal(barrier, inc=1, device_id=other, device_id_type=MESH)

        return carry

    lax.fori_loop(1, peers, greet, 0)
    lane = lax.broadcasted_iota(jnp.int32, (obs_count, width), 1)

    def mark(group, carry):
        start = pl.multiple_of(group * 8, 8)
        columns = jnp.transpose(lists[pl.ds(start, 8), :] - me * domains)
        found = []
        for d in range(8):
            hit = columns[:, d : d + 1] == lane
            found.append(jnp.sum(jnp.where(hit, 1.0, 0.0), axis=0, keepdims=True))
        marks[pl.ds(start, 8), :] = jnp.concatenate(found, axis=0)
        return carry

    def marking(first, last):
        with jax.named_scope("marks"):
            lax.fori_loop(first, last, mark, 0)

    has_left, has_right = space > 0, space < spaces - 1

    def to_space(side):
        return lax.rem(space + 1 - side + spaces, spaces)

    strips = patch // LANES

    def pack():
        small[0].wait()
        values = sensors[...].astype(F32)
        rows = [values[:, LANES * t : LANES * (t + 1)] for t in range(strips)]
        spare = gathered.shape[2] - members * strips
        if spare:
            rows.append(jnp.zeros((spare, LANES), F32))
        gathered[1, slot(me)] = jnp.concatenate(rows, axis=0).astype(BF16)

    def slot_copy(other, half):
        place = gathered.at[1, slot(me)]
        return pltpu.make_async_remote_copy(
            place, place, small_sem.at[0], chip_recv.at[half],
            device_id={"member": other * cores + core}, device_id_type=MESH,
        )

    def near_slots():
        for j in range(1, half_chips if staged else chips):
            slot_copy(partner(chip, j, chips), 0).start()

    def cross_slot():
        if staged:
            slot_copy(half_chips - upper.astype(jnp.int32), 1).start()

    def relay_copy(j):
        rows = pl.ds(core * chips + (1 - upper.astype(jnp.int32)) * half_chips, half_chips)
        return pltpu.make_async_remote_copy(
            gathered.at[1, rows], gathered.at[1, rows], chip_send.at[j - 1], chip_recv.at[1],
            device_id={"member": partner(chip, j, chips) * cores + core}, device_id_type=MESH,
        )

    singles = [(left_readings, left_noises), (readings, noises), (right_readings, right_noises)]

    def near_copies(side):
        index = side // 2
        return [
            pltpu.make_async_remote_copy(
                source, place, small_sem.at[1 + 2 * index + i], near_recv.at[index, i],
                device_id={"space": to_space(side)}, device_id_type=MESH,
            )
            for i, (source, place) in enumerate(zip((readings_in, noises_in), singles[side]))
        ]

    def side_copy(side, t):
        rows = pl.ds(core * chips, chips)
        return pltpu.make_async_remote_copy(
            gathered.at[1, rows], gathered.at[side, rows],
            side_send.at[side], side_recv.at[side],
            device_id={"member": chip * cores + lax.rem(core + t, cores), "space": to_space(side)},
            device_id_type=MESH,
        )

    def in_copy(g, k, rows=None):
        to = partner(me, k, n)
        source, place = in_views(to, g)
        if rows is not None:
            source, place = stage.at[rows], place.at[rows]
        return pltpu.make_async_remote_copy(
            source, place, in_send.at[0], in_recv.at[g],
            device_id={"member": to}, device_id_type=MESH,
        )

    far = list(range(n // 2, n))
    close = list(range(1, n // 2))
    far_first = far + close
    pairs = [(g, k) for g in range(chunks) for k in far_first]
    facing = [(g, n - cores) for g in range(chunks)]
    crossed = [(g, k) for g in range(chunks) for k in range(n - cores + 1, n)]
    relayed = [(0, k) for k in close]
    middle_early = facing + crossed + relayed
    outer_early = [(g, k) for g in range(chunks) for k in close]
    half = domains // 16

    def start_near():
        @pl.when(has_right)
        def _():
            for copy in near_copies(0):
                copy.start()

        @pl.when(has_left)
        def _():
            for copy in near_copies(2):
                copy.start()

    def start_own():
        for g in range(chunks):
            source, place = in_views(me, g)
            pltpu.make_async_copy(source, place, in_recv.at[g]).start()

    @pl.when(middle)
    def _():
        with jax.named_scope("w_middle"):
            pl.semaphore_wait(barrier, 1)
        for i, rows in enumerate(stage_parts):
            landed(stage.at[rows], stage_sem.at[i])
            in_copy(*facing[0], rows).start()
        pack()
        cross_slot()
        for g, k in facing[1:]:
            in_copy(g, k).start()
        start_own()
        for copy in small[1:]:
            copy.wait()
        marking(0, half)
        with jax.named_scope("w_entered"):
            pl.semaphore_wait(entered, 1)
        near_slots()
        start_near()
        for g, k in crossed:
            in_copy(g, k).start()

    @pl.when(outer)
    def _():
        with jax.named_scope("w_barrier"):
            pl.semaphore_wait(barrier, peers - 1)
        if staged:
            @pl.when((me >= low + span) & (me < low + span + cores))
            def _():
                for j in range(1, 3):
                    pl.semaphore_signal(
                        entered, inc=1, device_id={"member": me - j * cores}, device_id_type=MESH
                    )
        pack()
        cross_slot()
        near_slots()
        for g, k in outer_early:
            in_copy(g, k).start()
        start_own()
        for copy in small[1:]:
            copy.wait()
        start_near()
        marking(0, half)

    for side, missing in ((0, space == 0), (2, space == spaces - 1)):
        @pl.when(missing)
        def _():
            gathered[side] = jnp.ones(gathered.shape[1:], BF16)
            for single in singles[side]:
                single[...] = jnp.ones(single.shape, BF16)

    marking(half, domains // 8)

    with jax.named_scope("w_chip"):
        if staged:
            landed(gathered.at[1, pl.ds(0, half_chips)], chip_recv.at[1])

            @pl.when(middle)
            def _():
                for j in range(1, half_chips):
                    relay_copy(j).start()
                for g, k in relayed:
                    in_copy(g, k).start()
        near = half_chips - 1 if staged else chips - 1
        if near:
            landed(gathered.at[1, pl.ds(0, near)], chip_recv.at[0])

    for t in range(1, cores):
        side_copy(1, t).start()

    @pl.when(has_right)
    def _():
        for t in range(cores):
            side_copy(0, t).start()

    @pl.when(has_left)
    def _():
        for t in range(cores):
            side_copy(2, t).start()

    with jax.named_scope("w_side"):
        sent = half_chips if staged else chips - 1
        if sent:
            landed(gathered.at[1, pl.ds(0, sent)], small_sem.at[0])
        if staged:
            @pl.when(middle)
            def _():
                for j in range(1, half_chips):
                    relay_copy(j).wait_send()
        if cores > 1:
            others = gathered.at[1, pl.ds(0, n - chips)]
            landed(others, side_send.at[1])
            landed(others, side_recv.at[1])

        @pl.when(has_right)
        def _():
            for copy in near_copies(0):
                copy.wait_send()
            for copy in near_copies(2):
                copy.wait_recv()
            landed(gathered.at[1], side_send.at[0])
            landed(gathered.at[2], side_recv.at[2])

        @pl.when(has_left)
        def _():
            for copy in near_copies(2):
                copy.wait_send()
            for copy in near_copies(0):
                copy.wait_recv()
            landed(gathered.at[1], side_send.at[2])
            landed(gathered.at[0], side_recv.at[0])

    for side in range(3):
        for s in range(n):
            rows = gathered[side, s % cores * chips + s // cores].astype(F32)
            for t in range(strips):
                at = patch * side + LANES * t
                full[members * s : members * (s + 1), at : at + LANES] = (
                    rows[members * t : members * (t + 1)]
                )
        for i, single in enumerate(singles[side]):
            full[lines + i : lines + i + 1, patch * side : patch * (side + 1)] = (
                single[...].astype(F32)[None]
            )
    total = 3 * patch
    shift = lax.rem(2 * total - (patch - halo) - me * domains, total)
    turned = pltpu.roll(full[...], shift, 1)[:, :width]
    values = turned[:lines]
    mean = jnp.sum(values, axis=0, keepdims=True) * (1.0 / lines)
    anomaly = values - mean
    anoms[...] = anomaly
    innov = turned[lines : lines + 1] - mean
    noise = turned[lines + 1 : lines + 2]
    squares = jnp.sum(anomaly * anomaly, axis=0, keepdims=True)

    own_tier = lax.broadcasted_iota(jnp.int32, (domains, patch), 1) == (
        lax.broadcasted_iota(jnp.int32, (domains, patch), 0) + me * domains
    )
    tier = jnp.sum(jnp.where(own_tier, tiers[...].astype(F32)[None], 0.0), axis=1, keepdims=True)
    radius = (tier + 2.0) * (0.5 * obs_count)
    place = lax.broadcasted_iota(jnp.int32, (domains, width), 1)
    row = lax.broadcasted_iota(jnp.int32, (domains, width), 0)
    distance = jnp.abs(place - halo - row).astype(F32) / radius
    weight = marks[...] * jnp.exp(-2.0 * distance * distance) / noise
    weights[...] = weight
    fit = jnp.sum(weight * (innov * innov))
    spread = jnp.sum(weight * squares)
    first = lax.broadcasted_iota(jnp.int32, (1, LANES), 1) == 0
    moved[...] = jnp.where(first, fit, spread)

    high, low = split(anomaly)
    pad = jnp.zeros((LANES - lines, width), F32)
    anoms_t[...] = jnp.concatenate(
        [
            jnp.transpose(jnp.concatenate([high.astype(F32), pad], axis=0)),
            jnp.transpose(jnp.concatenate([low.astype(F32), pad], axis=0)),
        ],
        axis=1,
    ).astype(BF16)

    def sum_copy(k):
        return pltpu.make_async_remote_copy(
            moved, sums.at[k], side_send.at[1], sum_recv.at[0],
            device_id=peer(k), device_id_type=MESH,
        )

    def start_sum(k, carry):
        sum_copy(k).start()
        return carry

    def add_sum(k, carry):
        return carry + sums[k]

    lax.fori_loop(1, peers, start_sum, 0)

    @pl.when(middle)
    def _():
        for g, k in pairs:
            if (g, k) not in middle_early:
                in_copy(g, k).start()

    hi, lo = split(weight * innov)
    aims = jnp.dot(jnp.concatenate([hi, lo], axis=0), anoms_t[...], preferred_element_type=F32)
    target[...] = aims[:domains, :LANES] + aims[:domains, LANES:] + aims[domains:, :LANES]

    def gram_group(g, carry):
        for d in range(2):
            c = g * 2 + d
            hi, lo = split(anoms[...] * weights[pl.ds(c, 1), :])
            prod = jnp.dot(
                jnp.concatenate([hi, lo], axis=0), anoms_t[...], preferred_element_type=F32
            )
            gram[c] = prod[:lines, :LANES] + prod[:lines, LANES:] + prod[lines:, :LANES]
        return carry

    with jax.named_scope("gram"):
        lax.fori_loop(0, domains // 4, gram_group, 0)

    @pl.when(outer)
    def _():
        for g, k in pairs:
            if (g, k) not in outer_early:
                in_copy(g, k).start()

    with jax.named_scope("gram"):
        lax.fori_loop(domains // 4, domains // 2, gram_group, 0)

    with jax.named_scope("w_sums"):
        if peers > 1:
            others = sums.at[pl.ds(1, peers - 1)]
            landed(others, side_send.at[1])
            landed(others, sum_recv.at[0])
        sums_all = lax.fori_loop(1, peers, add_sum, moved[...])

    scale = sums_all[:, 1:2] / sums_all[:, 0:1]
    eye = jnp.where(
        lax.broadcasted_iota(jnp.int32, (lines, LANES), 0)
        == lax.broadcasted_iota(jnp.int32, (lines, LANES), 1),
        1.0, 0.0,
    )
    diagonal = eye * scale

    def solve_group(g, carry):
        ids = [g * GROUP + d for d in range(GROUP)]
        mats = [gram[c] + diagonal for c in ids]
        bounds = [
            jnp.max(jnp.sum(jnp.abs(m), axis=0, keepdims=True), axis=1, keepdims=True)
            for m in mats
        ]
        ys = [m / b for m, b in zip(mats, bounds)]
        zs = [1.5 * eye - 0.5 * y for y in ys]
        ys = [times(y, z) for y, z in zip(ys, zs)]
        for step in range(1, NS_STEPS):
            ps = [1.5 * eye - 0.5 * times(z, y) for z, y in zip(zs, ys)]
            if step < NS_STEPS - 1:
                both = [
                    times(jnp.concatenate([y, z], axis=0), p) for y, z, p in zip(ys, zs, ps)
                ]
                ys = [b[:lines] for b in both]
                zs = [b[lines:] for b in both]
            else:
                zs = [times(z, p) for z, p in zip(zs, ps)]
        roots = [z * lax.rsqrt(b) for z, b in zip(zs, bounds)]
        for c, root in zip(ids, roots):
            half_gain = jnp.sum(root * target[pl.ds(c, 1), :], axis=1, keepdims=True)
            gain = jnp.sum(root * half_gain, axis=0, keepdims=True)
            w = (lines - 1.0) ** 0.5 * root + gain
            w = w - jnp.sum(w, axis=1, keepdims=True) * (1.0 / lines) + 1.0 / lines
            trans[c] = w.astype(BF16)
        return carry

    if staged:
        beyond = list(range(half_chips, chips)) + list(range(1, half_chips))
        receivers = [
            partner(chip, j, chips) * cores + c for j in beyond for c in reversed(range(cores))
        ] + [chip * cores + lax.rem(core + t, cores) for t in range(1, cores)]
    else:
        receivers = [partner(me, k, n) for k in far_first]

    def out_views(to, g):
        return (
            updated.at[pl.ds(to * members, members), pl.ds(g * CHUNK, CHUNK), :],
            out.at[:, pl.ds(pl.multiple_of(me * domains + g * CHUNK, 16), CHUNK), :],
        )

    def out_copy(g, to):
        source, place = out_views(to, g)
        return pltpu.make_async_remote_copy(
            source, place, side_send.at[0], out_recv.at[0],
            device_id={"member": to}, device_id_type=MESH,
        )

    for g in range(chunks):
        with jax.named_scope(f'solve{g}'):
            lax.fori_loop(g * CHUNK // GROUP, (g + 1) * CHUNK // GROUP, solve_group, 0)
        with jax.named_scope(f'w_in{g}'):
            landed(incoming.at[:, pl.ds(g * CHUNK, CHUNK), :], in_recv.at[g])
        states = jnp.swapaxes(incoming[:, g * CHUNK : (g + 1) * CHUNK, :].astype(F32), 0, 1)
        states = states.astype(BF16)
        results = [
            jnp.dot(trans[g * CHUNK + c][:, :lines], states[c], preferred_element_type=F32)
            for c in range(CHUNK)
        ]
        results = jnp.stack(results, axis=0)
        updated[:, g * CHUNK : (g + 1) * CHUNK, :] = jnp.swapaxes(results, 0, 1).astype(BF16)
        for to in receivers:
            out_copy(g, to).start()
        source, place = out_views(me, g)
        pltpu.make_async_copy(source, place, out_recv.at[0]).start()

    with jax.named_scope("w_out"):
        landed(out, out_recv.at[0])
    with jax.named_scope("w_sent"):
        if n > 1:
            landed(x.at[:, pl.ds(0, patch - domains), :], in_send.at[0])
            landed(updated.at[pl.ds(0, lines - members)], side_send.at[0])


def per_device(trials, sensors, readings, noises, lists, tiers):
    n, spaces = lax.axis_size("member"), lax.axis_size("space")
    members, patch, quantities = trials.shape
    obs_count = lists.shape[1]
    halo = 5 * obs_count // 2
    domains = patch // n
    chunks = domains // CHUNK
    lines = members * n
    width = -(-(domains + 2 * halo) // 256) * 256
    vmem = pl.BlockSpec(memory_space=pltpu.VMEM)
    anywhere = pl.BlockSpec(memory_space=pltpu.HBM)
    packed = -(-members * (patch // LANES) // 16) * 16
    full_rows = -(-(lines + 2) // 8) * 8
    dma = pltpu.SemaphoreType.DMA
    return pl.pallas_call(
        functools.partial(analyse_kernel, n, spaces, halo, obs_count),
        out_shape=pltpu.VMEM((members, patch, quantities), BF16),
        in_specs=[anywhere] * 6,
        out_specs=vmem,
        scratch_shapes=[
            pltpu.SemaphoreType.REGULAR,
            pltpu.VMEM((members, patch), BF16),
            pltpu.VMEM((patch,), BF16),
            pltpu.VMEM((patch,), BF16),
            pltpu.VMEM((patch,), BF16),
            pltpu.VMEM((patch,), BF16),
            pltpu.VMEM((patch,), BF16),
            pltpu.VMEM((patch,), BF16),
            pltpu.VMEM((domains, obs_count), jnp.int32),
            pltpu.VMEM((patch,), jnp.int32),
            dma((5,)), dma((2,)),
            pltpu.VMEM((members, CHUNK, quantities), BF16),
            pltpu.VMEM((lines, domains, quantities), BF16),
            pltpu.VMEM((lines, domains, quantities), BF16),
            pltpu.VMEM((3, n, packed, LANES), BF16),
            pltpu.VMEM((full_rows, 3 * patch), F32),
            pltpu.VMEM((lines, width), F32),
            pltpu.VMEM((width, 2 * LANES), BF16),
            pltpu.VMEM((domains, width), F32),
            pltpu.VMEM((domains, width), F32),
            pltpu.VMEM((domains, lines, LANES), F32),
            pltpu.VMEM((domains, LANES), F32),
            pltpu.VMEM((domains, lines, LANES), BF16),
            pltpu.VMEM((1, LANES), F32),
            pltpu.VMEM((n * spaces, 1, LANES), F32),
            dma((1,)), dma((chunks,)), dma((1,)),
            dma((2, 2)), dma((max(n // 4 - 1, 1),)), dma((2,)), dma((3,)), dma((3,)), dma((1,)),
        ],
        compiler_params=pltpu.CompilerParams(
            collective_id=0, has_side_effects=True, vmem_limit_bytes=40 << 20
        ),
        name="analyse",
    )(*[pltpu.with_memory_space_constraint(a, pltpu.HBM) for a in (trials, sensors, readings, noises, lists, tiers)])


def solution(mesh):
    return jax.shard_map(
        per_device,
        mesh=mesh,
        in_specs=(
            P("member", ("region", "space"), None),
            P("member", ("region", "space")),
            P(("region", "space")),
            P(("region", "space")),
            P(("region", "space"), None),
            P(("region", "space")),
        ),
        out_specs=P("member", ("region", "space"), None),
        check_vma=False,
    )
```

```python
import functools

import jax
import jax.numpy as jnp
from jax import lax
from jax.experimental import pallas as pl
from jax.experimental.pallas import tpu as pltpu
from jax.sharding import PartitionSpec as P

NS_STEPS = 4
LANES = 128
GROUP = 4
CHUNK = 16
MESH = pl.DeviceIdType.MESH
F32 = jnp.float32
BF16 = jnp.bfloat16


def partner(me, k, n):
    if n & (n - 1):
        return lax.rem(me + k, n)
    other, bit = me, 1
    while bit < n:
        if k & bit:
            other = other + bit * (1 - 2 * lax.rem(me // bit, 2))
        bit *= 2
    return other


def split(value):
    high = value.astype(BF16)
    return high, (value - high.astype(F32)).astype(BF16)


def times(left, right):
    lh, ll = split(left)
    rh, rl = split(right)
    rows, k = left.shape[0], right.shape[0]
    lhs = jnp.concatenate([lh, ll], axis=0)[:, :k]
    rhs = jnp.concatenate([rh, rl], axis=1)
    out = jnp.dot(lhs, rhs, preferred_element_type=F32)
    width = right.shape[1]
    return out[:rows, :width] + out[:rows, width:] + out[rows:, :width]


def analyse_kernel(
    n, spaces, halo, obs_count, x, sensors_in, readings_in, noises_in, lists_in, tiers_in,
    out,
    entered, sensors, readings, noises, left_readings, left_noises, right_readings, right_noises, lists, tiers, small_sem, stage_sem, stage, incoming, updated, gathered, full, anoms, anoms_t, marks, weights, gram, target, trans,
    moved, sums,
    in_send, in_recv, out_recv, near_recv, chip_send, chip_recv, side_send, side_recv, sum_recv,
):
    me = lax.axis_index("member")
    space = lax.axis_index("space")
    members, patch, _ = x.shape
    domains = patch // n
    lines = members * n
    width = anoms.shape[1]
    chunks = domains // CHUNK
    peers = n * spaces
    cores = 2 - n % 2
    chips = n // cores
    core, chip = lax.rem(me, cores), me // cores

    def landed(ref, sem):
        pltpu.make_async_copy(ref, ref, sem).wait()

    def slot(member):
        return lax.rem(member, cores) * chips + member // cores

    staged = n > 2 * cores and n & (n - 1) == 0
    low = n // 2 - cores if staged else n
    span = 2 * cores

    def central(member):
        return (member >= low) & (member < low + span)

    def in_views(to, g):
        return (
            x.at[:, pl.ds(pl.multiple_of(to * domains + g * CHUNK, 16), CHUNK), :],
            incoming.at[pl.ds(me * members, members), pl.ds(g * CHUNK, CHUNK), :],
        )

    lead = 1
    stage_parts = [pl.ds(0, lead), pl.ds(lead, members - lead)]
    middle = central(me)
    outer = jnp.logical_not(middle)
    barrier = pltpu.get_barrier_semaphore()

    def peer(k):
        other = lax.rem(me + space * n + k, peers)
        return {"member": lax.rem(other, n), "space": other // n}

    @pl.when(middle)
    def _():
        other = partner(me, n - cores, n)
        pl.semaphore_signal(barrier, inc=1, device_id={"member": other}, device_id_type=MESH)
        source, _ = in_views(other, 0)
        for i, rows in enumerate(stage_parts):
            pltpu.make_async_copy(source.at[rows], stage.at[rows], stage_sem.at[i]).start()

    half_chips = chips // 2
    upper = chip >= half_chips

    small = [
        pltpu.make_async_copy(source, place, small_sem.at[i])
        for i, (source, place) in enumerate(
            [
                (sensors_in, sensors), (readings_in, readings), (noises_in, noises),
                (lists_in.at[pl.ds(pl.multiple_of(me * domains, 8), domains)], lists),
                (tiers_in, tiers),
            ]
        )
    ]
    for copy in small:
        copy.start()

    def greet(k, carry):
        other = peer(k)

        @pl.when(jnp.logical_not(central(other["member"])))
        def _():
            pl.semaphore_signal(barrier, inc=1, device_id=other, device_id_type=MESH)

        return carry

    lax.fori_loop(1, peers, greet, 0)
    lane = lax.broadcasted_iota(jnp.int32, (obs_count, width), 1)

    def mark(group, carry):
        start = pl.multiple_of(group * 8, 8)
        columns = jnp.transpose(lists[pl.ds(start, 8), :] - me * domains)
        found = []
        for d in range(8):
            hit = columns[:, d : d + 1] == lane
            found.append(jnp.sum(jnp.where(hit, 1.0, 0.0), axis=0, keepdims=True))
        marks[pl.ds(start, 8), :] = jnp.concatenate(found, axis=0)
        return carry

    def marking(first, last):
        with jax.named_scope("marks"):
            lax.fori_loop(first, last, mark, 0)

    has_left, has_right = space > 0, space < spaces - 1

    def to_space(side):
        return lax.rem(space + 1 - side + spaces, spaces)

    strips = patch // LANES

    def pack():
        small[0].wait()
        values = sensors[...].astype(F32)
        rows = [values[:, LANES * t : LANES * (t + 1)] for t in range(strips)]
        spare = gathered.shape[2] - members * strips
        if spare:
            rows.append(jnp.zeros((spare, LANES), F32))
        gathered[1, slot(me)] = jnp.concatenate(rows, axis=0).astype(BF16)

    def slot_copy(other, half):
        place = gathered.at[1, slot(me)]
        return pltpu.make_async_remote_copy(
            place, place, small_sem.at[0], chip_recv.at[half],
            device_id={"member": other * cores + core}, device_id_type=MESH,
        )

    def near_slots():
        for j in range(1, half_chips if staged else chips):
            slot_copy(partner(chip, j, chips), 0).start()

    def cross_slot():
        if staged:
            slot_copy(half_chips - upper.astype(jnp.int32), 1).start()

    def relay_copy(j):
        rows = pl.ds(core * chips + (1 - upper.astype(jnp.int32)) * half_chips, half_chips)
        return pltpu.make_async_remote_copy(
            gathered.at[1, rows], gathered.at[1, rows], chip_send.at[j - 1], chip_recv.at[1],
            device_id={"member": partner(chip, j, chips) * cores + core}, device_id_type=MESH,
        )

    singles = [(left_readings, left_noises), (readings, noises), (right_readings, right_noises)]

    def near_copies(side):
        index = side // 2
        return [
            pltpu.make_async_remote_copy(
                source, place, small_sem.at[1 + 2 * index + i], near_recv.at[index, i],
                device_id={"space": to_space(side)}, device_id_type=MESH,
            )
            for i, (source, place) in enumerate(zip((readings_in, noises_in), singles[side]))
        ]

    def side_copy(side, t):
        rows = pl.ds(core * chips, chips)
        return pltpu.make_async_remote_copy(
            gathered.at[1, rows], gathered.at[side, rows],
            side_send.at[side], side_recv.at[side],
            device_id={"member": chip * cores + lax.rem(core + t, cores), "space": to_space(side)},
            device_id_type=MESH,
        )

    def in_copy(g, k, rows=None):
        to = partner(me, k, n)
        source, place = in_views(to, g)
        if rows is not None:
            source, place = stage.at[rows], place.at[rows]
        return pltpu.make_async_remote_copy(
            source, place, in_send.at[0], in_recv.at[g],
            device_id={"member": to}, device_id_type=MESH,
        )

    far = list(range(n // 2, n))
    close = list(range(1, n // 2))
    far_first = far + close
    pairs = [(g, k) for g in range(chunks) for k in far_first]
    facing = [(g, n - cores) for g in range(chunks)]
    crossed = [(g, k) for g in range(chunks) for k in range(n - cores + 1, n)]
    relayed = [(0, k) for k in close]
    middle_early = facing + crossed + relayed
    outer_early = [(g, k) for g in range(chunks) for k in close]
    half = domains // 16

    def start_near():
        @pl.when(has_right)
        def _():
            for copy in near_copies(0):
                copy.start()

        @pl.when(has_left)
        def _():
            for copy in near_copies(2):
                copy.start()

    def start_own():
        for g in range(chunks):
            source, place = in_views(me, g)
            pltpu.make_async_copy(source, place, in_recv.at[g]).start()

    @pl.when(middle)
    def _():
        with jax.named_scope("w_middle"):
            pl.semaphore_wait(barrier, 1)
        for i, rows in enumerate(stage_parts):
            landed(stage.at[rows], stage_sem.at[i])
            in_copy(*facing[0], rows).start()
        pack()
        cross_slot()
        for g, k in facing[1:]:
            in_copy(g, k).start()
        start_own()
        for copy in small[1:]:
            copy.wait()
        marking(0, half)
        with jax.named_scope("w_entered"):
            pl.semaphore_wait(entered, 1)
        near_slots()
        start_near()
        for g, k in crossed:
            in_copy(g, k).start()

    @pl.when(outer)
    def _():
        with jax.named_scope("w_barrier"):
            pl.semaphore_wait(barrier, peers - 1)
        if staged:
            @pl.when((me >= low + span) & (me < low + span + cores))
            def _():
                for j in range(1, 3):
                    pl.semaphore_signal(
                        entered, inc=1, device_id={"member": me - j * cores}, device_id_type=MESH
                    )
        pack()
        cross_slot()
        near_slots()
        for g, k in outer_early:
            in_copy(g, k).start()
        start_own()
        for copy in small[1:]:
            copy.wait()
        start_near()
        marking(0, half)

    for side, missing in ((0, space == 0), (2, space == spaces - 1)):
        @pl.when(missing)
        def _():
            gathered[side] = jnp.ones(gathered.shape[1:], BF16)
            for single in singles[side]:
                single[...] = jnp.ones(single.shape, BF16)

    marking(half, domains // 8)

    with jax.named_scope("w_chip"):
        if staged:
            landed(gathered.at[1, pl.ds(0, half_chips)], chip_recv.at[1])

            @pl.when(middle)
            def _():
                for j in range(1, half_chips):
                    relay_copy(j).start()
                for g, k in relayed:
                    in_copy(g, k).start()
        near = half_chips - 1 if staged else chips - 1
        if near:
            landed(gathered.at[1, pl.ds(0, near)], chip_recv.at[0])

    for t in range(1, cores):
        side_copy(1, t).start()

    @pl.when(has_right)
    def _():
        for t in range(cores):
            side_copy(0, t).start()

    @pl.when(has_left)
    def _():
        for t in range(cores):
            side_copy(2, t).start()

    with jax.named_scope("w_side"):
        sent = half_chips if staged else chips - 1
        if sent:
            landed(gathered.at[1, pl.ds(0, sent)], small_sem.at[0])
        if staged:
            @pl.when(middle)
            def _():
                for j in range(1, half_chips):
                    relay_copy(j).wait_send()
        if cores > 1:
            others = gathered.at[1, pl.ds(0, n - chips)]
            landed(others, side_send.at[1])
            landed(others, side_recv.at[1])

        @pl.when(has_right)
        def _():
            for copy in near_copies(0):
                copy.wait_send()
            for copy in near_copies(2):
                copy.wait_recv()
            landed(gathered.at[1], side_send.at[0])
            landed(gathered.at[2], side_recv.at[2])

        @pl.when(has_left)
        def _():
            for copy in near_copies(2):
                copy.wait_send()
            for copy in near_copies(0):
                copy.wait_recv()
            landed(gathered.at[1], side_send.at[2])
            landed(gathered.at[0], side_recv.at[0])

    for side in range(3):
        for s in range(n):
            rows = gathered[side, s % cores * chips + s // cores].astype(F32)
            for t in range(strips):
                at = patch * side + LANES * t
                full[members * s : members * (s + 1), at : at + LANES] = (
                    rows[members * t : members * (t + 1)]
                )
        for i, single in enumerate(singles[side]):
            full[lines + i : lines + i + 1, patch * side : patch * (side + 1)] = (
                single[...].astype(F32)[None]
            )
    total = 3 * patch
    shift = lax.rem(2 * total - (patch - halo) - me * domains, total)
    turned = pltpu.roll(full[...], shift, 1)[:, :width]
    values = turned[:lines]
    mean = jnp.sum(values, axis=0, keepdims=True) * (1.0 / lines)
    anomaly = values - mean
    anoms[...] = anomaly
    innov = turned[lines : lines + 1] - mean
    noise = turned[lines + 1 : lines + 2]
    squares = jnp.sum(anomaly * anomaly, axis=0, keepdims=True)

    own_tier = lax.broadcasted_iota(jnp.int32, (domains, patch), 1) == (
        lax.broadcasted_iota(jnp.int32, (domains, patch), 0) + me * domains
    )
    tier = jnp.sum(jnp.where(own_tier, tiers[...].astype(F32)[None], 0.0), axis=1, keepdims=True)
    radius = (tier + 2.0) * (0.5 * obs_count)
    place = lax.broadcasted_iota(jnp.int32, (domains, width), 1)
    row = lax.broadcasted_iota(jnp.int32, (domains, width), 0)
    distance = jnp.abs(place - halo - row).astype(F32) / radius
    weight = marks[...] * jnp.exp(-2.0 * distance * distance) / noise
    weights[...] = weight
    fit = jnp.sum(weight * (innov * innov))
    spread = jnp.sum(weight * squares)
    first = lax.broadcasted_iota(jnp.int32, (1, LANES), 1) == 0
    moved[...] = jnp.where(first, fit, spread)

    high, low = split(anomaly)
    pad = jnp.zeros((LANES - lines, width), F32)
    anoms_t[...] = jnp.concatenate(
        [
            jnp.transpose(jnp.concatenate([high.astype(F32), pad], axis=0)),
            jnp.transpose(jnp.concatenate([low.astype(F32), pad], axis=0)),
        ],
        axis=1,
    ).astype(BF16)

    def sum_copy(k):
        return pltpu.make_async_remote_copy(
            moved, sums.at[k], side_send.at[1], sum_recv.at[0],
            device_id=peer(k), device_id_type=MESH,
        )

    def start_sum(k, carry):
        sum_copy(k).start()
        return carry

    def add_sum(k, carry):
        return carry + sums[k]

    lax.fori_loop(1, peers, start_sum, 0)

    @pl.when(middle)
    def _():
        for g, k in pairs:
            if (g, k) not in middle_early:
                in_copy(g, k).start()

    @pl.when(outer)
    def _():
        for g, k in pairs:
            if (g, k) not in outer_early:
                in_copy(g, k).start()

    hi, lo = split(weight * innov)
    aims = jnp.dot(jnp.concatenate([hi, lo], axis=0), anoms_t[...], preferred_element_type=F32)
    target[...] = aims[:domains, :LANES] + aims[:domains, LANES:] + aims[domains:, :LANES]

    def gram_group(g, carry):
        for d in range(2):
            c = g * 2 + d
            hi, lo = split(anoms[...] * weights[pl.ds(c, 1), :])
            prod = jnp.dot(
                jnp.concatenate([hi, lo], axis=0), anoms_t[...], preferred_element_type=F32
            )
            gram[c] = prod[:lines, :LANES] + prod[:lines, LANES:] + prod[lines:, :LANES]
        return carry

    with jax.named_scope("gram"):
        lax.fori_loop(0, domains // 4, gram_group, 0)

    with jax.named_scope("gram"):
        lax.fori_loop(domains // 4, domains // 2, gram_group, 0)

    with jax.named_scope("w_sums"):
        if peers > 1:
            others = sums.at[pl.ds(1, peers - 1)]
            landed(others, side_send.at[1])
            landed(others, sum_recv.at[0])
        sums_all = lax.fori_loop(1, peers, add_sum, moved[...])

    scale = sums_all[:, 1:2] / sums_all[:, 0:1]
    eye = jnp.where(
        lax.broadcasted_iota(jnp.int32, (lines, LANES), 0)
        == lax.broadcasted_iota(jnp.int32, (lines, LANES), 1),
        1.0, 0.0,
    )
    diagonal = eye * scale

    def solve_group(g, carry):
        ids = [g * GROUP + d for d in range(GROUP)]
        mats = [gram[c] + diagonal for c in ids]
        bounds = [
            jnp.max(jnp.sum(jnp.abs(m), axis=0, keepdims=True), axis=1, keepdims=True)
            for m in mats
        ]
        ys = [m / b for m, b in zip(mats, bounds)]
        zs = [1.5 * eye - 0.5 * y for y in ys]
        ys = [times(y, z) for y, z in zip(ys, zs)]
        for step in range(1, NS_STEPS):
            ps = [1.5 * eye - 0.5 * times(z, y) for z, y in zip(zs, ys)]
            if step < NS_STEPS - 1:
                both = [
                    times(jnp.concatenate([y, z], axis=0), p) for y, z, p in zip(ys, zs, ps)
                ]
                ys = [b[:lines] for b in both]
                zs = [b[lines:] for b in both]
            else:
                zs = [times(z, p) for z, p in zip(zs, ps)]
        roots = [z * lax.rsqrt(b) for z, b in zip(zs, bounds)]
        for c, root in zip(ids, roots):
            half_gain = jnp.sum(root * target[pl.ds(c, 1), :], axis=1, keepdims=True)
            gain = jnp.sum(root * half_gain, axis=0, keepdims=True)
            w = (lines - 1.0) ** 0.5 * root + gain
            w = w - jnp.sum(w, axis=1, keepdims=True) * (1.0 / lines) + 1.0 / lines
            trans[c] = w.astype(BF16)
        return carry

    if staged:
        beyond = list(range(half_chips, chips)) + list(range(1, half_chips))
        receivers = [
            partner(chip, j, chips) * cores + c for j in beyond for c in reversed(range(cores))
        ] + [chip * cores + lax.rem(core + t, cores) for t in range(1, cores)]
    else:
        receivers = [partner(me, k, n) for k in far_first]

    def out_views(to, g):
        return (
            updated.at[pl.ds(to * members, members), pl.ds(g * CHUNK, CHUNK), :],
            out.at[:, pl.ds(pl.multiple_of(me * domains + g * CHUNK, 16), CHUNK), :],
        )

    def out_copy(g, to):
        source, place = out_views(to, g)
        return pltpu.make_async_remote_copy(
            source, place, side_send.at[0], out_recv.at[0],
            device_id={"member": to}, device_id_type=MESH,
        )

    for g in range(chunks):
        with jax.named_scope(f'solve{g}'):
            lax.fori_loop(g * CHUNK // GROUP, (g + 1) * CHUNK // GROUP, solve_group, 0)
        with jax.named_scope(f'w_in{g}'):
            landed(incoming.at[:, pl.ds(g * CHUNK, CHUNK), :], in_recv.at[g])
        states = jnp.swapaxes(incoming[:, g * CHUNK : (g + 1) * CHUNK, :].astype(F32), 0, 1)
        states = states.astype(BF16)
        results = [
            jnp.dot(trans[g * CHUNK + c][:, :lines], states[c], preferred_element_type=F32)
            for c in range(CHUNK)
        ]
        results = jnp.stack(results, axis=0)
        updated[:, g * CHUNK : (g + 1) * CHUNK, :] = jnp.swapaxes(results, 0, 1).astype(BF16)
        for to in receivers:
            out_copy(g, to).start()
        source, place = out_views(me, g)
        pltpu.make_async_copy(source, place, out_recv.at[0]).start()

    with jax.named_scope("w_out"):
        landed(out, out_recv.at[0])
    with jax.named_scope("w_sent"):
        if n > 1:
            landed(x.at[:, pl.ds(0, patch - domains), :], in_send.at[0])
            landed(updated.at[pl.ds(0, lines - members)], side_send.at[0])


def per_device(trials, sensors, readings, noises, lists, tiers):
    n, spaces = lax.axis_size("member"), lax.axis_size("space")
    members, patch, quantities = trials.shape
    obs_count = lists.shape[1]
    halo = 5 * obs_count // 2
    domains = patch // n
    chunks = domains // CHUNK
    lines = members * n
    width = -(-(domains + 2 * halo) // 256) * 256
    vmem = pl.BlockSpec(memory_space=pltpu.VMEM)
    anywhere = pl.BlockSpec(memory_space=pltpu.HBM)
    packed = -(-members * (patch // LANES) // 16) * 16
    full_rows = -(-(lines + 2) // 8) * 8
    dma = pltpu.SemaphoreType.DMA
    return pl.pallas_call(
        functools.partial(analyse_kernel, n, spaces, halo, obs_count),
        out_shape=pltpu.VMEM((members, patch, quantities), BF16),
        in_specs=[anywhere] * 6,
        out_specs=vmem,
        scratch_shapes=[
            pltpu.SemaphoreType.REGULAR,
            pltpu.VMEM((members, patch), BF16),
            pltpu.VMEM((patch,), BF16),
            pltpu.VMEM((patch,), BF16),
            pltpu.VMEM((patch,), BF16),
            pltpu.VMEM((patch,), BF16),
            pltpu.VMEM((patch,), BF16),
            pltpu.VMEM((patch,), BF16),
            pltpu.VMEM((domains, obs_count), jnp.int32),
            pltpu.VMEM((patch,), jnp.int32),
            dma((5,)), dma((2,)),
            pltpu.VMEM((members, CHUNK, quantities), BF16),
            pltpu.VMEM((lines, domains, quantities), BF16),
            pltpu.VMEM((lines, domains, quantities), BF16),
            pltpu.VMEM((3, n, packed, LANES), BF16),
            pltpu.VMEM((full_rows, 3 * patch), F32),
            pltpu.VMEM((lines, width), F32),
            pltpu.VMEM((width, 2 * LANES), BF16),
            pltpu.VMEM((domains, width), F32),
            pltpu.VMEM((domains, width), F32),
            pltpu.VMEM((domains, lines, LANES), F32),
            pltpu.VMEM((domains, LANES), F32),
            pltpu.VMEM((domains, lines, LANES), BF16),
            pltpu.VMEM((1, LANES), F32),
            pltpu.VMEM((n * spaces, 1, LANES), F32),
            dma((1,)), dma((chunks,)), dma((1,)),
            dma((2, 2)), dma((max(n // 4 - 1, 1),)), dma((2,)), dma((3,)), dma((3,)), dma((1,)),
        ],
        compiler_params=pltpu.CompilerParams(
            collective_id=0, has_side_effects=True, vmem_limit_bytes=40 << 20
        ),
        name="analyse",
    )(*[pltpu.with_memory_space_constraint(a, pltpu.HBM) for a in (trials, sensors, readings, noises, lists, tiers)])


def solution(mesh):
    return jax.shard_map(
        per_device,
        mesh=mesh,
        in_specs=(
            P("member", ("region", "space"), None),
            P("member", ("region", "space")),
            P(("region", "space")),
            P(("region", "space")),
            P(("region", "space"), None),
            P(("region", "space")),
        ),
        out_specs=P("member", ("region", "space"), None),
        check_vma=False,
    )
```
